8 devices in a mesh: dp: 2 (over z, y), sp: 4 (over x, core).
Axes of the slice: x: 2, y: 2, z: 1, core: 2. Of those that a mesh axis runs over, the one named last changes fastest.
Arguments:
- tok_in: bfloat16 [4096, 2560], P(('dp', 'sp')), parts along dimension 0
- tok_pos: int32 [4096], P(('dp', 'sp')), parts along dimension 0
- w_dq: bfloat16 [2560, 768], replicated
- g_q: float32 [768], replicated
- w_uq: bfloat16 [768, 40, 96], replicated
- w_dkv: bfloat16 [2560, 288], replicated
- g_kv: float32 [256], replicated
- w_uk: bfloat16 [256, 40, 64], replicated
- w_uv: bfloat16 [256, 40, 64], replicated
- w_o: bfloat16 [40, 64, 2560], replicated
Outputs:
- output 1: bfloat16 [4096, 2560], P(('dp', 'sp')), parts along dimension 0
- output 2: bfloat16 [4096, 256], P(('dp', 'sp')), parts along dimension 0
- output 3: bfloat16 [4096, 32], P(('dp', 'sp')), parts along dimension 0
There are 2 independent parts. The reference program is written for one: setup_inputs(seed, part) draws one part's arguments, and reference() takes and returns one part's arrays. A program takes and returns all parts, laid end to end along the dimension named above; an argument that names none is the same for every part.
All inputs are finite; a program needn't handle non-finite values.
Results may differ from the reference program's by a relative error of at most 0.00435966.
Values are sent between devices in bfloat16 or wider.
A program may use at most 1 GiB of HBM per device.

```python
import math
import jax
import jax.numpy as jnp
from jax import lax

SEQ_LEN = 2048
ROW_BLOCK = 512
MODEL_DIM = 2560
NUM_HEADS = 40
Q_RANK = 768
KV_RANK = 256
NOPE_DIM = 64
ROPE_DIM = 32
V_DIM = 64

ROPE_THETA = 10000.0
YARN_FACTOR = 40.0
ORIG_CTX = 4096.0
BETA_FAST = 32.0
BETA_SLOW = 1.0
NORM_EPS = 1e-6


def rope_freqs(rot_dim):
    half_dim = rot_dim // 2
    log_base = 2.0 * math.log(ROPE_THETA)
    low_idx = max(math.floor(rot_dim * math.log(ORIG_CTX / (BETA_FAST * 2.0 * math.pi)) / log_base), 0)
    high_idx = min(math.ceil(rot_dim * math.log(ORIG_CTX / (BETA_SLOW * 2.0 * math.pi)) / log_base), half_dim - 1)
    spread = max(high_idx - low_idx, 0.001)
    freq_list = []
    for freq_idx in range(half_dim):
        base_freq = ROPE_THETA ** (-2.0 * freq_idx / rot_dim)
        ramp_val = min(max((freq_idx - low_idx) / spread, 0.0), 1.0)
        freq_list.append(base_freq / YARN_FACTOR * ramp_val + base_freq * (1.0 - ramp_val))
    return jnp.asarray(freq_list, dtype=jnp.float32)


def rotate_half(act_in, cos_t, sin_t):
    half_dim = act_in.shape[-1] // 2
    first = act_in[..., :half_dim]
    second = act_in[..., half_dim:]
    return jnp.concatenate([first * cos_t - second * sin_t, second * cos_t + first * sin_t], axis=-1)


def rms_norm(act_in, gain):
    mean_sq = jnp.mean(act_in * act_in, axis=-1, keepdims=True)
    return act_in * lax.rsqrt(mean_sq + NORM_EPS) * gain


def setup_inputs(seed: int = 0, part: int = 0) -> dict:
    root_key = jax.random.key(seed)
    part_key = jax.random.fold_in(root_key, part)
    key_x, key_pos = jax.random.split(part_key)
    weight_keys = jax.random.split(root_key, 8)

    def draw_weight(sub_key, arr_shape, fan_in):
        return (jax.random.normal(sub_key, arr_shape, jnp.float32) * fan_in ** -0.5).astype(jnp.bfloat16)

    tok_in = jax.random.normal(key_x, (SEQ_LEN, MODEL_DIM), jnp.float32).astype(jnp.bfloat16)
    pos_steps = jax.random.randint(key_pos, (SEQ_LEN,), 1, 5, dtype=jnp.int32)
    tok_pos = (jnp.cumsum(pos_steps) - pos_steps[0]).astype(jnp.int32)
    w_dq = draw_weight(weight_keys[0], (MODEL_DIM, Q_RANK), MODEL_DIM)
    g_q = jax.random.uniform(weight_keys[1], (Q_RANK,), jnp.float32, 0.5, 1.5)
    w_uq = draw_weight(weight_keys[2], (Q_RANK, NUM_HEADS, NOPE_DIM + ROPE_DIM), Q_RANK)
    w_dkv = draw_weight(weight_keys[3], (MODEL_DIM, KV_RANK + ROPE_DIM), MODEL_DIM)
    g_kv = jax.random.uniform(weight_keys[4], (KV_RANK,), jnp.float32, 0.5, 1.5)
    w_uk = draw_weight(weight_keys[5], (KV_RANK, NUM_HEADS, NOPE_DIM), KV_RANK)
    w_uv = draw_weight(weight_keys[6], (KV_RANK, NUM_HEADS, V_DIM), KV_RANK)
    w_o = draw_weight(weight_keys[7], (NUM_HEADS, V_DIM, MODEL_DIM), NUM_HEADS * V_DIM)
    return dict(tok_in=tok_in, tok_pos=tok_pos, w_dq=w_dq, g_q=g_q, w_uq=w_uq, w_dkv=w_dkv, g_kv=g_kv, w_uk=w_uk, w_uv=w_uv, w_o=w_o)


def reference(tok_in, tok_pos, w_dq, g_q, w_uq, w_dkv, g_kv, w_uk, w_uv, w_o):
    qk_dim = NOPE_DIM + ROPE_DIM
    attn_scale = (0.1 * math.log(YARN_FACTOR) + 1.0) ** 2 / math.sqrt(qk_dim)
    angles = tok_pos.astype(jnp.float32)[:, None] * rope_freqs(ROPE_DIM)[None, :]
    cos_t = jnp.cos(angles)
    sin_t = jnp.sin(angles)
    q_lat = rms_norm(jnp.dot(tok_in, w_dq, preferred_element_type=jnp.float32), g_q).astype(jnp.bfloat16)
    q_full = jnp.dot(q_lat, w_uq.reshape(Q_RANK, NUM_HEADS * qk_dim), preferred_element_type=jnp.float32).reshape(SEQ_LEN, NUM_HEADS, qk_dim)
    q_nope = q_full[:, :, :NOPE_DIM].astype(jnp.bfloat16)
    q_rot = rotate_half(q_full[:, :, NOPE_DIM:], cos_t[:, None, :], sin_t[:, None, :]).astype(jnp.bfloat16)
    kv_lat = jnp.dot(tok_in, w_dkv, preferred_element_type=jnp.float32)
    cache_kv = rms_norm(kv_lat[:, :KV_RANK], g_kv).astype(jnp.bfloat16)
    cache_pe = rotate_half(kv_lat[:, KV_RANK:], cos_t, sin_t).astype(jnp.bfloat16)
    k_nope = jnp.dot(cache_kv, w_uk.reshape(KV_RANK, NUM_HEADS * NOPE_DIM), preferred_element_type=jnp.float32).reshape(SEQ_LEN, NUM_HEADS, NOPE_DIM).astype(jnp.bfloat16)
    values = jnp.dot(cache_kv, w_uv.reshape(KV_RANK, NUM_HEADS * V_DIM), preferred_element_type=jnp.float32).reshape(SEQ_LEN, NUM_HEADS, V_DIM).astype(jnp.bfloat16)
    key_idx = jnp.arange(SEQ_LEN)
    num_blocks = SEQ_LEN // ROW_BLOCK

    def head_attention(head_in):
        qn_head, qr_head, kn_head, v_head = head_in

        def block_attention(blk_idx):
            start = blk_idx * ROW_BLOCK
            qn_blk = lax.dynamic_slice_in_dim(qn_head, start, ROW_BLOCK, axis=0)
            qr_blk = lax.dynamic_slice_in_dim(qr_head, start, ROW_BLOCK, axis=0)
            logits = jnp.dot(qn_blk, kn_head.T, preferred_element_type=jnp.float32) + jnp.dot(qr_blk, cache_pe.T, preferred_element_type=jnp.float32)
            logits = logits * attn_scale
            row_idx = start + jnp.arange(ROW_BLOCK)
            logits = jnp.where(key_idx[None, :] <= row_idx[:, None], logits, -jnp.inf)
            attn_prob = jax.nn.softmax(logits, axis=-1).astype(jnp.bfloat16)
            return jnp.dot(attn_prob, v_head, preferred_element_type=jnp.float32).astype(jnp.bfloat16)

        return lax.map(block_attention, jnp.arange(num_blocks)).reshape(SEQ_LEN, V_DIM)

    head_outs = lax.map(head_attention, (jnp.swapaxes(q_nope, 0, 1), jnp.swapaxes(q_rot, 0, 1), jnp.swapaxes(k_nope, 0, 1), jnp.swapaxes(values, 0, 1)))
    attn_cat = jnp.swapaxes(head_outs, 0, 1).reshape(SEQ_LEN, NUM_HEADS * V_DIM)
    attn_out = jnp.dot(attn_cat, w_o.reshape(NUM_HEADS * V_DIM, MODEL_DIM), preferred_element_type=jnp.float32).astype(jnp.bfloat16)
    return attn_out, cache_kv, cache_pe
```

```python
import functools
import math
import jax
import jax.numpy as jnp
from jax import lax
from jax.experimental import pallas as pl
from jax.experimental.pallas import tpu as pltpu
from jax.sharding import PartitionSpec as P

ROPE_THETA = 10000.0
YARN_FACTOR = 40.0
ORIG_CTX = 4096.0
BETA_FAST = 32.0
BETA_SLOW = 1.0
NORM_EPS = 1e-6


def rope_freqs(rot_dim):
    half_dim = rot_dim // 2
    log_base = 2.0 * math.log(ROPE_THETA)
    low_idx = max(math.floor(rot_dim * math.log(ORIG_CTX / (BETA_FAST * 2.0 * math.pi)) / log_base), 0)
    high_idx = min(math.ceil(rot_dim * math.log(ORIG_CTX / (BETA_SLOW * 2.0 * math.pi)) / log_base), half_dim - 1)
    spread = max(high_idx - low_idx, 0.001)
    freq_list = []
    for freq_idx in range(half_dim):
        base_freq = ROPE_THETA ** (-2.0 * freq_idx / rot_dim)
        ramp_val = min(max((freq_idx - low_idx) / spread, 0.0), 1.0)
        freq_list.append(base_freq / YARN_FACTOR * ramp_val + base_freq * (1.0 - ramp_val))
    return jnp.asarray(freq_list, dtype=jnp.float32)


def rotate_half(act_in, cos_t, sin_t):
    half_dim = act_in.shape[-1] // 2
    first = act_in[..., :half_dim]
    second = act_in[..., half_dim:]
    return jnp.concatenate([first * cos_t - second * sin_t, second * cos_t + first * sin_t], axis=-1)


def rms_norm(act_in, gain):
    mean_sq = jnp.mean(act_in * act_in, axis=-1, keepdims=True)
    return act_in * lax.rsqrt(mean_sq + NORM_EPS) * gain


ATTN_GROUP = 8


def attention_kernel(nprev_ref, qt_ref, ck_ref, wuk_ref, wuv_ref, wo_hbm, out_ref,
                     qaug, kn, vt, s_a, s_b, c_a, c_b, m_s, l_s, acc, o_nat, wo, wo_sem,
                     *, scale2, rows, nope, rot, vdim):
    nprev = nprev_ref[0]
    heads = qt_ref.shape[0]
    G = ATTN_GROUP
    wo_copy = pltpu.make_async_copy(wo_hbm, wo, wo_sem)
    wo_copy.start()
    qaug[...] = jnp.zeros_like(qaug)
    NT = (((1,), (1,)), ((), ()))
    NN = (((1,), (0,)), ((), ()))
    f32 = jnp.float32
    bf16 = jnp.bfloat16
    half = rows // 2

    def keys(h, start, size):
        return jnp.concatenate([kn[h // 2, pl.ds(start, size), :], ck_ref[pl.ds(start, size), 256:384]], axis=1)

    def scores(h, blk, s_ref, c_ref):
        start = pl.multiple_of(blk * rows, rows)
        s = lax.dot_general(keys(h, start, rows), qaug[h], NN, preferred_element_type=f32)
        s_ref[...] = s
        c_ref[...] = jnp.max(s, axis=0, keepdims=True)

    def absorb(h, blk, s_ref, c_ref):
        start = pl.multiple_of(blk * rows, rows)
        m_old = m_s[h]
        m_new = jnp.maximum(m_old, c_ref[...])
        m_s[h] = m_new
        alpha = jnp.exp2((m_old - m_new) * scale2)
        p = jnp.exp2((s_ref[...] - m_new) * scale2)
        l_s[h] = l_s[h] * alpha + jnp.sum(p, axis=0, keepdims=True)
        pv = lax.dot_general(vt[h, :, pl.ds(start, rows)], p.astype(bf16), NN, preferred_element_type=f32)
        acc[h] = acc[h] * alpha + pv

    row_i = lax.broadcasted_iota(jnp.int32, (half, half), 0)
    col_i = lax.broadcasted_iota(jnp.int32, (half, half), 1)
    visible = row_i <= col_i
    own = pl.multiple_of(nprev * rows, rows)

    def diagonal(h):
        for a in range(2):
            qh = qaug[h, :, a * half:(a + 1) * half]
            nk = (a + 1) * half
            s = lax.dot_general(keys(h, own, nk), qh, NN, preferred_element_type=f32)
            tail = jnp.where(visible, s[a * half:, :], -jnp.inf)
            s = tail if a == 0 else jnp.concatenate([s[:half, :], tail], axis=0)
            m = jnp.max(s, axis=0, keepdims=True)
            p = jnp.exp2((s - m) * scale2)
            cols = slice(a * half, (a + 1) * half)
            m_s[h, :, cols] = m
            l_s[h, :, cols] = jnp.sum(p, axis=0, keepdims=True)
            acc[h, :, cols] = lax.dot_general(vt[h, :, pl.ds(own, nk)], p.astype(bf16), NN, preferred_element_type=f32)

    def group(g, carry):
        for h in range(G):
            lo = (h % 2) * nope
            qaug[h, lo:lo + nope, :] = qt_ref[g * G + h, :nope, :]
            qaug[h, 2 * nope:2 * nope + rot, :] = qt_ref[g * G + h, nope:, :]

        def up(b, c2):
            start = pl.multiple_of(b * rows, rows)
            ckb = ck_ref[pl.ds(start, rows), :256]
            for j in range(G // 4):
                wk = wuk_ref[pl.ds(pl.multiple_of((g * G + 4 * j) * nope, 4 * nope), 4 * nope), :]
                kk = lax.dot_general(ckb, wk, NT, preferred_element_type=f32).astype(bf16)
                kn[2 * j, pl.ds(start, rows), :] = kk[:, :128]
                kn[2 * j + 1, pl.ds(start, rows), :] = kk[:, 128:]
                wv = wuv_ref[pl.ds(pl.multiple_of((g * G + 4 * j) * vdim, 4 * vdim), 4 * vdim), :]
                vv = lax.dot_general(wv, ckb, NT, preferred_element_type=f32).astype(bf16)
                for i in range(4):
                    vt[4 * j + i, :, pl.ds(start, rows)] = vv[i * vdim:(i + 1) * vdim, :]
            return c2

        lax.fori_loop(0, nprev + 1, up, 0)
        for h in range(G):
            diagonal(h)

        @pl.when(nprev > 0)
        def _():
            scores(0, 0, s_a, c_a)

            def pair(t, c2):
                i0 = 2 * t
                h0, b0 = i0 // nprev, i0 % nprev
                i1 = i0 + 1
                h1, b1 = i1 // nprev, i1 % nprev
                i2 = jnp.minimum(i0 + 2, G * nprev - 1)
                h2, b2 = i2 // nprev, i2 % nprev
                scores(h1, b1, s_b, c_b)
                absorb(h0, b0, s_a, c_a)
                scores(h2, b2, s_a, c_a)
                absorb(h1, b1, s_b, c_b)
                return c2

            lax.fori_loop(0, G * nprev // 2, pair, 0)

        for j in range(G // 2):
            o2 = jnp.concatenate([acc[2 * j] / l_s[2 * j], acc[2 * j + 1] / l_s[2 * j + 1]], axis=0)
            o_nat[g * (G // 2) + j] = o2.T.astype(bf16)
        return carry

    lax.fori_loop(0, heads // G, group, 0)
    wo_copy.wait()
    npair = heads // 2
    o_all = jnp.concatenate([o_nat[j] for j in range(npair)], axis=1)
    d = wo.shape[1]
    for n in range(0, d, 512):
        out_ref[:, n:n + 512] = lax.dot_general(o_all, wo[:, n:n + 512], NN, preferred_element_type=f32).astype(bf16)


def attention(nprev, qt, ck, wukt, wuvt, wo, scale2):
    heads, qk, rows = qt.shape
    seq = ck.shape[0]
    vdim = wuvt.shape[0] // heads
    nope = wukt.shape[0] // heads
    rot = qk - nope
    G = ATTN_GROUP
    vm = pl.BlockSpec(memory_space=pltpu.VMEM)
    f32 = jnp.float32
    bf16 = jnp.bfloat16
    return pl.pallas_call(
        functools.partial(attention_kernel, scale2=scale2, rows=rows, nope=nope, rot=rot, vdim=vdim),
        out_shape=jax.ShapeDtypeStruct((rows, wo.shape[1]), bf16),
        in_specs=[pl.BlockSpec(memory_space=pltpu.SMEM), vm, vm, vm, vm, pl.BlockSpec(memory_space=pl.ANY)],
        out_specs=vm,
        scratch_shapes=[
            pltpu.VMEM((G, 256, rows), bf16),
            pltpu.VMEM((G // 2, seq, 128), bf16),
            pltpu.VMEM((G, vdim, seq), bf16),
            pltpu.VMEM((rows, rows), f32),
            pltpu.VMEM((rows, rows), f32),
            pltpu.VMEM((1, rows), f32),
            pltpu.VMEM((1, rows), f32),
            pltpu.VMEM((G, 1, rows), f32),
            pltpu.VMEM((G, 1, rows), f32),
            pltpu.VMEM((G, vdim, rows), f32),
            pltpu.VMEM((heads // 2, rows, 2 * vdim), bf16),
            pltpu.VMEM(wo.shape, bf16),
            pltpu.SemaphoreType.DMA,
        ],
        compiler_params=pltpu.CompilerParams(vmem_limit_bytes=60 * 1024 * 1024),
        cost_estimate=pl.CostEstimate(flops=40_000_000_000, bytes_accessed=40_000_000, transcendentals=30_000_000),
    )(nprev, qt, ck, wukt, wuvt, wo)


def solution(mesh):
    tok_spec = P(('dp', 'sp'))
    rows_spec = P(('dp', 'sp'), None)
    replicated = P()

    def local_step(tok_in, tok_pos, w_dq, g_q, w_uq, w_dkv, g_kv, w_uk, w_uv, w_o):
        rows = tok_in.shape[0]
        q_rank, num_heads, qk_dim = w_uq.shape
        kv_rank = g_kv.shape[0]
        rot_dim = w_dkv.shape[1] - kv_rank
        nope_dim = qk_dim - rot_dim
        v_dim = w_uv.shape[2]
        attn_scale = (0.1 * math.log(YARN_FACTOR) + 1.0) ** 2 / math.sqrt(qk_dim)
        f32 = jnp.float32
        angles = tok_pos.astype(f32)[:, None] * rope_freqs(rot_dim)[None, :]
        cos_t = jnp.cos(angles)
        sin_t = jnp.sin(angles)
        kv_lat = jnp.dot(tok_in, w_dkv, preferred_element_type=f32)
        cache_kv = rms_norm(kv_lat[:, :kv_rank], g_kv).astype(jnp.bfloat16)
        cache_pe = rotate_half(kv_lat[:, kv_rank:], cos_t, sin_t).astype(jnp.bfloat16)
        ck = jnp.concatenate([cache_kv, jnp.pad(cache_pe, ((0, 0), (0, 128 - rot_dim)))], axis=1)
        ck_all = lax.all_gather(ck, 'sp', axis=0, tiled=True)
        q_lat = rms_norm(jnp.dot(tok_in, w_dq, preferred_element_type=f32), g_q).astype(jnp.bfloat16)
        q_full = jnp.einsum('tc,che->het', q_lat, w_uq, preferred_element_type=f32)
        z1 = q_full[:, nope_dim:nope_dim + rot_dim // 2]
        z2 = q_full[:, nope_dim + rot_dim // 2:]
        ct, st = cos_t.T[None], sin_t.T[None]
        qt = jnp.concatenate([q_full[:, :nope_dim], z1 * ct - z2 * st, z2 * ct + z1 * st], axis=1).astype(jnp.bfloat16)
        wukt = jnp.transpose(w_uk, (1, 2, 0)).reshape(num_heads * nope_dim, kv_rank)
        wuvt = jnp.transpose(w_uv, (1, 2, 0)).reshape(num_heads * v_dim, kv_rank)
        nprev = lax.axis_index('sp').astype(jnp.int32)[None]
        attn_out = attention(nprev, qt, ck_all, wukt, wuvt, w_o.reshape(num_heads * v_dim, -1), attn_scale * math.log2(math.e))
        return attn_out, cache_kv, cache_pe

    return jax.shard_map(local_step, mesh=mesh, in_specs=(rows_spec, tok_spec, replicated, replicated, replicated, replicated, replicated, replicated, replicated, replicated), out_specs=(rows_spec, rows_spec, rows_spec), check_vma=False)
```

```python
import functools
import math
import jax
import jax.numpy as jnp
from jax import lax
from jax.experimental import pallas as pl
from jax.experimental.pallas import tpu as pltpu
from jax.sharding import PartitionSpec as P

ROPE_THETA = 10000.0
YARN_FACTOR = 40.0
ORIG_CTX = 4096.0
BETA_FAST = 32.0
BETA_SLOW = 1.0
NORM_EPS = 1e-6


def rope_freqs(rot_dim):
    half_dim = rot_dim // 2
    log_base = 2.0 * math.log(ROPE_THETA)
    low_idx = max(math.floor(rot_dim * math.log(ORIG_CTX / (BETA_FAST * 2.0 * math.pi)) / log_base), 0)
    high_idx = min(math.ceil(rot_dim * math.log(ORIG_CTX / (BETA_SLOW * 2.0 * math.pi)) / log_base), half_dim - 1)
    spread = max(high_idx - low_idx, 0.001)
    freq_list = []
    for freq_idx in range(half_dim):
        base_freq = ROPE_THETA ** (-2.0 * freq_idx / rot_dim)
        ramp_val = min(max((freq_idx - low_idx) / spread, 0.0), 1.0)
        freq_list.append(base_freq / YARN_FACTOR * ramp_val + base_freq * (1.0 - ramp_val))
    return jnp.asarray(freq_list, dtype=jnp.float32)


def rotate_half(act_in, cos_t, sin_t):
    half_dim = act_in.shape[-1] // 2
    first = act_in[..., :half_dim]
    second = act_in[..., half_dim:]
    return jnp.concatenate([first * cos_t - second * sin_t, second * cos_t + first * sin_t], axis=-1)


def rms_norm(act_in, gain):
    mean_sq = jnp.mean(act_in * act_in, axis=-1, keepdims=True)
    return act_in * lax.rsqrt(mean_sq + NORM_EPS) * gain


HEAD_GROUP = 20
QUAD = 4


def attention_kernel(nprev_ref, qt_ref, ck_ref, wuk_ref, wuv_ref, wo_hbm, out_ref,
                     qaug, kn, vt, s_buf, c_buf, p_buf, al_buf, m_s, acc, o_nat, wo, wo_sem,
                     *, scale2, rows, nope, rot, vdim):
    nprev = nprev_ref[0]
    heads = qt_ref.shape[0]
    G = HEAD_GROUP
    nq = G // QUAD
    wo_copy = pltpu.make_async_copy(wo_hbm, wo, wo_sem)
    wo_copy.start()
    qaug[...] = jnp.zeros_like(qaug)
    vt[:, vdim:, :] = jnp.ones((vt.shape[0], vt.shape[1] - vdim, vt.shape[2]), vt.dtype)
    NT = (((1,), (1,)), ((), ()))
    NN = (((1,), (0,)), ((), ()))
    f32 = jnp.float32
    bf16 = jnp.bfloat16
    half = rows // 2
    FULL = ((0, 0), (1, 0), (0, 1), (1, 1))
    OWN = ((0, 0), (0, 1), (1, 1))
    row_i = lax.broadcasted_iota(jnp.int32, (half, half), 0)
    col_i = lax.broadcasted_iota(jnp.int32, (half, half), 1)

    def cols(a):
        return slice(a * half, (a + 1) * half)

    def score_stage(u, quad, blk, pieces):
        start = pl.multiple_of(blk * rows, rows)
        tops = [None, None]
        for k, a in pieces:
            lhs = jnp.concatenate([kn[quad * (QUAD // 2) + u // 2, pl.ds(start + k * half, half), :],
                                   ck_ref[pl.ds(start + k * half, half), 256:384]], axis=1)
            s = lax.dot_general(lhs, qaug[quad * QUAD + u, :, cols(a)], NN, preferred_element_type=f32)
            if pieces is OWN and k == a:
                s = jnp.where(row_i <= col_i, s, -jnp.inf)
            s_buf[u, cols(k), cols(a)] = s
            top = jnp.max(s, axis=0, keepdims=True)
            tops[a] = top if tops[a] is None else jnp.maximum(tops[a], top)
        for a in range(2):
            c_buf[u, :, cols(a)] = tops[a]

    def exp_stage(u, quad, pieces):
        h = quad * QUAD + u
        m_new = c_buf[u]
        if pieces is FULL:
            m_old = m_s[h]
            m_new = jnp.maximum(m_old, m_new)
            al_buf[u] = jnp.exp2((m_old - m_new) * scale2)
        m_s[h] = m_new
        for k, a in pieces:
            p_buf[u, cols(k), cols(a)] = jnp.exp2((s_buf[u, cols(k), cols(a)] - m_new[:, cols(a)]) * scale2).astype(bf16)

    def value_stage(u, quad, blk, pieces):
        h = quad * QUAD + u
        start = pl.multiple_of(blk * rows, rows)
        for a in range(2):
            nk = rows if pieces is FULL else (a + 1) * half
            t = lax.dot_general(vt[h, :, pl.ds(start, nk)], p_buf[u, :nk, cols(a)], NN, preferred_element_type=f32)
            if pieces is FULL:
                t = t + acc[h, :, cols(a)] * al_buf[u, :, cols(a)]
            acc[h, :, cols(a)] = t

    def pipeline(count, place, pieces):
        def step(i, first, last):
            for u in range(QUAD):
                if first < 1:
                    value_stage(u, *place(i - 2), pieces)
                if first < 2 and last < 2:
                    exp_stage(u, place(i - 1)[0], pieces)
                if last < 1:
                    score_stage(u, *place(i), pieces)

        step(0, 2, 0)
        step(1, 1, 0)

        def body(i, c):
            step(i, 0, 0)
            return c

        lax.fori_loop(2, count, body, 0)
        step(count, 0, 1)
        step(count + 1, 0, 2)

    def group(g, carry):
        for h in range(G):
            lo = (h % 2) * nope
            qaug[h, lo:lo + nope, :] = qt_ref[g * G + h, :nope, :]
            qaug[h, 2 * nope:2 * nope + rot, :] = qt_ref[g * G + h, nope:, :]

        def up(b, c2):
            start = pl.multiple_of(b * rows, rows)
            ckb = ck_ref[pl.ds(start, rows), :256]
            for j in range(nq):
                wk = wuk_ref[pl.ds(pl.multiple_of((g * G + 4 * j) * nope, 4 * nope), 4 * nope), :]
                kk = lax.dot_general(ckb, wk, NT, preferred_element_type=f32).astype(bf16)
                kn[2 * j, pl.ds(start, rows), :] = kk[:, :128]
                kn[2 * j + 1, pl.ds(start, rows), :] = kk[:, 128:]
                wv = wuv_ref[pl.ds(pl.multiple_of((g * G + 4 * j) * vdim, 4 * vdim), 4 * vdim), :]
                vv = lax.dot_general(wv, ckb, NT, preferred_element_type=f32).astype(bf16)
                for i in range(4):
                    vt[4 * j + i, :vdim, pl.ds(start, rows)] = vv[i * vdim:(i + 1) * vdim, :]
            return c2

        lax.fori_loop(0, nprev + 1, up, 0)
        pipeline(nq, lambda i: (i, nprev), OWN)

        @pl.when(nprev > 0)
        def _():
            pipeline(nq * nprev, lambda i: (lax.rem(i, nq), lax.div(i, nq)), FULL)

        for j in range(G // 2):
            o2 = jnp.concatenate([acc[h, :vdim, :] / acc[h, vdim:vdim + 1, :] for h in (2 * j, 2 * j + 1)], axis=0)
            o_nat[g * (G // 2) + j] = o2.T.astype(bf16)
        return carry

    lax.fori_loop(0, heads // G, group, 0)
    wo_copy.wait()
    npair = heads // 2
    o_all = jnp.concatenate([o_nat[j] for j in range(npair)], axis=1)
    d = wo.shape[1]
    for n in range(0, d, 512):
        out_ref[:, n:n + 512] = lax.dot_general(o_all, wo[:, n:n + 512], NN, preferred_element_type=f32).astype(bf16)


def attention(nprev, qt, ck, wukt, wuvt, wo, scale2):
    heads, qk, rows = qt.shape
    seq = ck.shape[0]
    vdim = wuvt.shape[0] // heads
    nope = wukt.shape[0] // heads
    rot = qk - nope
    G = HEAD_GROUP
    vm = pl.BlockSpec(memory_space=pltpu.VMEM)
    f32 = jnp.float32
    bf16 = jnp.bfloat16
    return pl.pallas_call(
        functools.partial(attention_kernel, scale2=scale2, rows=rows, nope=nope, rot=rot, vdim=vdim),
        out_shape=jax.ShapeDtypeStruct((rows, wo.shape[1]), bf16),
        in_specs=[pl.BlockSpec(memory_space=pltpu.SMEM), vm, vm, vm, vm, pl.BlockSpec(memory_space=pl.ANY)],
        out_specs=vm,
        scratch_shapes=[
            pltpu.VMEM((G, 256, rows), bf16),
            pltpu.VMEM((G // 2, seq, 128), bf16),
            pltpu.VMEM((G, vdim + 16, seq), bf16),
            pltpu.VMEM((QUAD, rows, rows), f32),
            pltpu.VMEM((QUAD, 1, rows), f32),
            pltpu.VMEM((QUAD, rows, rows), bf16),
            pltpu.VMEM((QUAD, 1, rows), f32),
            pltpu.VMEM((G, 1, rows), f32),
            pltpu.VMEM((G, vdim + 16, rows), f32),
            pltpu.VMEM((heads // 2, rows, 2 * vdim), bf16),
            pltpu.VMEM(wo.shape, bf16),
            pltpu.SemaphoreType.DMA,
        ],
        compiler_params=pltpu.CompilerParams(vmem_limit_bytes=62 * 1024 * 1024),
        cost_estimate=pl.CostEstimate(flops=40_000_000_000, bytes_accessed=40_000_000, transcendentals=30_000_000),
    )(nprev, qt, ck, wukt, wuvt, wo)


def solution(mesh):
    tok_spec = P(('dp', 'sp'))
    rows_spec = P(('dp', 'sp'), None)
    replicated = P()

    def local_step(tok_in, tok_pos, w_dq, g_q, w_uq, w_dkv, g_kv, w_uk, w_uv, w_o):
        rows = tok_in.shape[0]
        q_rank, num_heads, qk_dim = w_uq.shape
        kv_rank = g_kv.shape[0]
        rot_dim = w_dkv.shape[1] - kv_rank
        nope_dim = qk_dim - rot_dim
        v_dim = w_uv.shape[2]
        attn_scale = (0.1 * math.log(YARN_FACTOR) + 1.0) ** 2 / math.sqrt(qk_dim)
        f32 = jnp.float32
        angles = tok_pos.astype(f32)[:, None] * rope_freqs(rot_dim)[None, :]
        cos_t = jnp.cos(angles)
        sin_t = jnp.sin(angles)
        kv_lat = jnp.dot(tok_in, w_dkv, preferred_element_type=f32)
        cache_kv = rms_norm(kv_lat[:, :kv_rank], g_kv).astype(jnp.bfloat16)
        cache_pe = rotate_half(kv_lat[:, kv_rank:], cos_t, sin_t).astype(jnp.bfloat16)
        ck = jnp.concatenate([cache_kv, jnp.pad(cache_pe, ((0, 0), (0, 128 - rot_dim)))], axis=1)
        ck_all = lax.all_gather(ck, 'sp', axis=0, tiled=True)
        q_lat = rms_norm(jnp.dot(tok_in, w_dq, preferred_element_type=f32), g_q).astype(jnp.bfloat16)
        q_full = jnp.einsum('tc,che->het', q_lat, w_uq, preferred_element_type=f32)
        z1 = q_full[:, nope_dim:nope_dim + rot_dim // 2]
        z2 = q_full[:, nope_dim + rot_dim // 2:]
        ct, st = cos_t.T[None], sin_t.T[None]
        qt = jnp.concatenate([q_full[:, :nope_dim], z1 * ct - z2 * st, z2 * ct + z1 * st], axis=1).astype(jnp.bfloat16)
        wukt = jnp.transpose(w_uk, (1, 2, 0)).reshape(num_heads * nope_dim, kv_rank)
        wuvt = jnp.transpose(w_uv, (1, 2, 0)).reshape(num_heads * v_dim, kv_rank)
        nprev = lax.axis_index('sp').astype(jnp.int32)[None]
        attn_out = attention(nprev, qt, ck_all, wukt, wuvt, w_o.reshape(num_heads * v_dim, -1), attn_scale * math.log2(math.e))
        return attn_out, cache_kv, cache_pe

    return jax.shard_map(local_step, mesh=mesh, in_specs=(rows_spec, tok_spec, replicated, replicated, replicated, replicated, replicated, replicated, replicated, replicated), out_specs=(rows_spec, rows_spec, rows_spec), check_vma=False)
```

```python
import functools
import math
import jax
import jax.numpy as jnp
from jax import lax
from jax.experimental import pallas as pl
from jax.experimental.pallas import tpu as pltpu
from jax.sharding import PartitionSpec as P

ROPE_THETA = 10000.0
YARN_FACTOR = 40.0
ORIG_CTX = 4096.0
BETA_FAST = 32.0
BETA_SLOW = 1.0
NORM_EPS = 1e-6


def rope_freqs(rot_dim):
    half_dim = rot_dim // 2
    log_base = 2.0 * math.log(ROPE_THETA)
    low_idx = max(math.floor(rot_dim * math.log(ORIG_CTX / (BETA_FAST * 2.0 * math.pi)) / log_base), 0)
    high_idx = min(math.ceil(rot_dim * math.log(ORIG_CTX / (BETA_SLOW * 2.0 * math.pi)) / log_base), half_dim - 1)
    spread = max(high_idx - low_idx, 0.001)
    freq_list = []
    for freq_idx in range(half_dim):
        base_freq = ROPE_THETA ** (-2.0 * freq_idx / rot_dim)
        ramp_val = min(max((freq_idx - low_idx) / spread, 0.0), 1.0)
        freq_list.append(base_freq / YARN_FACTOR * ramp_val + base_freq * (1.0 - ramp_val))
    return jnp.asarray(freq_list, dtype=jnp.float32)


GROUP = 8
SLOTS = 3
HELPED = (2, 1)


def layer_kernel(trig_in, gq_ref, gkv_ref, x_hbm, wdkv_hbm, wdq_hbm, wuq_hbm, wuk_hbm, wuv_hbm,
                 o_hbm, ckv_out, cpe_out,
                 x, wdkv, wdq, wuq, wuk, wuv, qlat, trig, ckv, pet, pen, qaug, kn, vt,
                 s_buf, c_buf, p_buf, al_buf, m_s, acc, o_nat, o_help,
                 load_sem, c_send, c_recv, pe_send, pe_recv, q_send, q_recv, t_send, t_recv, o_send, o_recv, out_sem,
                 *, scale2, rows, nope, rot, vdim, heads, groups):
    f32 = jnp.float32
    bf16 = jnp.bfloat16
    NT = (((1,), (1,)), ((), ()))
    NN = (((1,), (0,)), ((), ()))
    half = rows // 2
    qk = nope + rot
    pairs = GROUP // 2
    ngroup = heads // GROUP
    me = lax.axis_index('sp')
    partner = groups - 1 - me
    given = jnp.where(me == groups - 1, HELPED[0], jnp.where(me == groups - 2, HELPED[1], 0))
    helped = jnp.where(me == 0, HELPED[0], jnp.where(me == 1, HELPED[1], 0))
    n_own = ngroup - given
    n_all = n_own + helped

    loads = [pltpu.make_async_copy(s, d, load_sem.at[i]) for i, (s, d) in enumerate(
        ((x_hbm, x), (wdkv_hbm, wdkv), (wdq_hbm, wdq), (wuq_hbm, wuq), (wuk_hbm, wuk), (wuv_hbm, wuv)))]
    for c in loads:
        c.start()
    barrier = pltpu.get_barrier_semaphore()
    for d in range(1, groups):
        pl.semaphore_signal(barrier, inc=1, device_id={'sp': lax.rem(me + d, groups)}, device_id_type=pl.DeviceIdType.MESH)

    def remote(s, d, ssem, rsem, to):
        return pltpu.make_async_remote_copy(src_ref=s, dst_ref=d, send_sem=ssem, recv_sem=rsem,
                                            device_id={'sp': to}, device_id_type=pl.DeviceIdType.MESH)

    def latent_copies(origin, to):
        return (remote(ckv.at[origin], ckv.at[origin], c_send.at[to], c_recv.at[origin], to),
                remote(pet.at[origin], pet.at[origin], pe_send.at[to], pe_recv.at[origin], to))

    def query_copies(to):
        return (remote(qlat.at[0], qlat.at[1], q_send, q_recv, to),
                remote(trig.at[0], trig.at[1], t_send, t_recv, to))

    def start(copies):
        for c in copies:
            c.start()

    def received(origin):
        for c in latent_copies(origin, me):
            c.wait_recv()
        unpack_rope(origin)

    def unpack_rope(origin):
        wide = jnp.concatenate([pet[origin].astype(f32), jnp.zeros((128 - rot, rows), f32)], axis=0)
        pen[origin] = wide.T.astype(bf16)

    trig[0] = trig_in[...]
    hr = rot // 2
    loads[0].wait()
    loads[1].wait()
    kvt = lax.dot_general(wdkv[...], x[...], NT, preferred_element_type=f32)
    rank = ckv.shape[2]
    a = kvt[:rank]
    norm = a * lax.rsqrt(jnp.sum(a * a, axis=0, keepdims=True) / rank + NORM_EPS) * gkv_ref[...]
    c_own = norm.T.astype(bf16)
    ckv[me] = c_own
    ckv_out[...] = c_own
    z1, z2 = kvt[rank:rank + hr], kvt[rank + hr:]
    cos_t, sin_t = trig_in[:hr], trig_in[hr:]
    pe_own = jnp.concatenate([z1 * cos_t - z2 * sin_t, z2 * cos_t + z1 * sin_t], axis=0).astype(bf16)
    pet[me] = pe_own
    cpe_out[...] = pe_own
    loads[2].wait()
    ql = lax.dot_general(x[...], wdq[...], NN, preferred_element_type=f32)
    qrank = ql.shape[1]
    ql = ql * lax.rsqrt(jnp.sum(ql * ql, axis=1, keepdims=True) / qrank + NORM_EPS) * gq_ref[...]
    qlat[0] = ql.astype(bf16)
    pl.semaphore_wait(barrier, groups - 1)

    @pl.when(me == 0)
    def _():
        for t in (1, 3, 2):
            start(latent_copies(me, t))

    @pl.when(me == 1)
    def _():
        for t in (0, 2, 3):
            start(latent_copies(me, t))

    @pl.when(me == 2)
    def _():
        for t in (3, 0):
            start(latent_copies(me, t))

    unpack_rope(me)
    qaug[...] = jnp.zeros_like(qaug)
    vt[:, vdim:, :] = jnp.ones((vt.shape[0], vt.shape[1] - vdim, vt.shape[2]), vt.dtype)
    for c in loads[3:]:
        c.wait()

    @pl.when(me == 3)
    def _():
        start(query_copies(0))
        start(latent_copies(me, 0))

    FULL = ((0, 0), (1, 0), (0, 1), (1, 1))
    OWN = ((0, 0), (0, 1), (1, 1))
    row_i = lax.broadcasted_iota(jnp.int32, (half, half), 0)
    col_i = lax.broadcasted_iota(jnp.int32, (half, half), 1)

    def cols(i):
        return slice(i * half, (i + 1) * half)

    def score_stage(u, blk, own):
        tops = [None, None]
        for k, i in (OWN if own else FULL):
            lhs = jnp.concatenate([kn[u // 2, pl.ds(pl.multiple_of(blk * rows + k * half, half), half), :], pen[blk, cols(k), :]], axis=1)
            s = lax.dot_general(lhs, qaug[u, :, cols(i)], NN, preferred_element_type=f32)
            if own and k == i:
                s = jnp.where(row_i <= col_i, s, -jnp.inf)
            s_buf[u, cols(k), cols(i)] = s
            top = jnp.max(s, axis=0, keepdims=True)
            tops[i] = top if tops[i] is None else jnp.maximum(tops[i], top)
        if own:
            s_buf[u, cols(1), cols(0)] = jnp.full((half, half), -jnp.inf, f32)
        for i in range(2):
            c_buf[u, :, cols(i)] = tops[i]

    def exp_stage(u, slot):
        h = slot * GROUP + u
        m_old = m_s[h]
        m_new = jnp.maximum(m_old, c_buf[u])
        al_buf[u] = jnp.exp2((m_old - m_new) * scale2)
        m_s[h] = m_new
        for k, i in FULL:
            p_buf[u, cols(k), cols(i)] = jnp.exp2((s_buf[u, cols(k), cols(i)] - m_new[:, cols(i)]) * scale2).astype(bf16)

    def value_stage(u, slot, blk):
        h = slot * GROUP + u
        v = vt[h, :, pl.ds(pl.multiple_of(blk * rows, rows), rows)]
        for i in range(2):
            t = lax.dot_general(v, p_buf[u, :, cols(i)], NN, preferred_element_type=f32)
            acc[h, :, cols(i)] = t + acc[h, :, cols(i)] * al_buf[u, :, cols(i)]

    def output_copy(grp):
        return pltpu.make_async_copy(o_nat.at[pl.ds(grp * pairs, pairs)], o_hbm.at[pl.ds(grp * pairs, pairs)], out_sem.at[grp])

    def help_copy(k):
        grp = ngroup - helped + k
        return remote(o_help.at[k], o_nat.at[pl.ds(grp * pairs, pairs)], o_send.at[k], o_recv.at[k], partner)

    def finish(slot, gi):
        outs = []
        for j in range(pairs):
            t = jnp.concatenate([acc[slot * GROUP + h, :vdim, :] / acc[slot * GROUP + h, vdim:vdim + 1, :] for h in (2 * j, 2 * j + 1)], axis=0)
            outs.append(t.T.astype(bf16))

        @pl.when(gi < n_own)
        def _():
            for j in range(pairs):
                o_nat[gi * pairs + j] = outs[j]
            output_copy(gi).start()

        @pl.when(gi >= n_own)
        def _():
            for j in range(pairs):
                o_help[gi - n_own, j] = outs[j]
            help_copy(gi - n_own).start()

    def step(carry, new, own):
        (slot1, blk1, last1, gi1), (slot2, blk2, last2, gi2) = carry
        for u in range(GROUP):
            value_stage(u, slot2, blk2)
            exp_stage(u, slot1)
            if new is not None:
                score_stage(u, new[1], own)

        @pl.when(last2 == 1)
        def _():
            finish(slot2, gi2)

        return (new if new is not None else (SLOTS, 0, 0, 0)), (slot1, blk1, last1, gi1)

    def keys_and_values(slot, head0, blk):
        c = ckv[blk]
        at = pl.multiple_of(blk * rows, rows)
        for j in range(GROUP // 4):
            wk = wuk[pl.ds(pl.multiple_of((head0 + 4 * j) * nope, 4 * nope), 4 * nope), :]
            kk = lax.dot_general(c, wk, NT, preferred_element_type=f32).astype(bf16)
            kn[2 * j, pl.ds(at, rows), :] = kk[:, :128]
            kn[2 * j + 1, pl.ds(at, rows), :] = kk[:, 128:]
            wv = wuv[pl.ds(pl.multiple_of((head0 + 4 * j) * vdim, 4 * vdim), 4 * vdim), :]
            vv = lax.dot_general(wv, c, NT, preferred_element_type=f32).astype(bf16)
            for i in range(4):
                vt[slot * GROUP + 4 * j + i, :vdim, pl.ds(at, rows)] = vv[i * vdim:(i + 1) * vdim, :]

    def queries(src, head0):
        ct, st = trig[src, :hr], trig[src, hr:]
        for j in range(GROUP // 4):
            w = wuq[pl.ds(pl.multiple_of((head0 + 4 * j) * qk, 4 * qk), 4 * qk), :]
            q = lax.dot_general(w, qlat[src], NT, preferred_element_type=f32)
            for i in range(4):
                u = 4 * j + i
                qh = q[i * qk:(i + 1) * qk]
                lo = (u % 2) * nope
                qaug[u, lo:lo + nope, :] = qh[:nope].astype(bf16)
                r1, r2 = qh[nope:nope + hr], qh[nope + hr:]
                qaug[u, 2 * nope:2 * nope + rot, :] = jnp.concatenate([r1 * ct - r2 * st, r2 * ct + r1 * st], axis=0).astype(bf16)

    def group(gi, carry):
        helping = (gi >= n_own).astype(jnp.int32)
        target = jnp.where(gi >= n_own, partner, me)
        head0 = jnp.where(gi >= n_own, ngroup - helped + gi - n_own, gi) * GROUP
        slot = lax.rem(gi, SLOTS)

        @pl.when(gi == n_own)
        def _():
            for c in query_copies(me):
                c.wait_recv()
            received(2)

            @pl.when(me == 0)
            def _():
                received(1)
                received(3)

        queries(helping, head0)
        keys_and_values(slot, head0, target)
        for u in range(GROUP):
            m_s[slot * GROUP + u] = jnp.full((1, rows), -jnp.inf, f32)
            acc[slot * GROUP + u] = jnp.zeros(acc.shape[1:], f32)
        carry = step(carry, (slot, target, (target == 0).astype(jnp.int32), gi), True)

        def previous(j, carry):
            blk = lax.rem(j + target - 1, target)

            @pl.when(gi == 0)
            def _():
                received(blk)

            keys_and_values(slot, head0, blk)
            return step(carry, (slot, blk, (j == target - 1).astype(jnp.int32), gi), False)

        carry = lax.fori_loop(0, target, previous, carry)

        @pl.when((gi == 0) & (me == 2))
        def _():
            start(query_copies(1))
            start(latent_copies(me, 1))

        return carry

    idle = (jnp.int32(SLOTS), jnp.int32(0), jnp.int32(0), jnp.int32(0))
    carry = lax.fori_loop(0, n_all, group, (idle, idle))
    carry = step(carry, None, False)
    step(carry, None, False)

    @pl.when(me == 0)
    def _():
        for t in (1, 3, 2):
            for c in latent_copies(me, t):
                c.wait_send()

    @pl.when(me == 1)
    def _():
        for t in (0, 2, 3):
            for c in latent_copies(me, t):
                c.wait_send()

    @pl.when(me == 2)
    def _():
        for t in (3, 0, 1):
            for c in latent_copies(me, t):
                c.wait_send()
        for c in query_copies(1):
            c.wait_send()

    @pl.when(me == 3)
    def _():
        for c in latent_copies(me, 0) + query_copies(0):
            c.wait_send()

    for k in range(max(HELPED)):
        @pl.when(k < helped)
        def _():
            help_copy(k).wait_send()

        @pl.when(k < given)
        def _():
            grp = n_own + k
            remote(o_help.at[k], o_nat.at[pl.ds(grp * pairs, pairs)], o_send.at[k], o_recv.at[k], me).wait_recv()
            output_copy(grp).start()

    for grp in range(ngroup):
        output_copy(grp).wait()


def layer(trig, gq, gkv, x, wdkv, wdq, wuq, wuk, wuv, scale2, heads, groups):
    rows, dim = x.shape
    rank = gkv.shape[0]
    rot = wdkv.shape[0] - rank
    qrank = wdq.shape[1]
    nope = wuk.shape[0] // heads
    vdim = wuv.shape[0] // heads
    seq = rows * groups
    vm = pl.BlockSpec(memory_space=pltpu.VMEM)
    anym = pl.BlockSpec(memory_space=pl.ANY)
    f32 = jnp.float32
    bf16 = jnp.bfloat16
    dma = pltpu.SemaphoreType.DMA
    nhelp = max(HELPED)
    return pl.pallas_call(
        functools.partial(layer_kernel, scale2=scale2, rows=rows, nope=nope, rot=rot, vdim=vdim, heads=heads, groups=groups),
        out_shape=(jax.ShapeDtypeStruct((heads // 2, rows, 2 * vdim), bf16),
                   jax.ShapeDtypeStruct((rows, rank), bf16),
                   jax.ShapeDtypeStruct((rot, rows), bf16)),
        in_specs=[vm, vm, vm] + [anym] * 6,
        out_specs=(anym, vm, vm),
        scratch_shapes=[
            pltpu.VMEM(x.shape, bf16),
            pltpu.VMEM(wdkv.shape, bf16),
            pltpu.VMEM(wdq.shape, bf16),
            pltpu.VMEM(wuq.shape, bf16),
            pltpu.VMEM(wuk.shape, bf16),
            pltpu.VMEM(wuv.shape, bf16),
            pltpu.VMEM((2, rows, qrank), bf16),
            pltpu.VMEM((2, rot, rows), f32),
            pltpu.VMEM((groups, rows, rank), bf16),
            pltpu.VMEM((groups, rot, rows), bf16),
            pltpu.VMEM((groups, rows, 128), bf16),
            pltpu.VMEM((GROUP, 256, rows), bf16),
            pltpu.VMEM((GROUP // 2, seq, 128), bf16),
            pltpu.VMEM(((SLOTS + 1) * GROUP, vdim + 16, seq), bf16),
            pltpu.VMEM((GROUP, rows, rows), f32),
            pltpu.VMEM((GROUP, 1, rows), f32),
            pltpu.VMEM((GROUP, rows, rows), bf16),
            pltpu.VMEM((GROUP, 1, rows), f32),
            pltpu.VMEM(((SLOTS + 1) * GROUP, 1, rows), f32),
            pltpu.VMEM(((SLOTS + 1) * GROUP, vdim + 16, rows), f32),
            pltpu.VMEM((heads // 2, rows, 2 * vdim), bf16),
            pltpu.VMEM((nhelp, GROUP // 2, rows, 2 * vdim), bf16),
            dma((6,)),
            dma((groups,)), dma((groups,)), dma((groups,)), dma((groups,)),
            dma, dma, dma, dma,
            dma((nhelp,)), dma((nhelp,)),
            dma((heads // GROUP,)),
        ],
        compiler_params=pltpu.CompilerParams(vmem_limit_bytes=62 * 1024 * 1024, collective_id=0, has_side_effects=True),
        cost_estimate=pl.CostEstimate(flops=40_000_000_000, bytes_accessed=40_000_000, transcendentals=30_000_000),
    )(trig, gq, gkv, x, wdkv, wdq, wuq, wuk, wuv)


def project_kernel(o_ref, w_ref, out_ref):
    o_all = jnp.concatenate([o_ref[j] for j in range(o_ref.shape[0])], axis=1)
    out_ref[...] = jnp.dot(o_all, w_ref[...], preferred_element_type=jnp.float32).astype(out_ref.dtype)


def project(o, w):
    npair, rows, width = o.shape
    dim = w.shape[1]
    tile = 512
    return pl.pallas_call(
        project_kernel,
        grid=(dim // tile,),
        in_specs=[pl.BlockSpec((npair, rows, width), lambda i: (0, 0, 0)), pl.BlockSpec((w.shape[0], tile), lambda i: (0, i))],
        out_specs=pl.BlockSpec((rows, tile), lambda i: (0, i)),
        out_shape=jax.ShapeDtypeStruct((rows, dim), jnp.bfloat16),
        compiler_params=pltpu.CompilerParams(vmem_limit_bytes=24 * 1024 * 1024),
        cost_estimate=pl.CostEstimate(flops=2 * rows * dim * w.shape[0], bytes_accessed=2 * w.size, transcendentals=0),
    )(o, w)


def solution(mesh):
    groups = mesh.shape['sp']
    tok_spec = P(('dp', 'sp'))
    rows_spec = P(('dp', 'sp'), None)
    replicated = P()

    def local_step(tok_in, tok_pos, w_dq, g_q, w_uq, w_dkv, g_kv, w_uk, w_uv, w_o):
        heads, qk_dim = w_uq.shape[1:]
        kv_rank = g_kv.shape[0]
        rot_dim = w_dkv.shape[1] - kv_rank
        v_dim = w_uv.shape[2]
        attn_scale = (0.1 * math.log(YARN_FACTOR) + 1.0) ** 2 / math.sqrt(qk_dim)
        angles = tok_pos.astype(jnp.float32)[None, :] * rope_freqs(rot_dim)[:, None]
        trig = jnp.concatenate([jnp.cos(angles), jnp.sin(angles)], axis=0)

        def flat(w):
            return jnp.transpose(w, (1, 2, 0)).reshape(-1, w.shape[0])

        o, cache_kv, cache_pe = layer(trig, g_q[None, :], g_kv[:, None], tok_in, w_dkv.T, w_dq, flat(w_uq), flat(w_uk), flat(w_uv),
                                      attn_scale * math.log2(math.e), heads, groups)
        attn_out = project(o, w_o.reshape(heads * v_dim, -1))
        return attn_out, cache_kv, cache_pe.T

    return jax.shard_map(local_step, mesh=mesh, in_specs=(rows_spec, tok_spec, replicated, replicated, replicated, replicated, replicated, replicated, replicated, replicated), out_specs=(rows_spec, rows_spec, rows_spec), check_vma=False)
```

```python
import functools
import math
import jax
import jax.numpy as jnp
from jax import lax
from jax.experimental import pallas as pl
from jax.experimental.pallas import tpu as pltpu
from jax.sharding import PartitionSpec as P

ROPE_THETA = 10000.0
YARN_FACTOR = 40.0
ORIG_CTX = 4096.0
BETA_FAST = 32.0
BETA_SLOW = 1.0
NORM_EPS = 1e-6


def rope_freqs(rot_dim):
    half_dim = rot_dim // 2
    log_base = 2.0 * math.log(ROPE_THETA)
    low_idx = max(math.floor(rot_dim * math.log(ORIG_CTX / (BETA_FAST * 2.0 * math.pi)) / log_base), 0)
    high_idx = min(math.ceil(rot_dim * math.log(ORIG_CTX / (BETA_SLOW * 2.0 * math.pi)) / log_base), half_dim - 1)
    spread = max(high_idx - low_idx, 0.001)
    freq_list = []
    for freq_idx in range(half_dim):
        base_freq = ROPE_THETA ** (-2.0 * freq_idx / rot_dim)
        ramp_val = min(max((freq_idx - low_idx) / spread, 0.0), 1.0)
        freq_list.append(base_freq / YARN_FACTOR * ramp_val + base_freq * (1.0 - ramp_val))
    return freq_list


GROUP = 8
SLOTS = 3
HELPED = (2, 1)


def layer_kernel(pos_ref, gq_ref, gkv_ref, x_hbm, wdkv_hbm, wdq_hbm, wuq_hbm, wuk_hbm, wuv_hbm,
                 o_hbm, ckv_out, cpe_out,
                 x, wdkv, wdq, wuq, wuk, wuv, qlat, trig, ckv, pet, pen, qaug, kn, vt,
                 s_buf, c_buf, p_buf, al_buf, m_s, acc, o_nat, o_help,
                 load_sem, c_send, c_recv, pe_send, pe_recv, f_send, q_send, q_recv, t_send, t_recv, o_send, o_recv, out_sem,
                 *, scale2, rows, nope, rot, vdim, heads, groups):
    f32 = jnp.float32
    bf16 = jnp.bfloat16
    NT = (((1,), (1,)), ((), ()))
    NN = (((1,), (0,)), ((), ()))
    half = rows // 2
    qk = nope + rot
    pairs = GROUP // 2
    ngroup = heads // GROUP
    me = lax.axis_index('sp')
    partner = groups - 1 - me
    given = jnp.where(me == groups - 1, HELPED[0], jnp.where(me == groups - 2, HELPED[1], 0))
    helped = jnp.where(me == 0, HELPED[0], jnp.where(me == 1, HELPED[1], 0))
    n_own = ngroup - given
    n_all = n_own + helped

    loads = [pltpu.make_async_copy(s, d, load_sem.at[i]) for i, (s, d) in enumerate(
        ((x_hbm, x), (wdkv_hbm, wdkv), (wdq_hbm, wdq), (wuq_hbm, wuq), (wuk_hbm, wuk), (wuv_hbm, wuv)))]
    for c in loads:
        c.start()
    barrier = pltpu.get_barrier_semaphore()
    for d in range(1, groups):
        pl.semaphore_signal(barrier, inc=1, device_id={'sp': lax.rem(me + d, groups)}, device_id_type=pl.DeviceIdType.MESH)

    def remote(s, d, ssem, rsem, to):
        return pltpu.make_async_remote_copy(src_ref=s, dst_ref=d, send_sem=ssem, recv_sem=rsem,
                                            device_id={'sp': to}, device_id_type=pl.DeviceIdType.MESH)

    def latent_copies(origin, to):
        return (remote(ckv.at[origin], ckv.at[origin], c_send.at[to], c_recv.at[origin], to),
                remote(pet.at[origin], pet.at[origin], pe_send.at[to], pe_recv.at[origin], to))

    def forward_copies(origin):
        to = 5 - me
        return (remote(ckv.at[origin], ckv.at[origin], f_send.at[0], c_recv.at[origin], to),
                remote(pet.at[origin], pet.at[origin], f_send.at[1], pe_recv.at[origin], to))

    def query_copies(to):
        return (remote(qlat.at[0], qlat.at[1], q_send, q_recv, to),
                remote(trig.at[0], trig.at[1], t_send, t_recv, to))

    def start(copies):
        for c in copies:
            c.start()

    def received(origin):
        for c in latent_copies(origin, me):
            c.wait_recv()
        unpack_rope(origin)

    def unpack_rope(origin):
        wide = jnp.concatenate([pet[origin].astype(f32), jnp.zeros((128 - rot, rows), f32)], axis=0)
        pen[origin] = wide.T.astype(bf16)

    hr = rot // 2
    freq_i = lax.broadcasted_iota(jnp.int32, (hr, rows), 0)
    freq = jnp.zeros((hr, rows), f32)
    for i, f in enumerate(rope_freqs(rot)):
        freq = jnp.where(freq_i == i, f, freq)
    angle = pos_ref[...].astype(f32).reshape(1, rows) * freq
    cos_t, sin_t = jnp.cos(angle), jnp.sin(angle)
    trig[0, :hr] = cos_t
    trig[0, hr:] = sin_t
    loads[0].wait()
    loads[1].wait()
    kvt = lax.dot_general(wdkv[...], x[...], NT, preferred_element_type=f32)
    rank = ckv.shape[2]
    a = kvt[:rank]
    norm = a * lax.rsqrt(jnp.sum(a * a, axis=0, keepdims=True) / rank + NORM_EPS)
    c_own = (norm.T * gkv_ref[...].reshape(1, rank)).astype(bf16)
    ckv[me] = c_own
    ckv_out[...] = c_own
    z1, z2 = kvt[rank:rank + hr], kvt[rank + hr:]
    pe_own = jnp.concatenate([z1 * cos_t - z2 * sin_t, z2 * cos_t + z1 * sin_t], axis=0).astype(bf16)
    pet[me] = pe_own
    cpe_out[...] = pe_own
    loads[2].wait()
    tile = 256
    qrank = wdq.shape[1]
    first = lax.dot_general(x[...], wdq[:, :tile], NN, preferred_element_type=f32)
    s_buf[0, :, :tile] = first
    pl.semaphore_wait(barrier, groups - 1)

    @pl.when(me == 0)
    def _():
        for t in (1, 3):
            start(latent_copies(me, t))

    @pl.when(me == 1)
    def _():
        for t in (2, 0):
            start(latent_copies(me, t))

    @pl.when(me == 2)
    def _():
        for t in (3, 0):
            start(latent_copies(me, t))

    rest = lax.dot_general(x[...], wdq[:, tile:], NN, preferred_element_type=f32)
    ql = jnp.concatenate([s_buf[0, :, :tile], rest], axis=1)
    qlat[0] = (ql * lax.rsqrt(jnp.sum(ql * ql, axis=1, keepdims=True) / qrank + NORM_EPS) * gq_ref[...].reshape(1, qrank)).astype(bf16)
    unpack_rope(me)
    qaug[...] = jnp.zeros_like(qaug)
    vt[:, vdim:, :] = jnp.ones((vt.shape[0], vt.shape[1] - vdim, vt.shape[2]), vt.dtype)
    for c in loads[3:]:
        c.wait()

    @pl.when(me == 3)
    def _():
        start(query_copies(0))
        start(latent_copies(me, 0))

    FULL = ((0, 0), (1, 0), (0, 1), (1, 1))
    OWN = ((0, 0), (0, 1), (1, 1))
    row_i = lax.broadcasted_iota(jnp.int32, (half, half), 0)
    col_i = lax.broadcasted_iota(jnp.int32, (half, half), 1)

    def cols(i):
        return slice(i * half, (i + 1) * half)

    def score_stage(u, blk, own, gi):
        tops = [None, None]

        def place(s, k, i):
            s_buf[u, cols(k), cols(i)] = s
            top = jnp.max(s, axis=0, keepdims=True)
            tops[i] = top if tops[i] is None else jnp.maximum(tops[i], top)

        def dot(k0, k1, i0, i1):
            lhs = jnp.concatenate([kn[u // 2, pl.ds(pl.multiple_of(blk * rows + k0 * half, half), (k1 - k0) * half), :],
                                   pen[blk, k0 * half:k1 * half, :]], axis=1)
            return lax.dot_general(lhs, qaug[lax.rem(gi, 2), u, :, i0 * half:i1 * half], NN, preferred_element_type=f32)

        if own:
            s = dot(0, 1, 0, 2)
            place(jnp.where(row_i <= col_i, s[:, :half], -jnp.inf), 0, 0)
            place(s[:, half:], 0, 1)
            place(jnp.where(row_i <= col_i, dot(1, 2, 1, 2), -jnp.inf), 1, 1)
            s_buf[u, cols(1), cols(0)] = jnp.full((half, half), -jnp.inf, f32)
        else:
            s = dot(0, 2, 0, 2)
            for k, i in FULL:
                place(s[cols(k), cols(i)], k, i)
        for i in range(2):
            c_buf[u, :, cols(i)] = tops[i]

    def exp_stage(u, slot):
        h = slot * GROUP + u
        m_old = m_s[h]
        m_new = jnp.maximum(m_old, c_buf[u])
        al_buf[u] = jnp.exp2((m_old - m_new) * scale2)
        m_s[h] = m_new
        for k, i in FULL:
            p_buf[u, cols(k), cols(i)] = jnp.exp2((s_buf[u, cols(k), cols(i)] - m_new[:, cols(i)]) * scale2).astype(bf16)

    def value_stage(u, slot, blk):
        h = slot * GROUP + u
        v = vt[jnp.minimum(slot, SLOTS - 1) * GROUP + u, :, pl.ds(pl.multiple_of(blk * rows, rows), rows)]
        for i in range(2):
            t = lax.dot_general(v, p_buf[u, :, cols(i)], NN, preferred_element_type=f32)
            acc[h, :, cols(i)] = t + acc[h, :, cols(i)] * al_buf[u, :, cols(i)]

    def output_copy(grp):
        return pltpu.make_async_copy(o_nat.at[pl.ds(grp * pairs, pairs)], o_hbm.at[pl.ds(grp * pairs, pairs)], out_sem.at[grp])

    def help_copy(k):
        grp = ngroup - helped + k
        return remote(o_help.at[k], o_nat.at[pl.ds(grp * pairs, pairs)], o_send.at[k], o_recv.at[k], partner)

    def finish(slot, gi):
        outs = []
        for j in range(pairs):
            t = jnp.concatenate([acc[slot * GROUP + h, :vdim, :] / acc[slot * GROUP + h, vdim:vdim + 1, :] for h in (2 * j, 2 * j + 1)], axis=0)
            outs.append(t.T.astype(bf16))
        for h in range(GROUP):
            acc[slot * GROUP + h] = jnp.zeros(acc.shape[1:], f32)

        @pl.when(gi < n_own)
        def _():
            for j in range(pairs):
                o_nat[gi * pairs + j] = outs[j]
            output_copy(gi).start()

        @pl.when(gi >= n_own)
        def _():
            for j in range(pairs):
                o_help[gi - n_own, j] = outs[j]
            help_copy(gi - n_own).start()

    def step(carry, new, own, after=None):
        (slot1, blk1, last1, gi1), (slot2, blk2, last2, gi2) = carry
        for u in range(GROUP):
            value_stage(u, slot2, blk2)
            exp_stage(u, slot1)
            if new is not None:
                score_stage(u, new[1], own, new[3])
        if after is not None:
            after()

        @pl.when(last2 == 1)
        def _():
            finish(slot2, gi2)

        return (new if new is not None else (SLOTS, 0, 0, 0)), (slot1, blk1, last1, gi1)

    def keys_and_values(slot, head0, blk):
        c = ckv[blk]
        at = pl.multiple_of(blk * rows, rows)
        for j in range(GROUP // 4):
            wk = wuk[pl.ds(pl.multiple_of((head0 + 4 * j) * nope, 4 * nope), 4 * nope), :]
            kk = lax.dot_general(c, wk, NT, preferred_element_type=f32).astype(bf16)
            kn[2 * j, pl.ds(at, rows), :] = kk[:, :128]
            kn[2 * j + 1, pl.ds(at, rows), :] = kk[:, 128:]
            wv = wuv[pl.ds(pl.multiple_of((head0 + 4 * j) * vdim, 4 * vdim), 4 * vdim), :]
            vv = lax.dot_general(wv, c, NT, preferred_element_type=f32).astype(bf16)
            for i in range(4):
                vt[slot * GROUP + 4 * j + i, :vdim, pl.ds(at, rows)] = vv[i * vdim:(i + 1) * vdim, :]

    def queries(buf, src, head0):
        ct, st = trig[src, :hr], trig[src, hr:]
        for j in range(GROUP // 4):
            w = wuq[pl.ds(pl.multiple_of((head0 + 4 * j) * qk, 4 * qk), 4 * qk), :]
            q = lax.dot_general(w, qlat[src], NT, preferred_element_type=f32)
            for i in range(4):
                u = 4 * j + i
                qh = q[i * qk:(i + 1) * qk]
                lo = (u % 2) * nope
                qaug[buf, u, lo:lo + nope, :] = qh[:nope].astype(bf16)
                r1, r2 = qh[nope:nope + hr], qh[nope + hr:]
                qaug[buf, u, 2 * nope:2 * nope + rot, :] = jnp.concatenate([r1 * ct - r2 * st, r2 * ct + r1 * st], axis=0).astype(bf16)

    def place_of(gi):
        helping = gi >= n_own
        target = jnp.where(helping, partner, me)
        head0 = jnp.where(helping, ngroup - helped + gi - n_own, gi) * GROUP
        return helping.astype(jnp.int32), target, head0, lax.rem(gi, SLOTS)

    def clear(slot):
        for u in range(GROUP):
            m_s[slot * GROUP + u] = jnp.full((1, rows), -jnp.inf, f32)

    def earlier(target, j):
        return lax.rem(j + target - 1, jnp.maximum(target, 1))

    def group(gi, carry):
        _, target, head0, slot = place_of(gi)
        gn = jnp.minimum(gi + 1, n_all - 1)
        helping_n, target_n, head_n, _ = place_of(gn)
        slot_n = lax.rem(gi + 1, SLOTS)

        @pl.when((gi == n_own - 1) & (helped > 0))
        def _():
            for c in query_copies(me):
                c.wait_recv()
            received(2)

            @pl.when(me == 0)
            def _():
                received(1)
                received(3)

        def arrived(j):
            @pl.when((gi == 0) & (j < target))
            def _():
                blk = earlier(target, j)
                received(blk)

                @pl.when((me >= 2) & (blk == 3 - me))
                def _():
                    start(forward_copies(blk))

        def next_keys(j):
            more = j < target
            keys_and_values(jnp.where(more, slot, slot_n), jnp.where(more, head0, head_n),
                            jnp.where(more, earlier(target, j), target_n))

        def after_own():
            queries(lax.rem(gi + 1, 2), helping_n, head_n)
            next_keys(0)
            clear(slot_n)

        arrived(0)
        carry = step(carry, (slot, target, (target == 0).astype(jnp.int32), gi), True, after_own)

        def previous(j, carry):
            arrived(j + 1)
            return step(carry, (slot, earlier(target, j), (j == target - 1).astype(jnp.int32), gi), False,
                        lambda: next_keys(j + 1))

        carry = lax.fori_loop(0, target, previous, carry)

        @pl.when((gi == 0) & (me == 2))
        def _():
            start(query_copies(1))
            start(latent_copies(me, 1))

        return carry

    idle = (jnp.int32(SLOTS), jnp.int32(0), jnp.int32(0), jnp.int32(0))
    acc[...] = jnp.zeros_like(acc)
    queries(0, 0, 0)
    keys_and_values(0, 0, me)
    clear(0)
    carry = lax.fori_loop(0, n_all, group, (idle, idle))
    carry = step(carry, None, False)
    step(carry, None, False)

    @pl.when(me == 0)
    def _():
        for t in (1, 3):
            for c in latent_copies(me, t):
                c.wait_send()

    @pl.when(me == 1)
    def _():
        for t in (2, 0):
            for c in latent_copies(me, t):
                c.wait_send()

    @pl.when(me == 2)
    def _():
        for t in (3, 0, 1):
            for c in latent_copies(me, t):
                c.wait_send()
        for c in forward_copies(1) + query_copies(1):
            c.wait_send()

    @pl.when(me == 3)
    def _():
        for c in latent_copies(me, 0) + forward_copies(0) + query_copies(0):
            c.wait_send()

    for k in range(max(HELPED)):
        @pl.when(k < helped)
        def _():
            help_copy(k).wait_send()

        @pl.when(k < given)
        def _():
            grp = n_own + k
            remote(o_help.at[k], o_nat.at[pl.ds(grp * pairs, pairs)], o_send.at[k], o_recv.at[k], me).wait_recv()
            output_copy(grp).start()

    for grp in range(ngroup):
        output_copy(grp).wait()


def layer(pos, gq, gkv, x, wdkv, wdq, wuq, wuk, wuv, scale2, heads, groups):
    rows, dim = x.shape
    rank = gkv.shape[0]
    rot = wdkv.shape[0] - rank
    qrank = wdq.shape[1]
    nope = wuk.shape[0] // heads
    vdim = wuv.shape[0] // heads
    seq = rows * groups
    vm = pl.BlockSpec(memory_space=pltpu.VMEM)
    anym = pl.BlockSpec(memory_space=pl.ANY)
    f32 = jnp.float32
    bf16 = jnp.bfloat16
    dma = pltpu.SemaphoreType.DMA
    nhelp = max(HELPED)
    return pl.pallas_call(
        functools.partial(layer_kernel, scale2=scale2, rows=rows, nope=nope, rot=rot, vdim=vdim, heads=heads, groups=groups),
        out_shape=(jax.ShapeDtypeStruct((heads // 2, rows, 2 * vdim), bf16),
                   jax.ShapeDtypeStruct((rows, rank), bf16),
                   jax.ShapeDtypeStruct((rot, rows), bf16)),
        in_specs=[vm, vm, vm] + [anym] * 6,
        out_specs=(anym, vm, vm),
        scratch_shapes=[
            pltpu.VMEM(x.shape, bf16),
            pltpu.VMEM(wdkv.shape, bf16),
            pltpu.VMEM(wdq.shape, bf16),
            pltpu.VMEM(wuq.shape, bf16),
            pltpu.VMEM(wuk.shape, bf16),
            pltpu.VMEM(wuv.shape, bf16),
            pltpu.VMEM((2, rows, qrank), bf16),
            pltpu.VMEM((2, rot, rows), f32),
            pltpu.VMEM((groups, rows, rank), bf16),
            pltpu.VMEM((groups, rot, rows), bf16),
            pltpu.VMEM((groups, rows, 128), bf16),
            pltpu.VMEM((2, GROUP, 256, rows), bf16),
            pltpu.VMEM((GROUP // 2, seq, 128), bf16),
            pltpu.VMEM((SLOTS * GROUP, vdim + 16, seq), bf16),
            pltpu.VMEM((GROUP, rows, rows), f32),
            pltpu.VMEM((GROUP, 1, rows), f32),
            pltpu.VMEM((GROUP, rows, rows), bf16),
            pltpu.VMEM((GROUP, 1, rows), f32),
            pltpu.VMEM(((SLOTS + 1) * GROUP, 1, rows), f32),
            pltpu.VMEM(((SLOTS + 1) * GROUP, vdim + 16, rows), f32),
            pltpu.VMEM((heads // 2, rows, 2 * vdim), bf16),
            pltpu.VMEM((nhelp, GROUP // 2, rows, 2 * vdim), bf16),
            dma((6,)),
            dma((groups,)), dma((groups,)), dma((groups,)), dma((groups,)), dma((2,)),
            dma, dma, dma, dma,
            dma((nhelp,)), dma((nhelp,)),
            dma((heads // GROUP,)),
        ],
        compiler_params=pltpu.CompilerParams(vmem_limit_bytes=62 * 1024 * 1024, collective_id=0, has_side_effects=True),
        cost_estimate=pl.CostEstimate(flops=40_000_000_000, bytes_accessed=40_000_000, transcendentals=30_000_000),
    )(pos, gq, gkv, x, wdkv, wdq, wuq, wuk, wuv)


def project_kernel(o_ref, ckv_ref, cpe_ref, w_ref, out_ref, ckv_out, cpe_out):
    @pl.when(pl.program_id(0) == 0)
    def _():
        ckv_out[...] = ckv_ref[...]
        cpe_out[...] = cpe_ref[...]

    o_all = jnp.concatenate([o_ref[j] for j in range(o_ref.shape[0])], axis=1)
    out_ref[...] = jnp.dot(o_all, w_ref[...], preferred_element_type=jnp.float32).astype(out_ref.dtype)


def project(o, ckv, cpe, w):
    npair, rows, width = o.shape
    dim = w.shape[1]
    tile = 256

    def whole(a):
        return pl.BlockSpec(a.shape, lambda i: (0,) * a.ndim)

    return pl.pallas_call(
        project_kernel,
        grid=(dim // tile,),
        in_specs=[whole(o), whole(ckv), whole(cpe), pl.BlockSpec((w.shape[0], tile), lambda i: (0, i))],
        out_specs=(pl.BlockSpec((rows, tile), lambda i: (0, i)), whole(ckv), whole(cpe)),
        out_shape=(jax.ShapeDtypeStruct((rows, dim), jnp.bfloat16), jax.ShapeDtypeStruct(ckv.shape, ckv.dtype), jax.ShapeDtypeStruct(cpe.shape, cpe.dtype)),
        compiler_params=pltpu.CompilerParams(vmem_limit_bytes=62 * 1024 * 1024),
        cost_estimate=pl.CostEstimate(flops=2 * rows * dim * w.shape[0], bytes_accessed=2 * w.size, transcendentals=0),
    )(o, ckv, cpe, w)


def solution(mesh):
    groups = mesh.shape['sp']
    tok_spec = P(('dp', 'sp'))
    rows_spec = P(('dp', 'sp'), None)
    replicated = P()

    def local_step(tok_in, tok_pos, w_dq, g_q, w_uq, w_dkv, g_kv, w_uk, w_uv, w_o):
        heads, qk_dim = w_uq.shape[1:]
        kv_rank = g_kv.shape[0]
        rot_dim = w_dkv.shape[1] - kv_rank
        v_dim = w_uv.shape[2]
        attn_scale = (0.1 * math.log(YARN_FACTOR) + 1.0) ** 2 / math.sqrt(qk_dim)
        def flat(w):
            return jnp.transpose(w, (1, 2, 0)).reshape(-1, w.shape[0])

        o, ckv, cpe = layer(tok_pos, g_q, g_kv, tok_in, w_dkv.T, w_dq, flat(w_uq), flat(w_uk), flat(w_uv),
                                      attn_scale * math.log2(math.e), heads, groups)
        attn_out, cache_kv, cache_pe = project(o, ckv, cpe, w_o.reshape(heads * v_dim, -1))
        return attn_out, cache_kv, cache_pe.T

    return jax.shard_map(local_step, mesh=mesh, in_specs=(rows_spec, tok_spec, replicated, replicated, replicated, replicated, replicated, replicated, replicated, replicated), out_specs=(rows_spec, rows_spec, rows_spec), check_vma=False)
```

```python
import functools
import math
import jax
import jax.numpy as jnp
from jax import lax
from jax.experimental import pallas as pl
from jax.experimental.pallas import tpu as pltpu
from jax.sharding import PartitionSpec as P

ROPE_THETA = 10000.0
YARN_FACTOR = 40.0
ORIG_CTX = 4096.0
BETA_FAST = 32.0
BETA_SLOW = 1.0
NORM_EPS = 1e-6


def rope_freqs(rot_dim):
    half_dim = rot_dim // 2
    log_base = 2.0 * math.log(ROPE_THETA)
    low_idx = max(math.floor(rot_dim * math.log(ORIG_CTX / (BETA_FAST * 2.0 * math.pi)) / log_base), 0)
    high_idx = min(math.ceil(rot_dim * math.log(ORIG_CTX / (BETA_SLOW * 2.0 * math.pi)) / log_base), half_dim - 1)
    spread = max(high_idx - low_idx, 0.001)
    freq_list = []
    for freq_idx in range(half_dim):
        base_freq = ROPE_THETA ** (-2.0 * freq_idx / rot_dim)
        ramp_val = min(max((freq_idx - low_idx) / spread, 0.0), 1.0)
        freq_list.append(base_freq / YARN_FACTOR * ramp_val + base_freq * (1.0 - ramp_val))
    return freq_list


GROUP = 8
SLOTS = 3
MOST_HELPED = 2


def layer_kernel(pos_ref, gq_ref, gkv_ref, x_hbm, wdkv_hbm, wdq_hbm, wuq_hbm, wuk_hbm, wuv_hbm,
                 o_hbm, ckv_out, cpe_out,
                 x, wdkv, wdq, wuq, wuk, wuv, qlat, trig, ckv, pet, pen, qaug, kn, vt,
                 s_buf, c_buf, p_buf, al_buf, m_s, acc, o_nat, o_help,
                 load_sem, c_send, c_recv, pe_send, pe_recv, f_send, q_send, q_recv, t_send, t_recv, o_send, o_recv, out_sem,
                 *, scale2, rows, nope, rot, vdim, heads, groups):
    f32 = jnp.float32
    bf16 = jnp.bfloat16
    NT = (((1,), (1,)), ((), ()))
    NN = (((1,), (0,)), ((), ()))
    half = rows // 2
    qk = nope + rot
    pairs = GROUP // 2
    ngroup = heads // GROUP
    me = lax.axis_index('sp')
    given = jnp.where(me == 3, 2, jnp.where(me == 2, 1, 0))
    helped = jnp.where(me == 0, 2, jnp.where(me == 3, 1, 0))
    partner = jnp.where(me == 0, 3, 2)
    n_own = ngroup - given
    n_all = n_own + helped

    loads = [pltpu.make_async_copy(s, d, load_sem.at[i]) for i, (s, d) in enumerate(
        ((x_hbm, x), (wdkv_hbm, wdkv), (wdq_hbm, wdq), (wuq_hbm, wuq), (wuk_hbm, wuk), (wuv_hbm, wuv)))]
    for c in loads:
        c.start()
    barrier = pltpu.get_barrier_semaphore()
    for d in range(1, groups):
        pl.semaphore_signal(barrier, inc=1, device_id={'sp': lax.rem(me + d, groups)}, device_id_type=pl.DeviceIdType.MESH)

    def remote(s, d, ssem, rsem, to):
        return pltpu.make_async_remote_copy(src_ref=s, dst_ref=d, send_sem=ssem, recv_sem=rsem,
                                            device_id={'sp': to}, device_id_type=pl.DeviceIdType.MESH)

    def latent_copies(origin, to):
        return (remote(ckv.at[origin], ckv.at[origin], c_send.at[to], c_recv.at[origin], to),
                remote(pet.at[origin], pet.at[origin], pe_send.at[to], pe_recv.at[origin], to))

    def forward_copies(origin):
        to = 5 - me
        return (remote(ckv.at[origin], ckv.at[origin], f_send.at[0], c_recv.at[origin], to),
                remote(pet.at[origin], pet.at[origin], f_send.at[1], pe_recv.at[origin], to))

    def query_copies(to):
        return (remote(qlat.at[0], qlat.at[1], q_send, q_recv, to),
                remote(trig.at[0], trig.at[1], t_send, t_recv, to))

    def start(copies):
        for c in copies:
            c.start()

    def received(origin):
        for c in latent_copies(origin, me):
            c.wait_recv()
        unpack_rope(origin)

    def unpack_rope(origin):
        wide = jnp.concatenate([pet[origin].astype(f32), jnp.zeros((128 - rot, rows), f32)], axis=0)
        pen[origin] = wide.T.astype(bf16)

    hr = rot // 2
    freq_i = lax.broadcasted_iota(jnp.int32, (hr, rows), 0)
    freq = jnp.zeros((hr, rows), f32)
    for i, f in enumerate(rope_freqs(rot)):
        freq = jnp.where(freq_i == i, f, freq)
    angle = pos_ref[...].astype(f32).reshape(1, rows) * freq
    cos_t, sin_t = jnp.cos(angle), jnp.sin(angle)
    trig[0, :hr] = cos_t
    trig[0, hr:] = sin_t
    loads[0].wait()
    loads[1].wait()
    kvt = lax.dot_general(wdkv[...], x[...], NT, preferred_element_type=f32)
    rank = ckv.shape[2]
    a = kvt[:rank]
    norm = a * lax.rsqrt(jnp.sum(a * a, axis=0, keepdims=True) / rank + NORM_EPS)
    c_own = (norm.T * gkv_ref[...].reshape(1, rank)).astype(bf16)
    ckv[me] = c_own
    ckv_out[...] = c_own
    z1, z2 = kvt[rank:rank + hr], kvt[rank + hr:]
    pe_own = jnp.concatenate([z1 * cos_t - z2 * sin_t, z2 * cos_t + z1 * sin_t], axis=0).astype(bf16)
    pet[me] = pe_own
    cpe_out[...] = pe_own
    loads[2].wait()
    tile = 256
    qrank = wdq.shape[1]
    first = lax.dot_general(x[...], wdq[:, :tile], NN, preferred_element_type=f32)
    s_buf[0, :, :tile] = first
    pl.semaphore_wait(barrier, groups - 1)

    @pl.when(me == 0)
    def _():
        for t in (1, 3):
            start(latent_copies(me, t))

    @pl.when(me == 1)
    def _():
        for t in (2, 0):
            start(latent_copies(me, t))

    @pl.when(me == 2)
    def _():
        start(latent_copies(me, 3))

    rest = lax.dot_general(x[...], wdq[:, tile:], NN, preferred_element_type=f32)
    ql = jnp.concatenate([s_buf[0, :, :tile], rest], axis=1)
    qlat[0] = (ql * lax.rsqrt(jnp.sum(ql * ql, axis=1, keepdims=True) / qrank + NORM_EPS) * gq_ref[...].reshape(1, qrank)).astype(bf16)
    unpack_rope(me)
    qaug[...] = jnp.zeros_like(qaug)
    vt[:, vdim:, :] = jnp.ones((vt.shape[0], vt.shape[1] - vdim, vt.shape[2]), vt.dtype)
    for c in loads[3:]:
        c.wait()

    @pl.when(me == 2)
    def _():
        start(query_copies(3))

    @pl.when(me == 3)
    def _():
        start(query_copies(0))
        start(latent_copies(me, 0))

    FULL = ((0, 0), (1, 0), (0, 1), (1, 1))
    OWN = ((0, 0), (0, 1), (1, 1))
    row_i = lax.broadcasted_iota(jnp.int32, (half, half), 0)
    col_i = lax.broadcasted_iota(jnp.int32, (half, half), 1)

    def cols(i):
        return slice(i * half, (i + 1) * half)

    def score_stage(u, blk, own, gi):
        tops = [None, None]

        def place(s, k, i):
            s_buf[u, cols(k), cols(i)] = s
            top = jnp.max(s, axis=0, keepdims=True)
            tops[i] = top if tops[i] is None else jnp.maximum(tops[i], top)

        def dot(k0, k1, i0, i1):
            lhs = jnp.concatenate([kn[u // 2, pl.ds(pl.multiple_of(blk * rows + k0 * half, half), (k1 - k0) * half), :],
                                   pen[blk, k0 * half:k1 * half, :]], axis=1)
            return lax.dot_general(lhs, qaug[lax.rem(gi, 2), u, :, i0 * half:i1 * half], NN, preferred_element_type=f32)

        if own:
            s = dot(0, 1, 0, 2)
            place(jnp.where(row_i <= col_i, s[:, :half], -jnp.inf), 0, 0)
            place(s[:, half:], 0, 1)
            place(jnp.where(row_i <= col_i, dot(1, 2, 1, 2), -jnp.inf), 1, 1)
            s_buf[u, cols(1), cols(0)] = jnp.full((half, half), -jnp.inf, f32)
        else:
            s = dot(0, 2, 0, 2)
            for k, i in FULL:
                place(s[cols(k), cols(i)], k, i)
        for i in range(2):
            c_buf[u, :, cols(i)] = tops[i]

    def exp_stage(u, slot):
        h = slot * GROUP + u
        m_old = m_s[h]
        m_new = jnp.maximum(m_old, c_buf[u])
        al_buf[u] = jnp.exp2((m_old - m_new) * scale2)
        m_s[h] = m_new
        for k, i in FULL:
            p_buf[u, cols(k), cols(i)] = jnp.exp2((s_buf[u, cols(k), cols(i)] - m_new[:, cols(i)]) * scale2).astype(bf16)

    def value_stage(u, slot, blk):
        h = slot * GROUP + u
        v = vt[jnp.minimum(slot, SLOTS - 1) * GROUP + u, :, pl.ds(pl.multiple_of(blk * rows, rows), rows)]
        for i in range(2):
            t = lax.dot_general(v, p_buf[u, :, cols(i)], NN, preferred_element_type=f32)
            acc[h, :, cols(i)] = t + acc[h, :, cols(i)] * al_buf[u, :, cols(i)]

    def place_of(gi):
        helping = (gi >= n_own - 1) & (gi < n_own - 1 + helped)
        target = jnp.where(helping, partner, me)
        grp = jnp.where(helping, ngroup - helped + gi - n_own + 1, jnp.minimum(gi, n_own - 1))
        return helping, target, grp, lax.rem(gi, SLOTS)

    def output_copy(grp):
        return pltpu.make_async_copy(o_nat.at[pl.ds(grp * pairs, pairs)], o_hbm.at[pl.ds(grp * pairs, pairs)], out_sem.at[grp])

    def help_copy(k, to):
        grp = ngroup - helped + k
        return remote(o_help.at[k], o_nat.at[pl.ds(grp * pairs, pairs)], o_send.at[k], o_recv.at[grp], to)

    def finish(slot, gi):
        outs = []
        for j in range(pairs):
            t = jnp.concatenate([acc[slot * GROUP + h, :vdim, :] / acc[slot * GROUP + h, vdim:vdim + 1, :] for h in (2 * j, 2 * j + 1)], axis=0)
            outs.append(t.T.astype(bf16))
        for h in range(GROUP):
            acc[slot * GROUP + h] = jnp.zeros(acc.shape[1:], f32)

        helping, _, grp, _ = place_of(gi)

        @pl.when(jnp.logical_not(helping))
        def _():
            for j in range(pairs):
                o_nat[grp * pairs + j] = outs[j]
            output_copy(grp).start()

        @pl.when(helping)
        def _():
            k = gi - n_own + 1
            for j in range(pairs):
                o_help[k, j] = outs[j]
            help_copy(k, partner).start()

    def step(carry, new, own, after=None):
        (slot1, blk1, last1, gi1), (slot2, blk2, last2, gi2) = carry
        for u in range(GROUP):
            value_stage(u, slot2, blk2)
            exp_stage(u, slot1)
            if new is not None:
                score_stage(u, new[1], own, new[3])
        if after is not None:
            after()

        @pl.when(last2 == 1)
        def _():
            finish(slot2, gi2)

        return (new if new is not None else (SLOTS, 0, 0, 0)), (slot1, blk1, last1, gi1)

    def keys_and_values(slot, head0, blk):
        c = ckv[blk]
        at = pl.multiple_of(blk * rows, rows)
        for j in range(GROUP // 4):
            wk = wuk[pl.ds(pl.multiple_of((head0 + 4 * j) * nope, 4 * nope), 4 * nope), :]
            kk = lax.dot_general(c, wk, NT, preferred_element_type=f32).astype(bf16)
            kn[2 * j, pl.ds(at, rows), :] = kk[:, :128]
            kn[2 * j + 1, pl.ds(at, rows), :] = kk[:, 128:]
            wv = wuv[pl.ds(pl.multiple_of((head0 + 4 * j) * vdim, 4 * vdim), 4 * vdim), :]
            vv = lax.dot_general(wv, c, NT, preferred_element_type=f32).astype(bf16)
            for i in range(4):
                vt[slot * GROUP + 4 * j + i, :vdim, pl.ds(at, rows)] = vv[i * vdim:(i + 1) * vdim, :]

    def queries(buf, src, head0):
        ct, st = trig[src, :hr], trig[src, hr:]
        for j in range(GROUP // 4):
            w = wuq[pl.ds(pl.multiple_of((head0 + 4 * j) * qk, 4 * qk), 4 * qk), :]
            q = lax.dot_general(w, qlat[src], NT, preferred_element_type=f32)
            for i in range(4):
                u = 4 * j + i
                qh = q[i * qk:(i + 1) * qk]
                lo = (u % 2) * nope
                qaug[buf, u, lo:lo + nope, :] = qh[:nope].astype(bf16)
                r1, r2 = qh[nope:nope + hr], qh[nope + hr:]
                qaug[buf, u, 2 * nope:2 * nope + rot, :] = jnp.concatenate([r1 * ct - r2 * st, r2 * ct + r1 * st], axis=0).astype(bf16)

    def clear(slot):
        for u in range(GROUP):
            m_s[slot * GROUP + u] = jnp.full((1, rows), -jnp.inf, f32)

    def earlier(target, j):
        return lax.rem(j + target - 1, jnp.maximum(target, 1))

    def group(gi, carry):
        _, target, grp, slot = place_of(gi)
        gn = jnp.minimum(gi + 1, n_all - 1)
        helping_n, target_n, grp_n, _ = place_of(gn)
        slot_n = lax.rem(gi + 1, SLOTS)
        head0, head_n = grp * GROUP, grp_n * GROUP

        @pl.when((gi == n_own - 2) & (helped > 0))
        def _():
            for c in query_copies(me):
                c.wait_recv()

        @pl.when((gi == n_own - 2) & (me == 0))
        def _():
            received(3)

        @pl.when((gi == n_own - 1) & (me == 0))
        def _():
            received(1)
            received(2)

        def arrived(j):
            @pl.when((gi == 0) & (j < target))
            def _():
                blk = earlier(target, j)
                received(blk)

                @pl.when((me >= 2) & (blk == 3 - me))
                def _():
                    start(forward_copies(blk))

        def next_keys(j):
            more = j < target
            keys_and_values(jnp.where(more, slot, slot_n), jnp.where(more, head0, head_n),
                            jnp.where(more, earlier(target, j), target_n))

        def after_own():
            queries(lax.rem(gi + 1, 2), helping_n.astype(jnp.int32), head_n)
            next_keys(0)
            clear(slot_n)

        arrived(0)
        carry = step(carry, (slot, target, (target == 0).astype(jnp.int32), gi), True, after_own)

        def previous(j, carry):
            arrived(j + 1)
            return step(carry, (slot, earlier(target, j), (j == target - 1).astype(jnp.int32), gi), False,
                        lambda: next_keys(j + 1))

        @pl.when((gi == 0) & (me == 2))
        def _():
            start(latent_copies(me, 0))

        carry = lax.fori_loop(0, target, previous, carry)

        return carry

    idle = (jnp.int32(SLOTS), jnp.int32(0), jnp.int32(0), jnp.int32(0))
    acc[...] = jnp.zeros_like(acc)
    queries(0, 0, 0)
    keys_and_values(0, 0, me)
    clear(0)
    carry = lax.fori_loop(0, n_all, group, (idle, idle))
    carry = step(carry, None, False)
    step(carry, None, False)

    def sent(copies):
        for c in copies:
            c.wait_send()

    @pl.when(me == 0)
    def _():
        sent(latent_copies(me, 1) + latent_copies(me, 3))

    @pl.when(me == 1)
    def _():
        sent(latent_copies(me, 2) + latent_copies(me, 0))

    @pl.when(me == 2)
    def _():
        sent(latent_copies(me, 3) + latent_copies(me, 0) + forward_copies(1) + query_copies(3))

    @pl.when(me == 3)
    def _():
        sent(latent_copies(me, 0) + forward_copies(0) + query_copies(0))

    for k in range(MOST_HELPED):
        @pl.when(k < helped)
        def _():
            help_copy(k, partner).wait_send()

        @pl.when(k < given)
        def _():
            grp = n_own + k
            remote(o_help.at[k], o_nat.at[pl.ds(grp * pairs, pairs)], o_send.at[k], o_recv.at[grp], me).wait_recv()
            output_copy(grp).start()

    for grp in range(ngroup):
        output_copy(grp).wait()


def layer(pos, gq, gkv, x, wdkv, wdq, wuq, wuk, wuv, scale2, heads, groups):
    rows, dim = x.shape
    rank = gkv.shape[0]
    rot = wdkv.shape[0] - rank
    qrank = wdq.shape[1]
    nope = wuk.shape[0] // heads
    vdim = wuv.shape[0] // heads
    seq = rows * groups
    vm = pl.BlockSpec(memory_space=pltpu.VMEM)
    anym = pl.BlockSpec(memory_space=pl.ANY)
    f32 = jnp.float32
    bf16 = jnp.bfloat16
    dma = pltpu.SemaphoreType.DMA
    nhelp = MOST_HELPED
    return pl.pallas_call(
        functools.partial(layer_kernel, scale2=scale2, rows=rows, nope=nope, rot=rot, vdim=vdim, heads=heads, groups=groups),
        out_shape=(jax.ShapeDtypeStruct((heads // 2, rows, 2 * vdim), bf16),
                   jax.ShapeDtypeStruct((rows, rank), bf16),
                   jax.ShapeDtypeStruct((rot, rows), bf16)),
        in_specs=[vm, vm, vm] + [anym] * 6,
        out_specs=(anym, vm, vm),
        scratch_shapes=[
            pltpu.VMEM(x.shape, bf16),
            pltpu.VMEM(wdkv.shape, bf16),
            pltpu.VMEM(wdq.shape, bf16),
            pltpu.VMEM(wuq.shape, bf16),
            pltpu.VMEM(wuk.shape, bf16),
            pltpu.VMEM(wuv.shape, bf16),
            pltpu.VMEM((2, rows, qrank), bf16),
            pltpu.VMEM((2, rot, rows), f32),
            pltpu.VMEM((groups, rows, rank), bf16),
            pltpu.VMEM((groups, rot, rows), bf16),
            pltpu.VMEM((groups, rows, 128), bf16),
            pltpu.VMEM((2, GROUP, 256, rows), bf16),
            pltpu.VMEM((GROUP // 2, seq, 128), bf16),
            pltpu.VMEM((SLOTS * GROUP, vdim + 16, seq), bf16),
            pltpu.VMEM((GROUP, rows, rows), f32),
            pltpu.VMEM((GROUP, 1, rows), f32),
            pltpu.VMEM((GROUP, rows, rows), bf16),
            pltpu.VMEM((GROUP, 1, rows), f32),
            pltpu.VMEM(((SLOTS + 1) * GROUP, 1, rows), f32),
            pltpu.VMEM(((SLOTS + 1) * GROUP, vdim + 16, rows), f32),
            pltpu.VMEM((heads // 2, rows, 2 * vdim), bf16),
            pltpu.VMEM((nhelp, GROUP // 2, rows, 2 * vdim), bf16),
            dma((6,)),
            dma((groups,)), dma((groups,)), dma((groups,)), dma((groups,)), dma((2,)),
            dma, dma, dma, dma,
            dma((nhelp,)), dma((heads // GROUP,)),
            dma((heads // GROUP,)),
        ],
        compiler_params=pltpu.CompilerParams(vmem_limit_bytes=62 * 1024 * 1024, collective_id=0, has_side_effects=True),
        cost_estimate=pl.CostEstimate(flops=40_000_000_000, bytes_accessed=40_000_000, transcendentals=30_000_000),
    )(pos, gq, gkv, x, wdkv, wdq, wuq, wuk, wuv)


def project_kernel(o_ref, ckv_ref, cpe_ref, w_ref, out_ref, ckv_out, cpe_out):
    @pl.when(pl.program_id(0) == 0)
    def _():
        ckv_out[...] = ckv_ref[...]
        cpe_out[...] = cpe_ref[...]

    o_all = jnp.concatenate([o_ref[j] for j in range(o_ref.shape[0])], axis=1)
    out_ref[...] = jnp.dot(o_all, w_ref[...], preferred_element_type=jnp.float32).astype(out_ref.dtype)


def project(o, ckv, cpe, w):
    npair, rows, width = o.shape
    dim = w.shape[1]
    tile = 512

    def whole(a):
        return pl.BlockSpec(a.shape, lambda i: (0,) * a.ndim)

    return pl.pallas_call(
        project_kernel,
        grid=(dim // tile,),
        in_specs=[whole(o), whole(ckv), whole(cpe), pl.BlockSpec((w.shape[0], tile), lambda i: (0, i))],
        out_specs=(pl.BlockSpec((rows, tile), lambda i: (0, i)), whole(ckv), whole(cpe)),
        out_shape=(jax.ShapeDtypeStruct((rows, dim), jnp.bfloat16), jax.ShapeDtypeStruct(ckv.shape, ckv.dtype), jax.ShapeDtypeStruct(cpe.shape, cpe.dtype)),
        compiler_params=pltpu.CompilerParams(vmem_limit_bytes=62 * 1024 * 1024),
        cost_estimate=pl.CostEstimate(flops=2 * rows * dim * w.shape[0], bytes_accessed=2 * w.size, transcendentals=0),
    )(o, ckv, cpe, w)


def solution(mesh):
    groups = mesh.shape['sp']
    tok_spec = P(('dp', 'sp'))
    rows_spec = P(('dp', 'sp'), None)
    replicated = P()

    def local_step(tok_in, tok_pos, w_dq, g_q, w_uq, w_dkv, g_kv, w_uk, w_uv, w_o):
        heads, qk_dim = w_uq.shape[1:]
        kv_rank = g_kv.shape[0]
        rot_dim = w_dkv.shape[1] - kv_rank
        v_dim = w_uv.shape[2]
        attn_scale = (0.1 * math.log(YARN_FACTOR) + 1.0) ** 2 / math.sqrt(qk_dim)
        def flat(w):
            return jnp.transpose(w, (1, 2, 0)).reshape(-1, w.shape[0])

        o, ckv, cpe = layer(tok_pos, g_q, g_kv, tok_in, w_dkv.T, w_dq, flat(w_uq), flat(w_uk), flat(w_uv),
                                      attn_scale * math.log2(math.e), heads, groups)
        attn_out, cache_kv, cache_pe = project(o, ckv, cpe, w_o.reshape(heads * v_dim, -1))
        return attn_out, cache_kv, cache_pe.T

    return jax.shard_map(local_step, mesh=mesh, in_specs=(rows_spec, tok_spec, replicated, replicated, replicated, replicated, replicated, replicated, replicated, replicated), out_specs=(rows_spec, rows_spec, rows_spec), check_vma=False)
```

```python
import functools
import math
import jax
import jax.numpy as jnp
from jax import lax
from jax.experimental import pallas as pl
from jax.experimental.pallas import tpu as pltpu
from jax.sharding import PartitionSpec as P

ROPE_THETA = 10000.0
YARN_FACTOR = 40.0
ORIG_CTX = 4096.0
BETA_FAST = 32.0
BETA_SLOW = 1.0
NORM_EPS = 1e-6


def rope_freqs(rot_dim):
    half_dim = rot_dim // 2
    log_base = 2.0 * math.log(ROPE_THETA)
    low_idx = max(math.floor(rot_dim * math.log(ORIG_CTX / (BETA_FAST * 2.0 * math.pi)) / log_base), 0)
    high_idx = min(math.ceil(rot_dim * math.log(ORIG_CTX / (BETA_SLOW * 2.0 * math.pi)) / log_base), half_dim - 1)
    spread = max(high_idx - low_idx, 0.001)
    freq_list = []
    for freq_idx in range(half_dim):
        base_freq = ROPE_THETA ** (-2.0 * freq_idx / rot_dim)
        ramp_val = min(max((freq_idx - low_idx) / spread, 0.0), 1.0)
        freq_list.append(base_freq / YARN_FACTOR * ramp_val + base_freq * (1.0 - ramp_val))
    return freq_list


GROUP = 8
SLOTS = 3
MOST_HELPED = 2


def layer_kernel(pos_ref, gq_ref, gkv_ref, x_hbm, wdkv_hbm, wdq_hbm, wuq_hbm, wuk_hbm, wuv_hbm,
                 o_hbm, ckv_out, cpe_out,
                 x, wdkv, wdq, wuq, wuk, wuv, qlat, trig, ckv, pet, pen, qaug, kn, vt,
                 s_buf, c_buf, p_buf, al_buf, m_s, acc, o_nat, o_help,
                 load_sem, c_send, c_recv, pe_send, pe_recv, f_send, q_send, q_recv, t_send, t_recv, o_send, o_recv, out_sem,
                 *, scale2, rows, nope, rot, vdim, heads, groups):
    f32 = jnp.float32
    bf16 = jnp.bfloat16
    NT = (((1,), (1,)), ((), ()))
    NN = (((1,), (0,)), ((), ()))
    half = rows // 2
    qk = nope + rot
    pairs = GROUP // 2
    ngroup = heads // GROUP
    me = lax.axis_index('sp')
    given = jnp.where(me == 3, 2, jnp.where(me == 2, 1, 0))
    helped = jnp.where(me == 0, 2, jnp.where(me == 3, 1, 0))
    partner = jnp.where(me == 0, 3, 2)
    n_own = ngroup - given
    n_all = n_own + helped

    loads = [pltpu.make_async_copy(s, d, load_sem.at[i]) for i, (s, d) in enumerate(
        ((x_hbm, x), (wdkv_hbm, wdkv), (wdq_hbm, wdq), (wuq_hbm, wuq), (wuk_hbm, wuk), (wuv_hbm, wuv)))]
    for c in loads:
        c.start()
    barrier = pltpu.get_barrier_semaphore()
    for d in range(1, groups):
        pl.semaphore_signal(barrier, inc=1, device_id={'sp': lax.rem(me + d, groups)}, device_id_type=pl.DeviceIdType.MESH)

    def remote(s, d, ssem, rsem, to):
        return pltpu.make_async_remote_copy(src_ref=s, dst_ref=d, send_sem=ssem, recv_sem=rsem,
                                            device_id={'sp': to}, device_id_type=pl.DeviceIdType.MESH)

    def latent_copies(origin, to):
        return (remote(ckv.at[origin], ckv.at[origin], c_send.at[to], c_recv.at[origin], to),
                remote(pet.at[origin], pet.at[origin], pe_send.at[to], pe_recv.at[origin], to))

    def forward_copies(origin):
        to = 5 - me
        return (remote(ckv.at[origin], ckv.at[origin], f_send.at[0], c_recv.at[origin], to),
                remote(pet.at[origin], pet.at[origin], f_send.at[1], pe_recv.at[origin], to))

    def query_copies(to):
        return (remote(qlat.at[0], qlat.at[1], q_send.at[0], q_recv.at[0], to),
                remote(trig.at[0], trig.at[1], t_send, t_recv, to))

    def query_halves():
        top, low = pl.ds(0, half), pl.ds(half, half)
        return (remote(qlat.at[0, low], qlat.at[1, low], q_send.at[1], q_recv.at[1], 2),
                remote(trig.at[0], trig.at[1], t_send, t_recv, 0),
                remote(qlat.at[0, top], qlat.at[1, top], q_send.at[0], q_recv.at[0], 0))

    def query_relay():
        low = pl.ds(half, half)
        return remote(qlat.at[1, low], qlat.at[1, low], q_send.at[2], q_recv.at[2], 0)

    def start(copies):
        for c in copies:
            c.start()

    def received(origin):
        for c in latent_copies(origin, me):
            c.wait_recv()
        unpack_rope(origin)

    def unpack_rope(origin):
        wide = jnp.concatenate([pet[origin].astype(f32), jnp.zeros((128 - rot, rows), f32)], axis=0)
        pen[origin] = wide.T.astype(bf16)

    hr = rot // 2
    freq_i = lax.broadcasted_iota(jnp.int32, (hr, rows), 0)
    freq = jnp.zeros((hr, rows), f32)
    for i, f in enumerate(rope_freqs(rot)):
        freq = jnp.where(freq_i == i, f, freq)
    angle = pos_ref[...].astype(f32).reshape(1, rows) * freq
    cos_t, sin_t = jnp.cos(angle), jnp.sin(angle)
    trig[0, :hr] = cos_t
    trig[0, hr:] = sin_t
    loads[0].wait()
    loads[1].wait()
    kvt = lax.dot_general(wdkv[...], x[...], NT, preferred_element_type=f32)
    rank = ckv.shape[2]
    a = kvt[:rank]
    norm = a * lax.rsqrt(jnp.sum(a * a, axis=0, keepdims=True) / rank + NORM_EPS)
    c_own = (norm.T * gkv_ref[...].reshape(1, rank)).astype(bf16)
    ckv[me] = c_own
    ckv_out[...] = c_own
    z1, z2 = kvt[rank:rank + hr], kvt[rank + hr:]
    pe_own = jnp.concatenate([z1 * cos_t - z2 * sin_t, z2 * cos_t + z1 * sin_t], axis=0).astype(bf16)
    pet[me] = pe_own
    cpe_out[...] = pe_own
    loads[2].wait()
    tile = 256
    qrank = wdq.shape[1]
    first = lax.dot_general(x[...], wdq[:, :tile], NN, preferred_element_type=f32)
    s_buf[0, :, :tile] = first
    pl.semaphore_wait(barrier, groups - 1)

    @pl.when(me == 0)
    def _():
        for t in (1, 3):
            start(latent_copies(me, t))

    @pl.when(me == 1)
    def _():
        for t in (2, 0):
            start(latent_copies(me, t))

    @pl.when(me == 2)
    def _():
        start(latent_copies(me, 3))

    rest = lax.dot_general(x[...], wdq[:, tile:], NN, preferred_element_type=f32)
    ql = jnp.concatenate([s_buf[0, :, :tile], rest], axis=1)
    qlat[0] = (ql * lax.rsqrt(jnp.sum(ql * ql, axis=1, keepdims=True) / qrank + NORM_EPS) * gq_ref[...].reshape(1, qrank)).astype(bf16)
    unpack_rope(me)
    qaug[...] = jnp.zeros_like(qaug)
    vt[:, vdim:, :] = jnp.ones((vt.shape[0], vt.shape[1] - vdim, vt.shape[2]), vt.dtype)
    for c in loads[3:]:
        c.wait()

    @pl.when(me == 2)
    def _():
        start(query_copies(3))

    @pl.when(me == 3)
    def _():
        start(query_halves())
        start(latent_copies(me, 0))

    FULL = ((0, 0), (1, 0), (0, 1), (1, 1))
    OWN = ((0, 0), (0, 1), (1, 1))
    row_i = lax.broadcasted_iota(jnp.int32, (half, half), 0)
    col_i = lax.broadcasted_iota(jnp.int32, (half, half), 1)

    def cols(i):
        return slice(i * half, (i + 1) * half)

    def score_stage(u, blk, own, gi):
        tops = [None, None]

        def place(s, k, i):
            s_buf[u, cols(k), cols(i)] = s
            top = jnp.max(s, axis=0, keepdims=True)
            tops[i] = top if tops[i] is None else jnp.maximum(tops[i], top)

        def dot(k0, k1, i0, i1):
            lhs = jnp.concatenate([kn[u // 2, pl.ds(pl.multiple_of(blk * rows + k0 * half, half), (k1 - k0) * half), :],
                                   pen[blk, k0 * half:k1 * half, :]], axis=1)
            return lax.dot_general(lhs, qaug[lax.rem(gi, 2), u, :, i0 * half:i1 * half], NN, preferred_element_type=f32)

        if own:
            s = dot(0, 1, 0, 2)
            place(jnp.where(row_i <= col_i, s[:, :half], -jnp.inf), 0, 0)
            place(s[:, half:], 0, 1)
            place(jnp.where(row_i <= col_i, dot(1, 2, 1, 2), -jnp.inf), 1, 1)
            s_buf[u, cols(1), cols(0)] = jnp.full((half, half), -jnp.inf, f32)
        else:
            s = dot(0, 2, 0, 2)
            for k, i in FULL:
                place(s[cols(k), cols(i)], k, i)
        for i in range(2):
            c_buf[u, :, cols(i)] = tops[i]

    def exp_stage(u, slot):
        h = slot * GROUP + u
        m_old = m_s[h]
        m_new = jnp.maximum(m_old, c_buf[u])
        al_buf[u] = jnp.exp2((m_old - m_new) * scale2)
        m_s[h] = m_new
        for k, i in FULL:
            p_buf[u, cols(k), cols(i)] = jnp.exp2((s_buf[u, cols(k), cols(i)] - m_new[:, cols(i)]) * scale2).astype(bf16)

    def value_stage(u, slot, blk):
        h = slot * GROUP + u
        v = vt[jnp.minimum(slot, SLOTS - 1) * GROUP + u, :, pl.ds(pl.multiple_of(blk * rows, rows), rows)]
        for i in range(2):
            t = lax.dot_general(v, p_buf[u, :, cols(i)], NN, preferred_element_type=f32)
            acc[h, :, cols(i)] = t + acc[h, :, cols(i)] * al_buf[u, :, cols(i)]

    def place_of(gi):
        helping = (gi >= n_own - 1) & (gi < n_own - 1 + helped)
        target = jnp.where(helping, partner, me)
        grp = jnp.where(helping, ngroup - helped + gi - n_own + 1, jnp.minimum(gi, n_own - 1))
        return helping, target, grp, lax.rem(gi, SLOTS)

    def output_copy(grp):
        return pltpu.make_async_copy(o_nat.at[pl.ds(grp * pairs, pairs)], o_hbm.at[pl.ds(grp * pairs, pairs)], out_sem.at[grp])

    def half_at(grp, part):
        return o_nat.at[pl.ds(grp * pairs + part * (pairs // 2), pairs // 2)]

    def help_half(k, part, to):
        grp = ngroup - helped + k
        return remote(o_help.at[k, pl.ds(part * (pairs // 2), pairs // 2)], half_at(grp, part), o_send.at[k, part], o_recv.at[grp, part], to)

    def help_detour():
        spot = o_help.at[1, pl.ds(pairs // 2, pairs // 2)]
        return remote(spot, spot, o_send.at[1, 1], o_recv.at[ngroup - 1, 1], 1)

    def help_relay():
        return remote(o_help.at[1, pl.ds(pairs // 2, pairs // 2)], half_at(ngroup - 1, 1), o_send.at[1, 1], o_recv.at[ngroup - 1, 1], 3)

    def finish(slot, gi):
        outs = []
        for j in range(pairs):
            t = jnp.concatenate([acc[slot * GROUP + h, :vdim, :] / acc[slot * GROUP + h, vdim:vdim + 1, :] for h in (2 * j, 2 * j + 1)], axis=0)
            outs.append(t.T.astype(bf16))
        for h in range(GROUP):
            acc[slot * GROUP + h] = jnp.zeros(acc.shape[1:], f32)

        helping, _, grp, _ = place_of(gi)

        @pl.when(jnp.logical_not(helping))
        def _():
            for j in range(pairs):
                o_nat[grp * pairs + j] = outs[j]
            output_copy(grp).start()

        @pl.when(helping)
        def _():
            k = gi - n_own + 1
            for j in range(pairs):
                o_help[k, j] = outs[j]
            help_half(k, 0, partner).start()
            detour = (me == 0) & (k == 1)

            @pl.when(detour)
            def _():
                help_detour().start()

            @pl.when(jnp.logical_not(detour))
            def _():
                help_half(k, 1, partner).start()

    def step(carry, new, own, after=None):
        (slot1, blk1, last1, gi1), (slot2, blk2, last2, gi2) = carry
        for u in range(GROUP):
            value_stage(u, slot2, blk2)
            exp_stage(u, slot1)
            if new is not None:
                score_stage(u, new[1], own, new[3])
        if after is not None:
            after()

        @pl.when(last2 == 1)
        def _():
            finish(slot2, gi2)

        return (new if new is not None else (SLOTS, 0, 0, 0)), (slot1, blk1, last1, gi1)

    def keys_and_values(slot, head0, blk):
        c = ckv[blk]
        at = pl.multiple_of(blk * rows, rows)
        for j in range(GROUP // 4):
            wk = wuk[pl.ds(pl.multiple_of((head0 + 4 * j) * nope, 4 * nope), 4 * nope), :]
            kk = lax.dot_general(c, wk, NT, preferred_element_type=f32).astype(bf16)
            kn[2 * j, pl.ds(at, rows), :] = kk[:, :128]
            kn[2 * j + 1, pl.ds(at, rows), :] = kk[:, 128:]
            wv = wuv[pl.ds(pl.multiple_of((head0 + 4 * j) * vdim, 4 * vdim), 4 * vdim), :]
            vv = lax.dot_general(wv, c, NT, preferred_element_type=f32).astype(bf16)
            for i in range(4):
                vt[slot * GROUP + 4 * j + i, :vdim, pl.ds(at, rows)] = vv[i * vdim:(i + 1) * vdim, :]

    def queries(buf, src, head0):
        ct, st = trig[src, :hr], trig[src, hr:]
        for j in range(GROUP // 4):
            w = wuq[pl.ds(pl.multiple_of((head0 + 4 * j) * qk, 4 * qk), 4 * qk), :]
            q = lax.dot_general(w, qlat[src], NT, preferred_element_type=f32)
            for i in range(4):
                u = 4 * j + i
                qh = q[i * qk:(i + 1) * qk]
                lo = (u % 2) * nope
                qaug[buf, u, lo:lo + nope, :] = qh[:nope].astype(bf16)
                r1, r2 = qh[nope:nope + hr], qh[nope + hr:]
                qaug[buf, u, 2 * nope:2 * nope + rot, :] = jnp.concatenate([r1 * ct - r2 * st, r2 * ct + r1 * st], axis=0).astype(bf16)

    def clear(slot):
        for u in range(GROUP):
            m_s[slot * GROUP + u] = jnp.full((1, rows), -jnp.inf, f32)

    def earlier(target, j):
        return lax.rem(j + target - 1, jnp.maximum(target, 1))

    def group(gi, carry):
        _, target, grp, slot = place_of(gi)
        gn = jnp.minimum(gi + 1, n_all - 1)
        helping_n, target_n, grp_n, _ = place_of(gn)
        slot_n = lax.rem(gi + 1, SLOTS)
        head0, head_n = grp * GROUP, grp_n * GROUP

        @pl.when((gi == n_own - 2) & (me == 3))
        def _():
            for c in query_copies(me):
                c.wait_recv()

        @pl.when((gi == n_own - 2) & (me == 0))
        def _():
            for c in query_halves()[1:] + (query_relay(),):
                c.wait_recv()
            received(3)

        @pl.when((gi == n_own - 1) & (me == 0))
        def _():
            received(1)
            received(2)

        def arrived(j):
            @pl.when((gi == 0) & (j < target))
            def _():
                blk = earlier(target, j)
                received(blk)

                @pl.when((me >= 2) & (blk == 3 - me))
                def _():
                    start(forward_copies(blk))

        def next_keys(j):
            more = j < target
            keys_and_values(jnp.where(more, slot, slot_n), jnp.where(more, head0, head_n),
                            jnp.where(more, earlier(target, j), target_n))

        def after_own():
            queries(lax.rem(gi + 1, 2), helping_n.astype(jnp.int32), head_n)
            next_keys(0)
            clear(slot_n)

        arrived(0)

        @pl.when((gi == 0) & (me == 2))
        def _():
            query_halves()[0].wait_recv()
            query_relay().start()
            start(latent_copies(me, 0))

        carry = step(carry, (slot, target, (target == 0).astype(jnp.int32), gi), True, after_own)

        def previous(j, carry):
            arrived(j + 1)
            return step(carry, (slot, earlier(target, j), (j == target - 1).astype(jnp.int32), gi), False,
                        lambda: next_keys(j + 1))

        carry = lax.fori_loop(0, target, previous, carry)

        return carry

    idle = (jnp.int32(SLOTS), jnp.int32(0), jnp.int32(0), jnp.int32(0))
    acc[...] = jnp.zeros_like(acc)
    queries(0, 0, 0)
    keys_and_values(0, 0, me)
    clear(0)
    carry = lax.fori_loop(0, n_all, group, (idle, idle))
    carry = step(carry, None, False)
    step(carry, None, False)

    @pl.when(me == 1)
    def _():
        help_detour().wait_recv()
        help_relay().start()
        help_relay().wait_send()

    def sent(copies):
        for c in copies:
            c.wait_send()

    @pl.when(me == 0)
    def _():
        sent(latent_copies(me, 1) + latent_copies(me, 3))

    @pl.when(me == 1)
    def _():
        sent(latent_copies(me, 2) + latent_copies(me, 0))

    @pl.when(me == 2)
    def _():
        sent(latent_copies(me, 3) + latent_copies(me, 0) + forward_copies(1) + query_copies(3) + (query_relay(),))

    @pl.when(me == 3)
    def _():
        sent(latent_copies(me, 0) + forward_copies(0) + query_halves())

    for k in range(MOST_HELPED):
        @pl.when(k < helped)
        def _():
            for part in range(2):
                help_half(k, part, partner).wait_send()

        @pl.when(k < given)
        def _():
            grp = n_own + k
            for part in range(2):
                remote(half_at(grp, part), half_at(grp, part), o_send.at[k, part], o_recv.at[grp, part], me).wait_recv()
            output_copy(grp).start()

    for grp in range(ngroup):
        output_copy(grp).wait()


def layer(pos, gq, gkv, x, wdkv, wdq, wuq, wuk, wuv, scale2, heads, groups):
    rows, dim = x.shape
    rank = gkv.shape[0]
    rot = wdkv.shape[0] - rank
    qrank = wdq.shape[1]
    nope = wuk.shape[0] // heads
    vdim = wuv.shape[0] // heads
    seq = rows * groups
    vm = pl.BlockSpec(memory_space=pltpu.VMEM)
    anym = pl.BlockSpec(memory_space=pl.ANY)
    f32 = jnp.float32
    bf16 = jnp.bfloat16
    dma = pltpu.SemaphoreType.DMA
    nhelp = MOST_HELPED
    return pl.pallas_call(
        functools.partial(layer_kernel, scale2=scale2, rows=rows, nope=nope, rot=rot, vdim=vdim, heads=heads, groups=groups),
        out_shape=(jax.ShapeDtypeStruct((heads // 2, rows, 2 * vdim), bf16),
                   jax.ShapeDtypeStruct((rows, rank), bf16),
                   jax.ShapeDtypeStruct((rot, rows), bf16)),
        in_specs=[vm, vm, vm] + [anym] * 6,
        out_specs=(anym, vm, vm),
        scratch_shapes=[
            pltpu.VMEM(x.shape, bf16),
            pltpu.VMEM(wdkv.shape, bf16),
            pltpu.VMEM(wdq.shape, bf16),
            pltpu.VMEM(wuq.shape, bf16),
            pltpu.VMEM(wuk.shape, bf16),
            pltpu.VMEM(wuv.shape, bf16),
            pltpu.VMEM((2, rows, qrank), bf16),
            pltpu.VMEM((2, rot, rows), f32),
            pltpu.VMEM((groups, rows, rank), bf16),
            pltpu.VMEM((groups, rot, rows), bf16),
            pltpu.VMEM((groups, rows, 128), bf16),
            pltpu.VMEM((2, GROUP, 256, rows), bf16),
            pltpu.VMEM((GROUP // 2, seq, 128), bf16),
            pltpu.VMEM((SLOTS * GROUP, vdim + 16, seq), bf16),
            pltpu.VMEM((GROUP, rows, rows), f32),
            pltpu.VMEM((GROUP, 1, rows), f32),
            pltpu.VMEM((GROUP, rows, rows), bf16),
            pltpu.VMEM((GROUP, 1, rows), f32),
            pltpu.VMEM(((SLOTS + 1) * GROUP, 1, rows), f32),
            pltpu.VMEM(((SLOTS + 1) * GROUP, vdim + 16, rows), f32),
            pltpu.VMEM((heads // 2, rows, 2 * vdim), bf16),
            pltpu.VMEM((nhelp, GROUP // 2, rows, 2 * vdim), bf16),
            dma((6,)),
            dma((groups,)), dma((groups,)), dma((groups,)), dma((groups,)), dma((2,)),
            dma((3,)), dma((3,)), dma, dma,
            dma((nhelp, 2)), dma((heads // GROUP, 2)),
            dma((heads // GROUP,)),
        ],
        compiler_params=pltpu.CompilerParams(vmem_limit_bytes=62 * 1024 * 1024, collective_id=0, has_side_effects=True),
        cost_estimate=pl.CostEstimate(flops=40_000_000_000, bytes_accessed=40_000_000, transcendentals=30_000_000),
    )(pos, gq, gkv, x, wdkv, wdq, wuq, wuk, wuv)


def project_kernel(o_ref, ckv_ref, cpe_ref, w_ref, out_ref, ckv_out, cpe_out):
    @pl.when(pl.program_id(0) == 0)
    def _():
        ckv_out[...] = ckv_ref[...]
        cpe_out[...] = cpe_ref[...]

    o_all = jnp.concatenate([o_ref[j] for j in range(o_ref.shape[0])], axis=1)
    out_ref[...] = jnp.dot(o_all, w_ref[...], preferred_element_type=jnp.float32).astype(out_ref.dtype)


def project(o, ckv, cpe, w):
    npair, rows, width = o.shape
    dim = w.shape[1]
    tile = 512

    def whole(a):
        return pl.BlockSpec(a.shape, lambda i: (0,) * a.ndim)

    return pl.pallas_call(
        project_kernel,
        grid=(dim // tile,),
        in_specs=[whole(o), whole(ckv), whole(cpe), pl.BlockSpec((w.shape[0], tile), lambda i: (0, i))],
        out_specs=(pl.BlockSpec((rows, tile), lambda i: (0, i)), whole(ckv), whole(cpe)),
        out_shape=(jax.ShapeDtypeStruct((rows, dim), jnp.bfloat16), jax.ShapeDtypeStruct(ckv.shape, ckv.dtype), jax.ShapeDtypeStruct(cpe.shape, cpe.dtype)),
        compiler_params=pltpu.CompilerParams(vmem_limit_bytes=62 * 1024 * 1024),
        cost_estimate=pl.CostEstimate(flops=2 * rows * dim * w.shape[0], bytes_accessed=2 * w.size, transcendentals=0),
    )(o, ckv, cpe, w)


def solution(mesh):
    groups = mesh.shape['sp']
    tok_spec = P(('dp', 'sp'))
    rows_spec = P(('dp', 'sp'), None)
    replicated = P()

    def local_step(tok_in, tok_pos, w_dq, g_q, w_uq, w_dkv, g_kv, w_uk, w_uv, w_o):
        heads, qk_dim = w_uq.shape[1:]
        kv_rank = g_kv.shape[0]
        rot_dim = w_dkv.shape[1] - kv_rank
        v_dim = w_uv.shape[2]
        attn_scale = (0.1 * math.log(YARN_FACTOR) + 1.0) ** 2 / math.sqrt(qk_dim)
        def flat(w):
            return jnp.transpose(w, (1, 2, 0)).reshape(-1, w.shape[0])

        o, ckv, cpe = layer(tok_pos, g_q, g_kv, tok_in, w_dkv.T, w_dq, flat(w_uq), flat(w_uk), flat(w_uv),
                                      attn_scale * math.log2(math.e), heads, groups)
        attn_out, cache_kv, cache_pe = project(o, ckv, cpe, w_o.reshape(heads * v_dim, -1))
        return attn_out, cache_kv, cache_pe.T

    return jax.shard_map(local_step, mesh=mesh, in_specs=(rows_spec, tok_spec, replicated, replicated, replicated, replicated, replicated, replicated, replicated, replicated), out_specs=(rows_spec, rows_spec, rows_spec), check_vma=False)
```

```python
import functools
import math
import jax
import jax.numpy as jnp
from jax import lax
from jax.experimental import pallas as pl
from jax.experimental.pallas import tpu as pltpu
from jax.sharding import PartitionSpec as P

ROPE_THETA = 10000.0
YARN_FACTOR = 40.0
ORIG_CTX = 4096.0
BETA_FAST = 32.0
BETA_SLOW = 1.0
NORM_EPS = 1e-6


def rope_freqs(rot_dim):
    half_dim = rot_dim // 2
    log_base = 2.0 * math.log(ROPE_THETA)
    low_idx = max(math.floor(rot_dim * math.log(ORIG_CTX / (BETA_FAST * 2.0 * math.pi)) / log_base), 0)
    high_idx = min(math.ceil(rot_dim * math.log(ORIG_CTX / (BETA_SLOW * 2.0 * math.pi)) / log_base), half_dim - 1)
    spread = max(high_idx - low_idx, 0.001)
    freq_list = []
    for freq_idx in range(half_dim):
        base_freq = ROPE_THETA ** (-2.0 * freq_idx / rot_dim)
        ramp_val = min(max((freq_idx - low_idx) / spread, 0.0), 1.0)
        freq_list.append(base_freq / YARN_FACTOR * ramp_val + base_freq * (1.0 - ramp_val))
    return freq_list


GROUP = 8
SLOTS = 3
MOST_HELPED = 2


def layer_kernel(pos_ref, gq_ref, gkv_ref, x_hbm, wdkv_hbm, wdq_hbm, wuq_hbm, wuk_hbm, wuv_hbm,
                 o_hbm, ckv_out, cpe_out,
                 x, wdkv, wdq, wuq, wuk, wuv, qlat, posf, trig, ckv, pet, pen, qaug, kn, vt,
                 s_buf, c_buf, p_buf, al_buf, m_s, acc, o_nat, o_help,
                 load_sem, c_send, c_recv, pe_send, pe_recv, f_send, q_send, q_recv, t_send, t_recv, o_send, o_recv, out_sem,
                 *, scale2, rows, nope, rot, vdim, heads, groups):
    f32 = jnp.float32
    bf16 = jnp.bfloat16
    NT = (((1,), (1,)), ((), ()))
    NN = (((1,), (0,)), ((), ()))
    half = rows // 2
    qk = nope + rot
    pairs = GROUP // 2
    ngroup = heads // GROUP
    me = lax.axis_index('sp')
    given = jnp.where(me == 3, 2, jnp.where(me == 2, 1, 0))
    helped = jnp.where(me == 0, 2, jnp.where(me == 3, 1, 0))
    partner = jnp.where(me == 0, 3, 2)
    n_own = ngroup - given
    n_all = n_own + helped

    loads = [pltpu.make_async_copy(s, d, load_sem.at[i]) for i, (s, d) in enumerate(
        ((x_hbm, x), (wdkv_hbm, wdkv), (wdq_hbm, wdq), (wuq_hbm, wuq), (wuk_hbm, wuk), (wuv_hbm, wuv)))]
    for c in loads:
        c.start()
    barrier = pltpu.get_barrier_semaphore()
    for d in range(1, groups):
        pl.semaphore_signal(barrier, inc=1, device_id={'sp': lax.rem(me + d, groups)}, device_id_type=pl.DeviceIdType.MESH)

    def remote(s, d, ssem, rsem, to):
        return pltpu.make_async_remote_copy(src_ref=s, dst_ref=d, send_sem=ssem, recv_sem=rsem,
                                            device_id={'sp': to}, device_id_type=pl.DeviceIdType.MESH)

    def latent_copies(origin, to):
        return (remote(ckv.at[origin], ckv.at[origin], c_send.at[to], c_recv.at[origin], to),
                remote(pet.at[origin], pet.at[origin], pe_send.at[to], pe_recv.at[origin], to))

    def forward_copies(origin):
        to = 5 - me
        return (remote(ckv.at[origin], ckv.at[origin], f_send.at[0], c_recv.at[origin], to),
                remote(pet.at[origin], pet.at[origin], f_send.at[1], pe_recv.at[origin], to))

    def query_copies(to):
        return (remote(qlat.at[0], qlat.at[1], q_send.at[0], q_recv.at[0], to),
                remote(posf.at[0], posf.at[1], t_send, t_recv, to))

    def query_halves():
        top, low = pl.ds(0, half), pl.ds(half, half)
        return (remote(qlat.at[0, low], qlat.at[1, low], q_send.at[1], q_recv.at[1], 2),
                remote(posf.at[0], posf.at[1], t_send, t_recv, 0),
                remote(qlat.at[0, top], qlat.at[1, top], q_send.at[0], q_recv.at[0], 0))

    def query_relay():
        low = pl.ds(half, half)
        return remote(qlat.at[1, low], qlat.at[1, low], q_send.at[2], q_recv.at[2], 0)

    def start(copies):
        for c in copies:
            c.start()

    def received(origin):
        for c in latent_copies(origin, me):
            c.wait_recv()
        unpack_rope(origin)

    def unpack_rope(origin):
        wide = jnp.concatenate([pet[origin].astype(f32), jnp.zeros((128 - rot, rows), f32)], axis=0)
        pen[origin] = wide.T.astype(bf16)

    hr = rot // 2
    freq_i = lax.broadcasted_iota(jnp.int32, (hr, rows), 0)
    freq = jnp.zeros((hr, rows), f32)
    for i, f in enumerate(rope_freqs(rot)):
        freq = jnp.where(freq_i == i, f, freq)

    def turn(i):
        angle = posf[i, :1] * freq
        trig[i, :hr] = jnp.cos(angle)
        trig[i, hr:] = jnp.sin(angle)

    posf[0] = jnp.broadcast_to(pos_ref[...].astype(f32).reshape(1, rows), (8, rows))
    turn(0)
    cos_t, sin_t = trig[0, :hr], trig[0, hr:]
    loads[0].wait()
    loads[1].wait()
    kvt = lax.dot_general(wdkv[...], x[...], NT, preferred_element_type=f32)
    rank = ckv.shape[2]
    a = kvt[:rank]
    norm = a * lax.rsqrt(jnp.sum(a * a, axis=0, keepdims=True) / rank + NORM_EPS)
    c_own = (norm.T * gkv_ref[...].reshape(1, rank)).astype(bf16)
    ckv[me] = c_own
    ckv_out[...] = c_own
    z1, z2 = kvt[rank:rank + hr], kvt[rank + hr:]
    pe_own = jnp.concatenate([z1 * cos_t - z2 * sin_t, z2 * cos_t + z1 * sin_t], axis=0).astype(bf16)
    pet[me] = pe_own
    cpe_out[...] = pe_own
    loads[2].wait()
    tile = 256
    qrank = wdq.shape[1]
    first = lax.dot_general(x[...], wdq[:, :tile], NN, preferred_element_type=f32)
    s_buf[0, :, :tile] = first
    pl.semaphore_wait(barrier, groups - 1)

    @pl.when(me == 0)
    def _():
        for t in (1, 3):
            start(latent_copies(me, t))

    @pl.when(me == 1)
    def _():
        for t in (2, 0):
            start(latent_copies(me, t))

    @pl.when(me == 2)
    def _():
        start(latent_copies(me, 3))

    rest = lax.dot_general(x[...], wdq[:, tile:], NN, preferred_element_type=f32)
    ql = jnp.concatenate([s_buf[0, :, :tile], rest], axis=1)
    qlat[0] = (ql * lax.rsqrt(jnp.sum(ql * ql, axis=1, keepdims=True) / qrank + NORM_EPS) * gq_ref[...].reshape(1, qrank)).astype(bf16)
    unpack_rope(me)
    qaug[...] = jnp.zeros_like(qaug)
    vt[:, vdim:, :] = jnp.ones((vt.shape[0], vt.shape[1] - vdim, vt.shape[2]), vt.dtype)
    for c in loads[3:]:
        c.wait()

    @pl.when(me == 2)
    def _():
        start(query_copies(3))

    @pl.when(me == 3)
    def _():
        start(query_halves())
        start(latent_copies(me, 0))

    FULL = ((0, 0), (1, 0), (0, 1), (1, 1))
    OWN = ((0, 0), (0, 1), (1, 1))
    row_i = lax.broadcasted_iota(jnp.int32, (half, half), 0)
    col_i = lax.broadcasted_iota(jnp.int32, (half, half), 1)

    def cols(i):
        return slice(i * half, (i + 1) * half)

    def score_stage(u, blk, own, gi):
        tops = [None, None]

        def place(s, k, i):
            s_buf[u, cols(k), cols(i)] = s
            top = jnp.max(s, axis=0, keepdims=True)
            tops[i] = top if tops[i] is None else jnp.maximum(tops[i], top)

        def dot(k0, k1, i0, i1):
            lhs = jnp.concatenate([kn[u // 2, pl.ds(pl.multiple_of(blk * rows + k0 * half, half), (k1 - k0) * half), :],
                                   pen[blk, k0 * half:k1 * half, :]], axis=1)
            return lax.dot_general(lhs, qaug[lax.rem(gi, 2), u, :, i0 * half:i1 * half], NN, preferred_element_type=f32)

        if own:
            s = dot(0, 1, 0, 2)
            place(jnp.where(row_i <= col_i, s[:, :half], -jnp.inf), 0, 0)
            place(s[:, half:], 0, 1)
            place(jnp.where(row_i <= col_i, dot(1, 2, 1, 2), -jnp.inf), 1, 1)
            s_buf[u, cols(1), cols(0)] = jnp.full((half, half), -jnp.inf, f32)
        else:
            s = dot(0, 2, 0, 2)
            for k, i in FULL:
                place(s[cols(k), cols(i)], k, i)
        for i in range(2):
            c_buf[u, :, cols(i)] = tops[i]

    def exp_stage(u, slot):
        h = slot * GROUP + u
        m_old = m_s[h]
        m_new = jnp.maximum(m_old, c_buf[u])
        al_buf[u] = jnp.exp2((m_old - m_new) * scale2)
        m_s[h] = m_new
        for k, i in FULL:
            p_buf[u, cols(k), cols(i)] = jnp.exp2((s_buf[u, cols(k), cols(i)] - m_new[:, cols(i)]) * scale2).astype(bf16)

    def value_stage(u, slot, blk):
        h = slot * GROUP + u
        v = vt[jnp.minimum(slot, SLOTS - 1) * GROUP + u, :, pl.ds(pl.multiple_of(blk * rows, rows), rows)]
        for i in range(2):
            t = lax.dot_general(v, p_buf[u, :, cols(i)], NN, preferred_element_type=f32)
            acc[h, :, cols(i)] = t + acc[h, :, cols(i)] * al_buf[u, :, cols(i)]

    def place_of(gi):
        helping = (gi >= n_own - 1) & (gi < n_own - 1 + helped)
        target = jnp.where(helping, partner, me)
        grp = jnp.where(helping, ngroup - helped + gi - n_own + 1, jnp.minimum(gi, n_own - 1))
        return helping, target, grp, lax.rem(gi, SLOTS)

    def output_copy(grp):
        return pltpu.make_async_copy(o_nat.at[pl.ds(grp * pairs, pairs)], o_hbm.at[pl.ds(grp * pairs, pairs)], out_sem.at[grp])

    def half_at(grp, part):
        return o_nat.at[pl.ds(grp * pairs + part * (pairs // 2), pairs // 2)]

    def help_half(k, part, to):
        grp = ngroup - helped + k
        return remote(o_help.at[k, pl.ds(part * (pairs // 2), pairs // 2)], half_at(grp, part), o_send.at[k, part], o_recv.at[grp, part], to)

    def help_detour():
        spot = o_help.at[1, pl.ds(pairs // 2, pairs // 2)]
        return remote(spot, spot, o_send.at[1, 1], o_recv.at[ngroup - 1, 1], 1)

    def help_relay():
        return remote(o_help.at[1, pl.ds(pairs // 2, pairs // 2)], half_at(ngroup - 1, 1), o_send.at[1, 1], o_recv.at[ngroup - 1, 1], 3)

    def finish(slot, gi):
        outs = []
        for j in range(pairs):
            t = jnp.concatenate([acc[slot * GROUP + h, :vdim, :] / acc[slot * GROUP + h, vdim:vdim + 1, :] for h in (2 * j, 2 * j + 1)], axis=0)
            outs.append(t.T.astype(bf16))
        for h in range(GROUP):
            acc[slot * GROUP + h] = jnp.zeros(acc.shape[1:], f32)

        helping, _, grp, _ = place_of(gi)

        @pl.when(jnp.logical_not(helping))
        def _():
            for j in range(pairs):
                o_nat[grp * pairs + j] = outs[j]
            output_copy(grp).start()

        @pl.when(helping)
        def _():
            k = gi - n_own + 1
            for j in range(pairs):
                o_help[k, j] = outs[j]
            help_half(k, 0, partner).start()
            detour = (me == 0) & (k == 1)

            @pl.when(detour)
            def _():
                help_detour().start()

            @pl.when(jnp.logical_not(detour))
            def _():
                help_half(k, 1, partner).start()

    def step(carry, new, own, after=None):
        (slot1, _, _, _), (slot2, blk2, last2, gi2) = carry
        for u in range(GROUP):
            value_stage(u, slot2, blk2)
            exp_stage(u, slot1)
            if new is not None:
                score_stage(u, new[1], own, new[3])
        if after is not None:
            after()

        @pl.when(last2 == 1)
        def _():
            finish(slot2, gi2)

    def keys_and_values(slot, head0, blk):
        c = ckv[blk]
        at = pl.multiple_of(blk * rows, rows)
        for j in range(GROUP // 4):
            wk = wuk[pl.ds(pl.multiple_of((head0 + 4 * j) * nope, 4 * nope), 4 * nope), :]
            kk = lax.dot_general(c, wk, NT, preferred_element_type=f32).astype(bf16)
            kn[2 * j, pl.ds(at, rows), :] = kk[:, :128]
            kn[2 * j + 1, pl.ds(at, rows), :] = kk[:, 128:]
            wv = wuv[pl.ds(pl.multiple_of((head0 + 4 * j) * vdim, 4 * vdim), 4 * vdim), :]
            vv = lax.dot_general(wv, c, NT, preferred_element_type=f32).astype(bf16)
            for i in range(4):
                vt[slot * GROUP + 4 * j + i, :vdim, pl.ds(at, rows)] = vv[i * vdim:(i + 1) * vdim, :]

    def queries(buf, src, head0):
        ct, st = trig[src, :hr], trig[src, hr:]
        for j in range(GROUP // 4):
            w = wuq[pl.ds(pl.multiple_of((head0 + 4 * j) * qk, 4 * qk), 4 * qk), :]
            q = lax.dot_general(w, qlat[src], NT, preferred_element_type=f32)
            for i in range(4):
                u = 4 * j + i
                qh = q[i * qk:(i + 1) * qk]
                lo = (u % 2) * nope
                qaug[buf, u, lo:lo + nope, :] = qh[:nope].astype(bf16)
                r1, r2 = qh[nope:nope + hr], qh[nope + hr:]
                qaug[buf, u, 2 * nope:2 * nope + rot, :] = jnp.concatenate([r1 * ct - r2 * st, r2 * ct + r1 * st], axis=0).astype(bf16)

    def clear(slot):
        for u in range(GROUP):
            m_s[slot * GROUP + u] = jnp.full((1, rows), -jnp.inf, f32)

    def block_at(helping, target, i):
        usual = jnp.where(i == 0, target, lax.rem(i + target - 2, jnp.maximum(target, 1)))
        return jnp.where(helping & (me == 0), jnp.where(i < 2, i, 5 - i), usual)

    def group(gi, carry):
        helping, target, grp, slot = place_of(gi)
        gn = jnp.minimum(gi + 1, n_all - 1)
        helping_n, target_n, grp_n, _ = place_of(gn)
        slot_n = lax.rem(gi + 1, SLOTS)

        @pl.when((gi == n_own - 2) & (me == 3))
        def _():
            for c in query_copies(me):
                c.wait_recv()
            turn(1)

        @pl.when((gi == n_own - 2) & (me == 0))
        def _():
            for c in query_halves()[1:] + (query_relay(),):
                c.wait_recv()
            turn(1)

        fresh = jnp.where(me == 0, gi == n_own - 1, gi == 0)

        def one(i, carry):
            blk = block_at(helping, target, i)
            more = i < target
            blk_n = jnp.where(more, block_at(helping, target, i + 1), block_at(helping_n, target_n, 0))

            @pl.when(fresh & more)
            def _():
                received(blk_n)

                @pl.when((me >= 2) & (blk_n == 3 - me))
                def _():
                    start(forward_copies(blk_n))

            @pl.when((gi == 0) & (me == 2) & (i == 0))
            def _():
                query_halves()[0].wait_recv()
                query_relay().start()
                start(latent_copies(me, 0))

            new = (slot, blk, (i == target).astype(jnp.int32), gi)

            def next_keys():
                keys_and_values(jnp.where(more, slot, slot_n), jnp.where(more, grp, grp_n) * GROUP, blk_n)

            def after_own():
                queries(lax.rem(gi + 1, 2), helping_n.astype(jnp.int32), grp_n * GROUP)
                next_keys()
                clear(slot_n)

            @pl.when(blk == target)
            def _():
                step(carry, new, True, after_own)

            @pl.when(blk != target)
            def _():
                step(carry, new, False, next_keys)

            return new, carry[0]

        return lax.fori_loop(0, target + 1, one, carry)

    idle = (jnp.int32(SLOTS), jnp.int32(0), jnp.int32(0), jnp.int32(0))
    acc[...] = jnp.zeros_like(acc)
    queries(0, 0, 0)
    keys_and_values(0, 0, me)
    clear(0)
    carry = lax.fori_loop(0, n_all, group, (idle, idle))
    step(carry, None, False)
    step((idle, carry[0]), None, False)

    @pl.when(me == 1)
    def _():
        help_detour().wait_recv()
        help_relay().start()
        help_relay().wait_send()

    def sent(copies):
        for c in copies:
            c.wait_send()

    @pl.when(me == 0)
    def _():
        sent(latent_copies(me, 1) + latent_copies(me, 3))

    @pl.when(me == 1)
    def _():
        sent(latent_copies(me, 2) + latent_copies(me, 0))

    @pl.when(me == 2)
    def _():
        sent(latent_copies(me, 3) + latent_copies(me, 0) + forward_copies(1) + query_copies(3) + (query_relay(),))

    @pl.when(me == 3)
    def _():
        sent(latent_copies(me, 0) + forward_copies(0) + query_halves())

    for k in range(MOST_HELPED):
        @pl.when(k < helped)
        def _():
            for part in range(2):
                help_half(k, part, partner).wait_send()

        @pl.when(k < given)
        def _():
            grp = n_own + k
            for part in range(2):
                remote(half_at(grp, part), half_at(grp, part), o_send.at[k, part], o_recv.at[grp, part], me).wait_recv()
            output_copy(grp).start()

    for grp in range(ngroup):
        output_copy(grp).wait()


def layer(pos, gq, gkv, x, wdkv, wdq, wuq, wuk, wuv, scale2, heads, groups):
    rows, dim = x.shape
    rank = gkv.shape[0]
    rot = wdkv.shape[0] - rank
    qrank = wdq.shape[1]
    nope = wuk.shape[0] // heads
    vdim = wuv.shape[0] // heads
    seq = rows * groups
    vm = pl.BlockSpec(memory_space=pltpu.VMEM)
    anym = pl.BlockSpec(memory_space=pl.ANY)
    f32 = jnp.float32
    bf16 = jnp.bfloat16
    dma = pltpu.SemaphoreType.DMA
    nhelp = MOST_HELPED
    return pl.pallas_call(
        functools.partial(layer_kernel, scale2=scale2, rows=rows, nope=nope, rot=rot, vdim=vdim, heads=heads, groups=groups),
        out_shape=(jax.ShapeDtypeStruct((heads // 2, rows, 2 * vdim), bf16),
                   jax.ShapeDtypeStruct((rows, rank), bf16),
                   jax.ShapeDtypeStruct((rot, rows), bf16)),
        in_specs=[vm, vm, vm] + [anym] * 6,
        out_specs=(anym, vm, vm),
        scratch_shapes=[
            pltpu.VMEM(x.shape, bf16),
            pltpu.VMEM(wdkv.shape, bf16),
            pltpu.VMEM(wdq.shape, bf16),
            pltpu.VMEM(wuq.shape, bf16),
            pltpu.VMEM(wuk.shape, bf16),
            pltpu.VMEM(wuv.shape, bf16),
            pltpu.VMEM((2, rows, qrank), bf16),
            pltpu.VMEM((2, 8, rows), f32),
            pltpu.VMEM((2, rot, rows), f32),
            pltpu.VMEM((groups, rows, rank), bf16),
            pltpu.VMEM((groups, rot, rows), bf16),
            pltpu.VMEM((groups, rows, 128), bf16),
            pltpu.VMEM((2, GROUP, 256, rows), bf16),
            pltpu.VMEM((GROUP // 2, seq, 128), bf16),
            pltpu.VMEM((SLOTS * GROUP, vdim + 16, seq), bf16),
            pltpu.VMEM((GROUP, rows, rows), f32),
            pltpu.VMEM((GROUP, 1, rows), f32),
            pltpu.VMEM((GROUP, rows, rows), bf16),
            pltpu.VMEM((GROUP, 1, rows), f32),
            pltpu.VMEM(((SLOTS + 1) * GROUP, 1, rows), f32),
            pltpu.VMEM(((SLOTS + 1) * GROUP, vdim + 16, rows), f32),
            pltpu.VMEM((heads // 2, rows, 2 * vdim), bf16),
            pltpu.VMEM((nhelp, GROUP // 2, rows, 2 * vdim), bf16),
            dma((6,)),
            dma((groups,)), dma((groups,)), dma((groups,)), dma((groups,)), dma((2,)),
            dma((3,)), dma((3,)), dma, dma,
            dma((nhelp, 2)), dma((heads // GROUP, 2)),
            dma((heads // GROUP,)),
        ],
        compiler_params=pltpu.CompilerParams(vmem_limit_bytes=62 * 1024 * 1024, collective_id=0, has_side_effects=True),
        cost_estimate=pl.CostEstimate(flops=40_000_000_000, bytes_accessed=40_000_000, transcendentals=30_000_000),
    )(pos, gq, gkv, x, wdkv, wdq, wuq, wuk, wuv)


def project_kernel(ckv_ref, cpe_ref, o_hbm, w_hbm, out_hbm, ckv_out, cpe_out, o, w, total, out, o_sem, w_sem, first_sem, out_sem, *, tile):
    f32 = jnp.float32
    npair, rows, width = o.shape
    depth, dim = w.shape
    parts = dim // tile
    deep = depth // parts
    per = npair // parts

    def cut(i):
        return pl.ds(i * tile, tile)

    o_copies = [pltpu.make_async_copy(o_hbm.at[pl.ds(i * per, per)], o.at[pl.ds(i * per, per)], o_sem.at[i]) for i in range(parts)]
    first = [pltpu.make_async_copy(w_hbm.at[pl.ds(i * deep, deep), cut(0)], w.at[pl.ds(i * deep, deep), cut(0)], first_sem.at[i]) for i in range(parts)]
    w_copies = [pltpu.make_async_copy(w_hbm.at[:, cut(i)], w.at[:, cut(i)], w_sem.at[i]) for i in range(parts)]
    out_copies = [pltpu.make_async_copy(out.at[:, cut(i)], out_hbm.at[:, cut(i)], out_sem.at[i]) for i in range(parts)]
    for i in range(parts):
        o_copies[i].start()
        first[i].start()
    for c in w_copies[1:]:
        c.start()
    ckv_out[...] = ckv_ref[...]
    cpe_out[...] = cpe_ref[...]
    for i in range(parts):
        o_copies[i].wait()
        first[i].wait()
        lhs = jnp.concatenate([o[i * per + j] for j in range(per)], axis=1)
        t = jnp.dot(lhs, w[i * deep:(i + 1) * deep, :tile], preferred_element_type=f32)
        total[...] = t if i == 0 else total[...] + t
    out[:, cut(0)] = total[...].astype(out.dtype)
    out_copies[0].start()
    for i in range(1, parts):
        w_copies[i].wait()
        lhs = jnp.concatenate([o[j] for j in range(npair)], axis=1)
        out[:, cut(i)] = jnp.dot(lhs, w[:, cut(i)], preferred_element_type=f32).astype(out.dtype)
        out_copies[i].start()
    for c in out_copies:
        c.wait()


def project(o, ckv, cpe, w):
    npair, rows, width = o.shape
    dim = w.shape[1]
    tile = 512
    parts = dim // tile
    bf16 = jnp.bfloat16
    vm = pl.BlockSpec(memory_space=pltpu.VMEM)
    anym = pl.BlockSpec(memory_space=pl.ANY)
    dma = pltpu.SemaphoreType.DMA
    return pl.pallas_call(
        functools.partial(project_kernel, tile=tile),
        in_specs=[vm, vm, anym, anym],
        out_specs=(anym, vm, vm),
        out_shape=(jax.ShapeDtypeStruct((rows, dim), bf16), jax.ShapeDtypeStruct(ckv.shape, ckv.dtype), jax.ShapeDtypeStruct(cpe.shape, cpe.dtype)),
        scratch_shapes=[pltpu.VMEM(o.shape, bf16), pltpu.VMEM(w.shape, bf16), pltpu.VMEM((rows, tile), jnp.float32), pltpu.VMEM((rows, dim), bf16),
                        dma((parts,)), dma((parts,)), dma((parts,)), dma((parts,))],
        compiler_params=pltpu.CompilerParams(vmem_limit_bytes=62 * 1024 * 1024),
        cost_estimate=pl.CostEstimate(flops=2 * rows * dim * w.shape[0], bytes_accessed=2 * w.size, transcendentals=0),
    )(ckv, cpe, o, w)


def solution(mesh):
    groups = mesh.shape['sp']
    tok_spec = P(('dp', 'sp'))
    rows_spec = P(('dp', 'sp'), None)
    replicated = P()

    def local_step(tok_in, tok_pos, w_dq, g_q, w_uq, w_dkv, g_kv, w_uk, w_uv, w_o):
        heads, qk_dim = w_uq.shape[1:]
        kv_rank = g_kv.shape[0]
        rot_dim = w_dkv.shape[1] - kv_rank
        v_dim = w_uv.shape[2]
        attn_scale = (0.1 * math.log(YARN_FACTOR) + 1.0) ** 2 / math.sqrt(qk_dim)
        def flat(w):
            return jnp.transpose(w, (1, 2, 0)).reshape(-1, w.shape[0])

        o, ckv, cpe = layer(tok_pos, g_q, g_kv, tok_in, w_dkv.T, w_dq, flat(w_uq), flat(w_uk), flat(w_uv),
                                      attn_scale * math.log2(math.e), heads, groups)
        attn_out, cache_kv, cache_pe = project(o, ckv, cpe, w_o.reshape(heads * v_dim, -1))
        return attn_out, cache_kv, cache_pe.T

    return jax.shard_map(local_step, mesh=mesh, in_specs=(rows_spec, tok_spec, replicated, replicated, replicated, replicated, replicated, replicated, replicated, replicated), out_specs=(rows_spec, rows_spec, rows_spec), check_vma=False)
```

```python
import functools
import math
import jax
import jax.numpy as jnp
from jax import lax
from jax.experimental import pallas as pl
from jax.experimental.pallas import tpu as pltpu
from jax.sharding import PartitionSpec as P

ROPE_THETA = 10000.0
YARN_FACTOR = 40.0
ORIG_CTX = 4096.0
BETA_FAST = 32.0
BETA_SLOW = 1.0
NORM_EPS = 1e-6


def rope_freqs(rot_dim):
    half_dim = rot_dim // 2
    log_base = 2.0 * math.log(ROPE_THETA)
    low_idx = max(math.floor(rot_dim * math.log(ORIG_CTX / (BETA_FAST * 2.0 * math.pi)) / log_base), 0)
    high_idx = min(math.ceil(rot_dim * math.log(ORIG_CTX / (BETA_SLOW * 2.0 * math.pi)) / log_base), half_dim - 1)
    spread = max(high_idx - low_idx, 0.001)
    freq_list = []
    for freq_idx in range(half_dim):
        base_freq = ROPE_THETA ** (-2.0 * freq_idx / rot_dim)
        ramp_val = min(max((freq_idx - low_idx) / spread, 0.0), 1.0)
        freq_list.append(base_freq / YARN_FACTOR * ramp_val + base_freq * (1.0 - ramp_val))
    return freq_list


GROUP = 8
SLOTS = 3
MOST_HELPED = 2


def layer_kernel(pos_ref, gq_ref, gkv_ref, x_hbm, wdkv_hbm, wdq_hbm, wuq_hbm, wuk_hbm, wuv_hbm,
                 o_hbm, ckv_out, cpe_out,
                 x, wdkv, wdq, wuq, wuk, wuv, qlat, posf, trig, ckv, pet, pen, qaug, kn, vt,
                 s_buf, c_buf, p_buf, al_buf, m_s, acc, o_nat, o_help,
                 load_sem, c_send, c_recv, pe_send, pe_recv, f_send, q_send, q_recv, t_send, t_recv, o_send, o_recv, out_sem,
                 *, scale2, rows, nope, rot, vdim, heads, groups):
    f32 = jnp.float32
    bf16 = jnp.bfloat16
    NT = (((1,), (1,)), ((), ()))
    NN = (((1,), (0,)), ((), ()))
    half = rows // 2
    qk = nope + rot
    pairs = GROUP // 2
    ngroup = heads // GROUP
    me = lax.axis_index('sp')
    given = jnp.where(me == 3, 2, jnp.where(me == 2, 1, 0))
    helped = jnp.where(me == 0, 2, jnp.where(me == 3, 1, 0))
    partner = jnp.where(me == 0, 3, 2)
    n_own = ngroup - given
    n_all = n_own + helped

    loads = [pltpu.make_async_copy(s, d, load_sem.at[i]) for i, (s, d) in enumerate(
        ((x_hbm, x), (wdkv_hbm, wdkv), (wdq_hbm, wdq), (wuq_hbm, wuq), (wuk_hbm, wuk), (wuv_hbm, wuv)))]
    for c in loads[:3]:
        c.start()
    barrier = pltpu.get_barrier_semaphore()
    for d in range(1, groups):
        pl.semaphore_signal(barrier, inc=1, device_id={'sp': lax.rem(me + d, groups)}, device_id_type=pl.DeviceIdType.MESH)

    def remote(s, d, ssem, rsem, to):
        return pltpu.make_async_remote_copy(src_ref=s, dst_ref=d, send_sem=ssem, recv_sem=rsem,
                                            device_id={'sp': to}, device_id_type=pl.DeviceIdType.MESH)

    def latent_copies(origin, to):
        return (remote(ckv.at[origin], ckv.at[origin], c_send.at[to], c_recv.at[origin], to),
                remote(pet.at[origin], pet.at[origin], pe_send.at[to], pe_recv.at[origin], to))

    def forward_copies(origin):
        to = 5 - me
        return (remote(ckv.at[origin], ckv.at[origin], f_send.at[0], c_recv.at[origin], to),
                remote(pet.at[origin], pet.at[origin], f_send.at[1], pe_recv.at[origin], to))

    def query_copies(to):
        return (remote(qlat.at[0], qlat.at[1], q_send.at[0], q_recv.at[0], to),
                remote(posf.at[0], posf.at[1], t_send, t_recv, to))

    def query_halves():
        top, low = pl.ds(0, half), pl.ds(half, half)
        return (remote(qlat.at[0, low], qlat.at[1, low], q_send.at[1], q_recv.at[1], 2),
                remote(posf.at[0], posf.at[1], t_send, t_recv, 0),
                remote(qlat.at[0, top], qlat.at[1, top], q_send.at[0], q_recv.at[0], 0))

    def query_relay():
        low = pl.ds(half, half)
        return remote(qlat.at[1, low], qlat.at[1, low], q_send.at[2], q_recv.at[2], 0)

    def start(copies):
        for c in copies:
            c.start()

    def received(origin):
        for c in latent_copies(origin, me):
            c.wait_recv()
        unpack_rope(origin)

    def unpack_rope(origin):
        wide = jnp.concatenate([pet[origin].astype(f32), jnp.zeros((128 - rot, rows), f32)], axis=0)
        pen[origin] = wide.T.astype(bf16)

    hr = rot // 2
    freq_i = lax.broadcasted_iota(jnp.int32, (hr, rows), 0)
    freq = jnp.zeros((hr, rows), f32)
    for i, f in enumerate(rope_freqs(rot)):
        freq = jnp.where(freq_i == i, f, freq)

    def turn(i):
        angle = posf[i, :1] * freq
        trig[i, :hr] = jnp.cos(angle)
        trig[i, hr:] = jnp.sin(angle)

    posf[0] = jnp.broadcast_to(pos_ref[...].astype(f32).reshape(1, rows), (8, rows))
    turn(0)
    cos_t, sin_t = trig[0, :hr], trig[0, hr:]
    loads[0].wait()
    loads[1].wait()
    for c in loads[3:]:
        c.start()
    kvt = lax.dot_general(wdkv[...], x[...], NT, preferred_element_type=f32)
    rank = ckv.shape[2]
    a = kvt[:rank]
    norm = a * lax.rsqrt(jnp.sum(a * a, axis=0, keepdims=True) / rank + NORM_EPS)
    c_own = (norm.T * gkv_ref[...].reshape(1, rank)).astype(bf16)
    ckv[me] = c_own
    ckv_out[...] = c_own
    z1, z2 = kvt[rank:rank + hr], kvt[rank + hr:]
    pe_own = jnp.concatenate([z1 * cos_t - z2 * sin_t, z2 * cos_t + z1 * sin_t], axis=0).astype(bf16)
    pet[me] = pe_own
    cpe_out[...] = pe_own
    loads[2].wait()
    tile = 256
    qrank = wdq.shape[1]
    first = lax.dot_general(x[...], wdq[:, :tile], NN, preferred_element_type=f32)
    s_buf[0, :, :tile] = first
    pl.semaphore_wait(barrier, groups - 1)

    @pl.when(me == 0)
    def _():
        for t in (1, 3):
            start(latent_copies(me, t))

    @pl.when(me == 1)
    def _():
        for t in (2, 0):
            start(latent_copies(me, t))

    @pl.when(me == 2)
    def _():
        start(latent_copies(me, 3))

    rest = lax.dot_general(x[...], wdq[:, tile:], NN, preferred_element_type=f32)
    ql = jnp.concatenate([s_buf[0, :, :tile], rest], axis=1)
    qlat[0] = (ql * lax.rsqrt(jnp.sum(ql * ql, axis=1, keepdims=True) / qrank + NORM_EPS) * gq_ref[...].reshape(1, qrank)).astype(bf16)
    unpack_rope(me)
    qaug[...] = jnp.zeros_like(qaug)
    vt[:, vdim:, :] = jnp.ones((vt.shape[0], vt.shape[1] - vdim, vt.shape[2]), vt.dtype)
    for c in loads[3:]:
        c.wait()

    @pl.when(me == 2)
    def _():
        start(query_copies(3))

    @pl.when(me == 3)
    def _():
        start(query_halves())
        start(latent_copies(me, 0))

    FULL = ((0, 0), (1, 0), (0, 1), (1, 1))
    OWN = ((0, 0), (0, 1), (1, 1))
    row_i = lax.broadcasted_iota(jnp.int32, (half, half), 0)
    col_i = lax.broadcasted_iota(jnp.int32, (half, half), 1)

    def cols(i):
        return slice(i * half, (i + 1) * half)

    def score_stage(u, blk, own, gi):
        tops = [None, None]

        def place(s, k, i):
            s_buf[u, cols(k), cols(i)] = s
            top = jnp.max(s, axis=0, keepdims=True)
            tops[i] = top if tops[i] is None else jnp.maximum(tops[i], top)

        def dot(k0, k1, i0, i1):
            lhs = jnp.concatenate([kn[u // 2, pl.ds(pl.multiple_of(blk * rows + k0 * half, half), (k1 - k0) * half), :],
                                   pen[blk, k0 * half:k1 * half, :]], axis=1)
            return lax.dot_general(lhs, qaug[lax.rem(gi, 2), u, :, i0 * half:i1 * half], NN, preferred_element_type=f32)

        if own:
            s = dot(0, 1, 0, 2)
            place(jnp.where(row_i <= col_i, s[:, :half], -jnp.inf), 0, 0)
            place(s[:, half:], 0, 1)
            place(jnp.where(row_i <= col_i, dot(1, 2, 1, 2), -jnp.inf), 1, 1)
            s_buf[u, cols(1), cols(0)] = jnp.full((half, half), -jnp.inf, f32)
        else:
            s = dot(0, 2, 0, 2)
            for k, i in FULL:
                place(s[cols(k), cols(i)], k, i)
        for i in range(2):
            c_buf[u, :, cols(i)] = tops[i]

    def exp_stage(u, slot):
        h = slot * GROUP + u
        m_old = m_s[h]
        m_new = jnp.maximum(m_old, c_buf[u])
        al_buf[u] = jnp.exp2((m_old - m_new) * scale2)
        m_s[h] = m_new
        for k, i in FULL:
            p_buf[u, cols(k), cols(i)] = jnp.exp2((s_buf[u, cols(k), cols(i)] - m_new[:, cols(i)]) * scale2).astype(bf16)

    def value_stage(u, slot, blk):
        h = slot * GROUP + u
        v = vt[jnp.minimum(slot, SLOTS - 1) * GROUP + u, :, pl.ds(pl.multiple_of(blk * rows, rows), rows)]
        for i in range(2):
            t = lax.dot_general(v, p_buf[u, :, cols(i)], NN, preferred_element_type=f32)
            acc[h, :, cols(i)] = t + acc[h, :, cols(i)] * al_buf[u, :, cols(i)]

    def place_of(gi):
        helping = (gi >= n_own - 1) & (gi < n_own - 1 + helped)
        target = jnp.where(helping, partner, me)
        grp = jnp.where(helping, ngroup - helped + gi - n_own + 1, jnp.minimum(gi, n_own - 1))
        return helping, target, grp, lax.rem(gi, SLOTS)

    def output_copy(grp):
        return pltpu.make_async_copy(o_nat.at[pl.ds(grp * pairs, pairs)], o_hbm.at[pl.ds(grp * pairs, pairs)], out_sem.at[grp])

    def half_at(grp, part):
        return o_nat.at[pl.ds(grp * pairs + part * (pairs // 2), pairs // 2)]

    def help_half(k, part, to):
        grp = ngroup - helped + k
        return remote(o_help.at[k, pl.ds(part * (pairs // 2), pairs // 2)], half_at(grp, part), o_send.at[k, part], o_recv.at[grp, part], to)

    def help_detour():
        spot = o_help.at[1, pl.ds(pairs // 2, pairs // 2)]
        return remote(spot, spot, o_send.at[1, 1], o_recv.at[ngroup - 1, 1], 1)

    def help_relay():
        return remote(o_help.at[1, pl.ds(pairs // 2, pairs // 2)], half_at(ngroup - 1, 1), o_send.at[1, 1], o_recv.at[ngroup - 1, 1], 3)

    def finish(slot, gi):
        outs = []
        for j in range(pairs):
            t = jnp.concatenate([acc[slot * GROUP + h, :vdim, :] / acc[slot * GROUP + h, vdim:vdim + 1, :] for h in (2 * j, 2 * j + 1)], axis=0)
            outs.append(t.T.astype(bf16))
        for h in range(GROUP):
            acc[slot * GROUP + h] = jnp.zeros(acc.shape[1:], f32)

        helping, _, grp, _ = place_of(gi)

        @pl.when(jnp.logical_not(helping))
        def _():
            for j in range(pairs):
                o_nat[grp * pairs + j] = outs[j]
            output_copy(grp).start()

        @pl.when(helping)
        def _():
            k = gi - n_own + 1
            for j in range(pairs):
                o_help[k, j] = outs[j]
            help_half(k, 0, partner).start()
            detour = (me == 0) & (k == 1)

            @pl.when(detour)
            def _():
                help_detour().start()

            @pl.when(jnp.logical_not(detour))
            def _():
                help_half(k, 1, partner).start()

    def step(carry, new, own, after=None):
        (slot1, _, _, _), (slot2, blk2, last2, gi2) = carry
        for u in range(GROUP):
            value_stage(u, slot2, blk2)
            exp_stage(u, slot1)
            if new is not None:
                score_stage(u, new[1], own, new[3])
        if after is not None:
            after()

        @pl.when(last2 == 1)
        def _():
            finish(slot2, gi2)

    def keys_and_values(slot, head0, blk):
        c = ckv[blk]
        at = pl.multiple_of(blk * rows, rows)
        for j in range(GROUP // 4):
            wk = wuk[pl.ds(pl.multiple_of((head0 + 4 * j) * nope, 4 * nope), 4 * nope), :]
            kk = lax.dot_general(c, wk, NT, preferred_element_type=f32).astype(bf16)
            kn[2 * j, pl.ds(at, rows), :] = kk[:, :128]
            kn[2 * j + 1, pl.ds(at, rows), :] = kk[:, 128:]
            wv = wuv[pl.ds(pl.multiple_of((head0 + 4 * j) * vdim, 4 * vdim), 4 * vdim), :]
            vv = lax.dot_general(wv, c, NT, preferred_element_type=f32).astype(bf16)
            for i in range(4):
                vt[slot * GROUP + 4 * j + i, :vdim, pl.ds(at, rows)] = vv[i * vdim:(i + 1) * vdim, :]

    def queries(buf, src, head0):
        ct, st = trig[src, :hr], trig[src, hr:]
        for j in range(GROUP // 4):
            w = wuq[pl.ds(pl.multiple_of((head0 + 4 * j) * qk, 4 * qk), 4 * qk), :]
            q = lax.dot_general(w, qlat[src], NT, preferred_element_type=f32)
            for i in range(4):
                u = 4 * j + i
                qh = q[i * qk:(i + 1) * qk]
                lo = (u % 2) * nope
                qaug[buf, u, lo:lo + nope, :] = qh[:nope].astype(bf16)
                r1, r2 = qh[nope:nope + hr], qh[nope + hr:]
                qaug[buf, u, 2 * nope:2 * nope + rot, :] = jnp.concatenate([r1 * ct - r2 * st, r2 * ct + r1 * st], axis=0).astype(bf16)

    def clear(slot):
        for u in range(GROUP):
            m_s[slot * GROUP + u] = jnp.full((1, rows), -jnp.inf, f32)

    def block_at(helping, target, i):
        usual = jnp.where(i == 0, target, lax.rem(i + target - 2, jnp.maximum(target, 1)))
        return jnp.where(helping & (me == 0), jnp.where(i < 2, i, 5 - i), usual)

    def group(gi, carry):
        helping, target, grp, slot = place_of(gi)
        gn = jnp.minimum(gi + 1, n_all - 1)
        helping_n, target_n, grp_n, _ = place_of(gn)
        slot_n = lax.rem(gi + 1, SLOTS)

        @pl.when((gi == n_own - 2) & (me == 3))
        def _():
            for c in query_copies(me):
                c.wait_recv()
            turn(1)

        @pl.when((gi == n_own - 2) & (me == 0))
        def _():
            for c in query_halves()[1:] + (query_relay(),):
                c.wait_recv()
            turn(1)

        fresh = jnp.where(me == 0, gi == n_own - 1, gi == 0)

        def one(i, carry):
            blk = block_at(helping, target, i)
            more = i < target
            blk_n = jnp.where(more, block_at(helping, target, i + 1), block_at(helping_n, target_n, 0))

            @pl.when(fresh & more)
            def _():
                received(blk_n)

                @pl.when((me >= 2) & (blk_n == 3 - me))
                def _():
                    start(forward_copies(blk_n))

            @pl.when((gi == 0) & (me == 2) & (i == 0))
            def _():
                query_halves()[0].wait_recv()
                query_relay().start()
                start(latent_copies(me, 0))

            new = (slot, blk, (i == target).astype(jnp.int32), gi)

            def next_keys():
                keys_and_values(jnp.where(more, slot, slot_n), jnp.where(more, grp, grp_n) * GROUP, blk_n)

            def after_own():
                queries(lax.rem(gi + 1, 2), helping_n.astype(jnp.int32), grp_n * GROUP)
                next_keys()
                clear(slot_n)

            @pl.when(blk == target)
            def _():
                step(carry, new, True, after_own)

            @pl.when(blk != target)
            def _():
                step(carry, new, False, next_keys)

            return new, carry[0]

        return lax.fori_loop(0, target + 1, one, carry)

    idle = (jnp.int32(SLOTS), jnp.int32(0), jnp.int32(0), jnp.int32(0))
    acc[...] = jnp.zeros_like(acc)
    queries(0, 0, 0)
    keys_and_values(0, 0, me)
    clear(0)
    carry = lax.fori_loop(0, n_all, group, (idle, idle))
    step(carry, None, False)
    step((idle, carry[0]), None, False)

    @pl.when(me == 1)
    def _():
        help_detour().wait_recv()
        help_relay().start()
        help_relay().wait_send()

    def sent(copies):
        for c in copies:
            c.wait_send()

    @pl.when(me == 0)
    def _():
        sent(latent_copies(me, 1) + latent_copies(me, 3))

    @pl.when(me == 1)
    def _():
        sent(latent_copies(me, 2) + latent_copies(me, 0))

    @pl.when(me == 2)
    def _():
        sent(latent_copies(me, 3) + latent_copies(me, 0) + forward_copies(1) + query_copies(3) + (query_relay(),))

    @pl.when(me == 3)
    def _():
        sent(latent_copies(me, 0) + forward_copies(0) + query_halves())

    for k in range(MOST_HELPED):
        @pl.when(k < helped)
        def _():
            for part in range(2):
                help_half(k, part, partner).wait_send()

        @pl.when(k < given)
        def _():
            grp = n_own + k
            for part in range(2):
                remote(half_at(grp, part), half_at(grp, part), o_send.at[k, part], o_recv.at[grp, part], me).wait_recv()
            output_copy(grp).start()

    for grp in range(ngroup):
        output_copy(grp).wait()


def layer(pos, gq, gkv, x, wdkv, wdq, wuq, wuk, wuv, scale2, heads, groups):
    rows, dim = x.shape
    rank = gkv.shape[0]
    rot = wdkv.shape[0] - rank
    qrank = wdq.shape[1]
    nope = wuk.shape[0] // heads
    vdim = wuv.shape[0] // heads
    seq = rows * groups
    vm = pl.BlockSpec(memory_space=pltpu.VMEM)
    anym = pl.BlockSpec(memory_space=pl.ANY)
    f32 = jnp.float32
    bf16 = jnp.bfloat16
    dma = pltpu.SemaphoreType.DMA
    nhelp = MOST_HELPED
    return pl.pallas_call(
        functools.partial(layer_kernel, scale2=scale2, rows=rows, nope=nope, rot=rot, vdim=vdim, heads=heads, groups=groups),
        out_shape=(jax.ShapeDtypeStruct((heads // 2, rows, 2 * vdim), bf16),
                   jax.ShapeDtypeStruct((rows, rank), bf16),
                   jax.ShapeDtypeStruct((rot, rows), bf16)),
        in_specs=[vm, vm, vm] + [anym] * 6,
        out_specs=(anym, vm, vm),
        scratch_shapes=[
            pltpu.VMEM(x.shape, bf16),
            pltpu.VMEM(wdkv.shape, bf16),
            pltpu.VMEM(wdq.shape, bf16),
            pltpu.VMEM(wuq.shape, bf16),
            pltpu.VMEM(wuk.shape, bf16),
            pltpu.VMEM(wuv.shape, bf16),
            pltpu.VMEM((2, rows, qrank), bf16),
            pltpu.VMEM((2, 8, rows), f32),
            pltpu.VMEM((2, rot, rows), f32),
            pltpu.VMEM((groups, rows, rank), bf16),
            pltpu.VMEM((groups, rot, rows), bf16),
            pltpu.VMEM((groups, rows, 128), bf16),
            pltpu.VMEM((2, GROUP, 256, rows), bf16),
            pltpu.VMEM((GROUP // 2, seq, 128), bf16),
            pltpu.VMEM((SLOTS * GROUP, vdim + 16, seq), bf16),
            pltpu.VMEM((GROUP, rows, rows), f32),
            pltpu.VMEM((GROUP, 1, rows), f32),
            pltpu.VMEM((GROUP, rows, rows), bf16),
            pltpu.VMEM((GROUP, 1, rows), f32),
            pltpu.VMEM(((SLOTS + 1) * GROUP, 1, rows), f32),
            pltpu.VMEM(((SLOTS + 1) * GROUP, vdim + 16, rows), f32),
            pltpu.VMEM((heads // 2, rows, 2 * vdim), bf16),
            pltpu.VMEM((nhelp, GROUP // 2, rows, 2 * vdim), bf16),
            dma((6,)),
            dma((groups,)), dma((groups,)), dma((groups,)), dma((groups,)), dma((2,)),
            dma((3,)), dma((3,)), dma, dma,
            dma((nhelp, 2)), dma((heads // GROUP, 2)),
            dma((heads // GROUP,)),
        ],
        compiler_params=pltpu.CompilerParams(vmem_limit_bytes=62 * 1024 * 1024, collective_id=0, has_side_effects=True),
        cost_estimate=pl.CostEstimate(flops=40_000_000_000, bytes_accessed=40_000_000, transcendentals=30_000_000),
    )(pos, gq, gkv, x, wdkv, wdq, wuq, wuk, wuv)


def project_kernel(ckv_ref, cpe_ref, o_hbm, w_hbm, out_hbm, ckv_out, cpe_out, o, w, total, out, o_sem, w_sem, out_sem, *, tile):
    f32 = jnp.float32
    npair = o.shape[0]
    depth, dim = w.shape
    parts = dim // tile
    deep = depth // parts
    per = npair // parts

    def cut(i):
        return pl.ds(i * tile, tile)

    o_copies = [pltpu.make_async_copy(o_hbm.at[pl.ds(i * per, per)], o.at[pl.ds(i * per, per)], o_sem.at[i]) for i in range(parts)]
    w_copies = [pltpu.make_async_copy(w_hbm.at[pl.ds(i * deep, deep)], w.at[pl.ds(i * deep, deep)], w_sem.at[i]) for i in range(parts)]
    out_copies = [pltpu.make_async_copy(out.at[:, cut(i)], out_hbm.at[:, cut(i)], out_sem.at[i]) for i in range(parts)]
    for i in range(parts):
        o_copies[i].start()
        w_copies[i].start()
    ckv_out[...] = ckv_ref[...]
    cpe_out[...] = cpe_ref[...]
    for i in range(parts):
        o_copies[i].wait()
        w_copies[i].wait()
        lhs = jnp.concatenate([o[i * per + j] for j in range(per)], axis=1)
        for n in range(parts):
            t = jnp.dot(lhs, w[i * deep:(i + 1) * deep, cut(n)], preferred_element_type=f32)
            if i > 0:
                t = t + total[:, cut(n)]
            if i < parts - 1:
                total[:, cut(n)] = t
            else:
                out[:, cut(n)] = t.astype(out.dtype)
                out_copies[n].start()
    for c in out_copies:
        c.wait()


def project(o, ckv, cpe, w):
    npair, rows, width = o.shape
    dim = w.shape[1]
    tile = 512
    parts = dim // tile
    bf16 = jnp.bfloat16
    vm = pl.BlockSpec(memory_space=pltpu.VMEM)
    anym = pl.BlockSpec(memory_space=pl.ANY)
    dma = pltpu.SemaphoreType.DMA
    return pl.pallas_call(
        functools.partial(project_kernel, tile=tile),
        in_specs=[vm, vm, anym, anym],
        out_specs=(anym, vm, vm),
        out_shape=(jax.ShapeDtypeStruct((rows, dim), bf16), jax.ShapeDtypeStruct(ckv.shape, ckv.dtype), jax.ShapeDtypeStruct(cpe.shape, cpe.dtype)),
        scratch_shapes=[pltpu.VMEM(o.shape, bf16), pltpu.VMEM(w.shape, bf16), pltpu.VMEM((rows, dim), jnp.float32), pltpu.VMEM((rows, dim), bf16),
                        dma((parts,)), dma((parts,)), dma((parts,))],
        compiler_params=pltpu.CompilerParams(vmem_limit_bytes=62 * 1024 * 1024),
        cost_estimate=pl.CostEstimate(flops=2 * rows * dim * w.shape[0], bytes_accessed=2 * w.size, transcendentals=0),
    )(ckv, cpe, o, w)


def solution(mesh):
    groups = mesh.shape['sp']
    tok_spec = P(('dp', 'sp'))
    rows_spec = P(('dp', 'sp'), None)
    replicated = P()

    def local_step(tok_in, tok_pos, w_dq, g_q, w_uq, w_dkv, g_kv, w_uk, w_uv, w_o):
        heads, qk_dim = w_uq.shape[1:]
        kv_rank = g_kv.shape[0]
        rot_dim = w_dkv.shape[1] - kv_rank
        v_dim = w_uv.shape[2]
        attn_scale = (0.1 * math.log(YARN_FACTOR) + 1.0) ** 2 / math.sqrt(qk_dim)
        def flat(w):
            return jnp.transpose(w, (1, 2, 0)).reshape(-1, w.shape[0])

        o, ckv, cpe = layer(tok_pos, g_q, g_kv, tok_in, w_dkv.T, w_dq, flat(w_uq), flat(w_uk), flat(w_uv),
                                      attn_scale * math.log2(math.e), heads, groups)
        attn_out, cache_kv, cache_pe = project(o, ckv, cpe, w_o.reshape(heads * v_dim, -1))
        return attn_out, cache_kv, cache_pe.T

    return jax.shard_map(local_step, mesh=mesh, in_specs=(rows_spec, tok_spec, replicated, replicated, replicated, replicated, replicated, replicated, replicated, replicated), out_specs=(rows_spec, rows_spec, rows_spec), check_vma=False)
```

```python
import functools
import math
import jax
import jax.numpy as jnp
from jax import lax
from jax.experimental import pallas as pl
from jax.experimental.pallas import tpu as pltpu
from jax.sharding import PartitionSpec as P

ROPE_THETA = 10000.0
YARN_FACTOR = 40.0
ORIG_CTX = 4096.0
BETA_FAST = 32.0
BETA_SLOW = 1.0
NORM_EPS = 1e-6


def rope_freqs(rot_dim):
    half_dim = rot_dim // 2
    log_base = 2.0 * math.log(ROPE_THETA)
    low_idx = max(math.floor(rot_dim * math.log(ORIG_CTX / (BETA_FAST * 2.0 * math.pi)) / log_base), 0)
    high_idx = min(math.ceil(rot_dim * math.log(ORIG_CTX / (BETA_SLOW * 2.0 * math.pi)) / log_base), half_dim - 1)
    spread = max(high_idx - low_idx, 0.001)
    freq_list = []
    for freq_idx in range(half_dim):
        base_freq = ROPE_THETA ** (-2.0 * freq_idx / rot_dim)
        ramp_val = min(max((freq_idx - low_idx) / spread, 0.0), 1.0)
        freq_list.append(base_freq / YARN_FACTOR * ramp_val + base_freq * (1.0 - ramp_val))
    return freq_list


GROUP = 8
SLOTS = 3
MOST_HELPED = 2


def layer_kernel(pos_ref, gq_ref, gkv_ref, x_hbm, wdkv_hbm, wdq_hbm, wuq_hbm, wuk_hbm, wuv_hbm,
                 o_hbm, ckv_out, cpe_out,
                 x, wdkv, wdq, wuq, wuk, wuv, qlat, posf, trig, ckv, pet, pen, qaug, kn, vt,
                 s_buf, c_buf, p_buf, al_buf, m_s, acc, o_nat, o_help,
                 load_sem, c_send, c_recv, pe_send, pe_recv, f_send, q_send, q_recv, t_send, t_recv, o_send, o_recv, out_sem,
                 *, scale2, rows, nope, rot, vdim, heads, groups):
    f32 = jnp.float32
    bf16 = jnp.bfloat16
    NT = (((1,), (1,)), ((), ()))
    NN = (((1,), (0,)), ((), ()))
    half = rows // 2
    qk = nope + rot
    pairs = GROUP // 2
    ngroup = heads // GROUP
    me = lax.axis_index('sp')
    given = jnp.where(me == 3, 2, jnp.where(me == 2, 1, 0))
    helped = jnp.where(me == 0, 2, jnp.where(me == 3, 1, 0))
    partner = jnp.where(me == 0, 3, 2)
    n_own = ngroup - given
    n_all = n_own + helped

    loads = [pltpu.make_async_copy(s, d, load_sem.at[i]) for i, (s, d) in enumerate(
        ((x_hbm, x), (wdkv_hbm, wdkv), (wdq_hbm, wdq), (wuq_hbm, wuq), (wuk_hbm, wuk), (wuv_hbm, wuv)))]
    for c in loads[:3]:
        c.start()
    barrier = pltpu.get_barrier_semaphore()
    for d in range(1, groups):
        pl.semaphore_signal(barrier, inc=1, device_id={'sp': lax.rem(me + d, groups)}, device_id_type=pl.DeviceIdType.MESH)

    def remote(s, d, ssem, rsem, to):
        return pltpu.make_async_remote_copy(src_ref=s, dst_ref=d, send_sem=ssem, recv_sem=rsem,
                                            device_id={'sp': to}, device_id_type=pl.DeviceIdType.MESH)

    def latent_copies(origin, to):
        return (remote(ckv.at[origin], ckv.at[origin], c_send.at[to], c_recv.at[origin], to),
                remote(pet.at[origin], pet.at[origin], pe_send.at[to], pe_recv.at[origin], to))

    def forward_copies(origin):
        to = 5 - me
        return (remote(ckv.at[origin], ckv.at[origin], f_send.at[0], c_recv.at[origin], to),
                remote(pet.at[origin], pet.at[origin], f_send.at[1], pe_recv.at[origin], to))

    def query_copies(to):
        return (remote(qlat.at[0], qlat.at[1], q_send.at[0], q_recv.at[0], to),
                remote(posf.at[0], posf.at[1], t_send, t_recv, to))

    def query_halves():
        top, low = pl.ds(0, half), pl.ds(half, half)
        return (remote(qlat.at[0, low], qlat.at[1, low], q_send.at[1], q_recv.at[1], 2),
                remote(posf.at[0], posf.at[1], t_send, t_recv, 0),
                remote(qlat.at[0, top], qlat.at[1, top], q_send.at[0], q_recv.at[0], 0))

    def query_relay():
        low = pl.ds(half, half)
        return remote(qlat.at[1, low], qlat.at[1, low], q_send.at[2], q_recv.at[2], 0)

    def start(copies):
        for c in copies:
            c.start()

    def received(origin):
        for c in latent_copies(origin, me):
            c.wait_recv()
        unpack_rope(origin)

    def unpack_rope(origin):
        wide = jnp.concatenate([pet[origin].astype(f32), jnp.zeros((128 - rot, rows), f32)], axis=0)
        pen[origin] = wide.T.astype(bf16)

    hr = rot // 2

    def cols(i):
        return slice(i * half, (i + 1) * half)

    freq_i = lax.broadcasted_iota(jnp.int32, (hr, rows), 0)
    freq = jnp.zeros((hr, rows), f32)
    for i, f in enumerate(rope_freqs(rot)):
        freq = jnp.where(freq_i == i, f, freq)

    def turn(i):
        angle = posf[i, :1] * freq
        trig[i, :hr] = jnp.cos(angle)
        trig[i, hr:] = jnp.sin(angle)

    posf[0] = jnp.broadcast_to(pos_ref[...].astype(f32).reshape(1, rows), (8, rows))
    turn(0)
    cos_t, sin_t = trig[0, :hr], trig[0, hr:]
    qaug[...] = jnp.zeros_like(qaug)
    vt[:, vdim:, :] = jnp.ones((vt.shape[0], vt.shape[1] - vdim, vt.shape[2]), vt.dtype)
    acc[...] = jnp.zeros_like(acc)
    loads[0].wait()
    loads[1].wait()
    for c in loads[3:]:
        c.start()
    kvt = lax.dot_general(wdkv[...], x[...], NT, preferred_element_type=f32)
    rank = ckv.shape[2]
    a = kvt[:rank]
    norm = a * lax.rsqrt(jnp.sum(a * a, axis=0, keepdims=True) / rank + NORM_EPS)
    c_own = (norm.T * gkv_ref[...].reshape(1, rank)).astype(bf16)
    ckv[me] = c_own
    ckv_out[...] = c_own
    z1, z2 = kvt[rank:rank + hr], kvt[rank + hr:]
    pe_own = jnp.concatenate([z1 * cos_t - z2 * sin_t, z2 * cos_t + z1 * sin_t], axis=0).astype(bf16)
    pet[me] = pe_own
    cpe_out[...] = pe_own
    loads[2].wait()
    qrank = wdq.shape[1]

    def query_latent(part):
        ql = lax.dot_general(x[cols(part)], wdq[...], NN, preferred_element_type=f32)
        ql = ql * lax.rsqrt(jnp.sum(ql * ql, axis=1, keepdims=True) / qrank + NORM_EPS) * gq_ref[...].reshape(1, qrank)
        qlat[0, cols(part)] = ql.astype(bf16)

    query_latent(0)
    pl.semaphore_wait(barrier, groups - 1)

    @pl.when(me == 0)
    def _():
        for t in (1, 3):
            start(latent_copies(me, t))

    @pl.when(me == 1)
    def _():
        for t in (2, 0):
            start(latent_copies(me, t))

    @pl.when(me == 2)
    def _():
        start(latent_copies(me, 3))

    query_latent(1)
    unpack_rope(me)
    for c in loads[3:]:
        c.wait()

    @pl.when(me == 2)
    def _():
        start(query_copies(3))

    @pl.when(me == 3)
    def _():
        start(query_halves())
        start(latent_copies(me, 0))

    FULL = ((0, 0), (1, 0), (0, 1), (1, 1))
    OWN = ((0, 0), (0, 1), (1, 1))
    row_i = lax.broadcasted_iota(jnp.int32, (half, half), 0)
    col_i = lax.broadcasted_iota(jnp.int32, (half, half), 1)

    def score_stage(u, blk, own, gi):
        tops = [None, None]

        def place(s, k, i):
            s_buf[u, cols(k), cols(i)] = s
            top = jnp.max(s, axis=0, keepdims=True)
            tops[i] = top if tops[i] is None else jnp.maximum(tops[i], top)

        def dot(k0, k1, i0, i1):
            lhs = jnp.concatenate([kn[u // 2, pl.ds(pl.multiple_of(blk * rows + k0 * half, half), (k1 - k0) * half), :],
                                   pen[blk, k0 * half:k1 * half, :]], axis=1)
            return lax.dot_general(lhs, qaug[lax.rem(gi, 2), u, :, i0 * half:i1 * half], NN, preferred_element_type=f32)

        if own:
            s = dot(0, 1, 0, 2)
            place(jnp.where(row_i <= col_i, s[:, :half], -jnp.inf), 0, 0)
            place(s[:, half:], 0, 1)
            place(jnp.where(row_i <= col_i, dot(1, 2, 1, 2), -jnp.inf), 1, 1)
            s_buf[u, cols(1), cols(0)] = jnp.full((half, half), -jnp.inf, f32)
        else:
            s = dot(0, 2, 0, 2)
            for k, i in FULL:
                place(s[cols(k), cols(i)], k, i)
        for i in range(2):
            c_buf[u, :, cols(i)] = tops[i]

    def exp_stage(u, slot):
        h = slot * GROUP + u
        m_old = m_s[h]
        m_new = jnp.maximum(m_old, c_buf[u])
        al_buf[u] = jnp.exp2((m_old - m_new) * scale2)
        m_s[h] = m_new
        for k, i in FULL:
            p_buf[u, cols(k), cols(i)] = jnp.exp2((s_buf[u, cols(k), cols(i)] - m_new[:, cols(i)]) * scale2).astype(bf16)

    def value_stage(u, slot, blk):
        h = slot * GROUP + u
        v = vt[jnp.minimum(slot, SLOTS - 1) * GROUP + u, :, pl.ds(pl.multiple_of(blk * rows, rows), rows)]
        for i in range(2):
            t = lax.dot_general(v, p_buf[u, :, cols(i)], NN, preferred_element_type=f32)
            acc[h, :, cols(i)] = t + acc[h, :, cols(i)] * al_buf[u, :, cols(i)]

    def place_of(gi):
        helping = (gi >= n_own - 1) & (gi < n_own - 1 + helped)
        target = jnp.where(helping, partner, me)
        grp = jnp.where(helping, ngroup - helped + gi - n_own + 1, jnp.minimum(gi, n_own - 1))
        return helping, target, grp, lax.rem(gi, SLOTS)

    def output_copy(grp):
        return pltpu.make_async_copy(o_nat.at[pl.ds(grp * pairs, pairs)], o_hbm.at[pl.ds(grp * pairs, pairs)], out_sem.at[grp])

    def half_at(grp, part):
        return o_nat.at[pl.ds(grp * pairs + part * (pairs // 2), pairs // 2)]

    def help_half(k, part, to):
        grp = ngroup - helped + k
        return remote(o_help.at[k, pl.ds(part * (pairs // 2), pairs // 2)], half_at(grp, part), o_send.at[k, part], o_recv.at[grp, part], to)

    def help_detour():
        spot = o_help.at[1, pl.ds(pairs // 2, pairs // 2)]
        return remote(spot, spot, o_send.at[1, 1], o_recv.at[ngroup - 1, 1], 1)

    def help_relay():
        return remote(o_help.at[1, pl.ds(pairs // 2, pairs // 2)], half_at(ngroup - 1, 1), o_send.at[1, 1], o_recv.at[ngroup - 1, 1], 3)

    def finish(slot, gi):
        outs = []
        for j in range(pairs):
            t = jnp.concatenate([acc[slot * GROUP + h, :vdim, :] / acc[slot * GROUP + h, vdim:vdim + 1, :] for h in (2 * j, 2 * j + 1)], axis=0)
            outs.append(t.T.astype(bf16))
        for h in range(GROUP):
            acc[slot * GROUP + h] = jnp.zeros(acc.shape[1:], f32)

        helping, _, grp, _ = place_of(gi)

        @pl.when(jnp.logical_not(helping))
        def _():
            for j in range(pairs):
                o_nat[grp * pairs + j] = outs[j]
            output_copy(grp).start()

        @pl.when(helping)
        def _():
            k = gi - n_own + 1
            for j in range(pairs):
                o_help[k, j] = outs[j]
            help_half(k, 0, partner).start()
            detour = (me == 0) & (k == 1)

            @pl.when(detour)
            def _():
                help_detour().start()

            @pl.when(jnp.logical_not(detour))
            def _():
                help_half(k, 1, partner).start()

    def step(carry, new, own, after=None, values_only=False):
        (slot1, _, _, _), (slot2, blk2, last2, gi2) = carry
        for u in range(GROUP):
            value_stage(u, slot2, blk2)
            if not values_only:
                exp_stage(u, slot1)
            if new is not None:
                score_stage(u, new[1], own, new[3])
        if after is not None:
            after()

        @pl.when(last2 == 1)
        def _():
            finish(slot2, gi2)

    def keys_and_values(slot, head0, blk):
        c = ckv[blk]
        at = pl.multiple_of(blk * rows, rows)
        for j in range(GROUP // 4):
            wk = wuk[pl.ds(pl.multiple_of((head0 + 4 * j) * nope, 4 * nope), 4 * nope), :]
            kk = lax.dot_general(c, wk, NT, preferred_element_type=f32).astype(bf16)
            kn[2 * j, pl.ds(at, rows), :] = kk[:, :128]
            kn[2 * j + 1, pl.ds(at, rows), :] = kk[:, 128:]
            wv = wuv[pl.ds(pl.multiple_of((head0 + 4 * j) * vdim, 4 * vdim), 4 * vdim), :]
            vv = lax.dot_general(wv, c, NT, preferred_element_type=f32).astype(bf16)
            for i in range(4):
                vt[slot * GROUP + 4 * j + i, :vdim, pl.ds(at, rows)] = vv[i * vdim:(i + 1) * vdim, :]

    def queries(buf, src, head0):
        ct, st = trig[src, :hr], trig[src, hr:]
        for j in range(GROUP // 4):
            w = wuq[pl.ds(pl.multiple_of((head0 + 4 * j) * qk, 4 * qk), 4 * qk), :]
            q = lax.dot_general(w, qlat[src], NT, preferred_element_type=f32)
            for i in range(4):
                u = 4 * j + i
                qh = q[i * qk:(i + 1) * qk]
                lo = (u % 2) * nope
                qaug[buf, u, lo:lo + nope, :] = qh[:nope].astype(bf16)
                r1, r2 = qh[nope:nope + hr], qh[nope + hr:]
                qaug[buf, u, 2 * nope:2 * nope + rot, :] = jnp.concatenate([r1 * ct - r2 * st, r2 * ct + r1 * st], axis=0).astype(bf16)

    def clear(slot):
        for u in range(GROUP):
            m_s[slot * GROUP + u] = jnp.full((1, rows), -jnp.inf, f32)

    def block_at(helping, target, i):
        usual = jnp.where(i == 0, target, lax.rem(i + target - 2, jnp.maximum(target, 1)))
        return jnp.where(helping & (me == 0), jnp.where(i < 2, i, 5 - i), usual)

    def group(gi, carry):
        helping, target, grp, slot = place_of(gi)
        gn = jnp.minimum(gi + 1, n_all - 1)
        helping_n, target_n, grp_n, _ = place_of(gn)
        slot_n = lax.rem(gi + 1, SLOTS)

        @pl.when((gi == n_own - 2) & (me == 3))
        def _():
            for c in query_copies(me):
                c.wait_recv()
            turn(1)

        @pl.when((gi == n_own - 2) & (me == 0))
        def _():
            for c in query_halves()[1:] + (query_relay(),):
                c.wait_recv()
            turn(1)

        fresh = jnp.where(me == 0, gi == n_own - 1, gi == 0)

        def one(i, carry):
            blk = block_at(helping, target, i)
            more = i < target
            blk_n = jnp.where(more, block_at(helping, target, i + 1), block_at(helping_n, target_n, 0))

            @pl.when(fresh & more)
            def _():
                received(blk_n)

                @pl.when((me >= 2) & (blk_n == 3 - me))
                def _():
                    start(forward_copies(blk_n))

            @pl.when((gi == 0) & (me == 2) & (i == 0))
            def _():
                query_halves()[0].wait_recv()
                query_relay().start()
                start(latent_copies(me, 0))

            new = (slot, blk, (i == target).astype(jnp.int32), gi)

            def next_keys():
                keys_and_values(jnp.where(more, slot, slot_n), jnp.where(more, grp, grp_n) * GROUP, blk_n)

            def after_own():
                queries(lax.rem(gi + 1, 2), helping_n.astype(jnp.int32), grp_n * GROUP)
                next_keys()
                clear(slot_n)

            @pl.when(blk == target)
            def _():
                step(carry, new, True, after_own)

            @pl.when(blk != target)
            def _():
                step(carry, new, False, next_keys)

            return new, carry[0]

        return lax.fori_loop(0, target + 1, one, carry)

    idle = (jnp.int32(SLOTS), jnp.int32(0), jnp.int32(0), jnp.int32(0))
    queries(0, 0, 0)

    @pl.when(me >= 0)
    def _():
        keys_and_values(0, 0, me)
        clear(0)

    carry = lax.fori_loop(0, n_all, group, (idle, idle))
    step(carry, None, False)
    step((idle, carry[0]), None, False, values_only=True)

    @pl.when(me == 1)
    def _():
        help_detour().wait_recv()
        help_relay().start()
        help_relay().wait_send()

    def sent(copies):
        for c in copies:
            c.wait_send()

    @pl.when(me == 0)
    def _():
        sent(latent_copies(me, 1) + latent_copies(me, 3))

    @pl.when(me == 1)
    def _():
        sent(latent_copies(me, 2) + latent_copies(me, 0))

    @pl.when(me == 2)
    def _():
        sent(latent_copies(me, 3) + latent_copies(me, 0) + forward_copies(1) + query_copies(3) + (query_relay(),))

    @pl.when(me == 3)
    def _():
        sent(latent_copies(me, 0) + forward_copies(0) + query_halves())

    for k in range(MOST_HELPED):
        @pl.when(k < helped)
        def _():
            for part in range(2):
                help_half(k, part, partner).wait_send()

        @pl.when(k < given)
        def _():
            grp = n_own + k
            for part in range(2):
                remote(half_at(grp, part), half_at(grp, part), o_send.at[k, part], o_recv.at[grp, part], me).wait_recv()
            output_copy(grp).start()

    for grp in range(ngroup):
        output_copy(grp).wait()


def layer(pos, gq, gkv, x, wdkv, wdq, wuq, wuk, wuv, scale2, heads, groups):
    rows, dim = x.shape
    rank = gkv.shape[0]
    rot = wdkv.shape[0] - rank
    qrank = wdq.shape[1]
    nope = wuk.shape[0] // heads
    vdim = wuv.shape[0] // heads
    seq = rows * groups
    vm = pl.BlockSpec(memory_space=pltpu.VMEM)
    anym = pl.BlockSpec(memory_space=pl.ANY)
    f32 = jnp.float32
    bf16 = jnp.bfloat16
    dma = pltpu.SemaphoreType.DMA
    nhelp = MOST_HELPED
    return pl.pallas_call(
        functools.partial(layer_kernel, scale2=scale2, rows=rows, nope=nope, rot=rot, vdim=vdim, heads=heads, groups=groups),
        out_shape=(jax.ShapeDtypeStruct((heads // 2, rows, 2 * vdim), bf16),
                   jax.ShapeDtypeStruct((rows, rank), bf16),
                   jax.ShapeDtypeStruct((rot, rows), bf16)),
        in_specs=[vm, vm, vm] + [anym] * 6,
        out_specs=(anym, vm, vm),
        scratch_shapes=[
            pltpu.VMEM(x.shape, bf16),
            pltpu.VMEM(wdkv.shape, bf16),
            pltpu.VMEM(wdq.shape, bf16),
            pltpu.VMEM(wuq.shape, bf16),
            pltpu.VMEM(wuk.shape, bf16),
            pltpu.VMEM(wuv.shape, bf16),
            pltpu.VMEM((2, rows, qrank), bf16),
            pltpu.VMEM((2, 8, rows), f32),
            pltpu.VMEM((2, rot, rows), f32),
            pltpu.VMEM((groups, rows, rank), bf16),
            pltpu.VMEM((groups, rot, rows), bf16),
            pltpu.VMEM((groups, rows, 128), bf16),
            pltpu.VMEM((2, GROUP, 256, rows), bf16),
            pltpu.VMEM((GROUP // 2, seq, 128), bf16),
            pltpu.VMEM((SLOTS * GROUP, vdim + 16, seq), bf16),
            pltpu.VMEM((GROUP, rows, rows), f32),
            pltpu.VMEM((GROUP, 1, rows), f32),
            pltpu.VMEM((GROUP, rows, rows), bf16),
            pltpu.VMEM((GROUP, 1, rows), f32),
            pltpu.VMEM(((SLOTS + 1) * GROUP, 1, rows), f32),
            pltpu.VMEM(((SLOTS + 1) * GROUP, vdim + 16, rows), f32),
            pltpu.VMEM((heads // 2, rows, 2 * vdim), bf16),
            pltpu.VMEM((nhelp, GROUP // 2, rows, 2 * vdim), bf16),
            dma((6,)),
            dma((groups,)), dma((groups,)), dma((groups,)), dma((groups,)), dma((2,)),
            dma((3,)), dma((3,)), dma, dma,
            dma((nhelp, 2)), dma((heads // GROUP, 2)),
            dma((heads // GROUP,)),
        ],
        compiler_params=pltpu.CompilerParams(vmem_limit_bytes=62 * 1024 * 1024, collective_id=0, has_side_effects=True),
        cost_estimate=pl.CostEstimate(flops=40_000_000_000, bytes_accessed=40_000_000, transcendentals=30_000_000),
    )(pos, gq, gkv, x, wdkv, wdq, wuq, wuk, wuv)


def project_kernel(ckv_ref, cpe_ref, o_hbm, w_hbm, out_hbm, ckv_out, cpe_out, o, w, total, out, o_sem, w_sem, out_sem, *, tile):
    f32 = jnp.float32
    npair = o.shape[0]
    depth, dim = w.shape
    parts = dim // tile
    deep = depth // parts
    per = npair // parts

    def cut(i):
        return pl.ds(i * tile, tile)

    o_copies = [pltpu.make_async_copy(o_hbm.at[pl.ds(i * per, per)], o.at[pl.ds(i * per, per)], o_sem.at[i]) for i in range(parts)]
    w_copies = [pltpu.make_async_copy(w_hbm.at[pl.ds(i * deep, deep)], w.at[pl.ds(i * deep, deep)], w_sem.at[i]) for i in range(parts)]
    out_copies = [pltpu.make_async_copy(out.at[:, cut(i)], out_hbm.at[:, cut(i)], out_sem.at[i]) for i in range(parts)]
    def fetch(i):
        if i < parts:
            o_copies[i].start()
            w_copies[i].start()

    fetch(0)
    ckv_out[...] = ckv_ref[...]
    cpe_out[...] = cpe_ref[...]
    for i in range(parts):
        o_copies[i].wait()
        w_copies[i].wait()
        if i == 0:
            fetch(1)
        fetch(i + 2)
        lhs = jnp.concatenate([o[i * per + j] for j in range(per)], axis=1)
        for n in range(parts):
            t = jnp.dot(lhs, w[i * deep:(i + 1) * deep, cut(n)], preferred_element_type=f32)
            if i > 0:
                t = t + total[:, cut(n)]
            if i < parts - 1:
                total[:, cut(n)] = t
            else:
                out[:, cut(n)] = t.astype(out.dtype)
                out_copies[n].start()
    for c in out_copies:
        c.wait()


def project(o, ckv, cpe, w):
    npair, rows, width = o.shape
    dim = w.shape[1]
    tile = 512
    parts = dim // tile
    bf16 = jnp.bfloat16
    vm = pl.BlockSpec(memory_space=pltpu.VMEM)
    anym = pl.BlockSpec(memory_space=pl.ANY)
    dma = pltpu.SemaphoreType.DMA
    return pl.pallas_call(
        functools.partial(project_kernel, tile=tile),
        in_specs=[vm, vm, anym, anym],
        out_specs=(anym, vm, vm),
        out_shape=(jax.ShapeDtypeStruct((rows, dim), bf16), jax.ShapeDtypeStruct(ckv.shape, ckv.dtype), jax.ShapeDtypeStruct(cpe.shape, cpe.dtype)),
        scratch_shapes=[pltpu.VMEM(o.shape, bf16), pltpu.VMEM(w.shape, bf16), pltpu.VMEM((rows, dim), jnp.float32), pltpu.VMEM((rows, dim), bf16),
                        dma((parts,)), dma((parts,)), dma((parts,))],
        compiler_params=pltpu.CompilerParams(vmem_limit_bytes=62 * 1024 * 1024),
        cost_estimate=pl.CostEstimate(flops=2 * rows * dim * w.shape[0], bytes_accessed=2 * w.size, transcendentals=0),
    )(ckv, cpe, o, w)


def solution(mesh):
    groups = mesh.shape['sp']
    tok_spec = P(('dp', 'sp'))
    rows_spec = P(('dp', 'sp'), None)
    replicated = P()

    def local_step(tok_in, tok_pos, w_dq, g_q, w_uq, w_dkv, g_kv, w_uk, w_uv, w_o):
        heads, qk_dim = w_uq.shape[1:]
        kv_rank = g_kv.shape[0]
        rot_dim = w_dkv.shape[1] - kv_rank
        v_dim = w_uv.shape[2]
        attn_scale = (0.1 * math.log(YARN_FACTOR) + 1.0) ** 2 / math.sqrt(qk_dim)
        def flat(w):
            return jnp.transpose(w, (1, 2, 0)).reshape(-1, w.shape[0])

        o, ckv, cpe = layer(tok_pos, g_q, g_kv, tok_in, w_dkv.T, w_dq, flat(w_uq), flat(w_uk), flat(w_uv),
                                      attn_scale * math.log2(math.e), heads, groups)
        attn_out, cache_kv, cache_pe = project(o, ckv, cpe, w_o.reshape(heads * v_dim, -1))
        return attn_out, cache_kv, cache_pe.T

    return jax.shard_map(local_step, mesh=mesh, in_specs=(rows_spec, tok_spec, replicated, replicated, replicated, replicated, replicated, replicated, replicated, replicated), out_specs=(rows_spec, rows_spec, rows_spec), check_vma=False)
```

```python
import functools
import math
import jax
import jax.numpy as jnp
from jax import lax
from jax.experimental import pallas as pl
from jax.experimental.pallas import tpu as pltpu
from jax.sharding import PartitionSpec as P

ROPE_THETA = 10000.0
YARN_FACTOR = 40.0
ORIG_CTX = 4096.0
BETA_FAST = 32.0
BETA_SLOW = 1.0
NORM_EPS = 1e-6


def rope_freqs(rot_dim):
    half_dim = rot_dim // 2
    log_base = 2.0 * math.log(ROPE_THETA)
    low_idx = max(math.floor(rot_dim * math.log(ORIG_CTX / (BETA_FAST * 2.0 * math.pi)) / log_base), 0)
    high_idx = min(math.ceil(rot_dim * math.log(ORIG_CTX / (BETA_SLOW * 2.0 * math.pi)) / log_base), half_dim - 1)
    spread = max(high_idx - low_idx, 0.001)
    freq_list = []
    for freq_idx in range(half_dim):
        base_freq = ROPE_THETA ** (-2.0 * freq_idx / rot_dim)
        ramp_val = min(max((freq_idx - low_idx) / spread, 0.0), 1.0)
        freq_list.append(base_freq / YARN_FACTOR * ramp_val + base_freq * (1.0 - ramp_val))
    return freq_list


GROUP = 8
SLOTS = 3


def layer_kernel(pos_ref, gq_ref, gkv_ref, x_hbm, wdkv_hbm, wdq_hbm, wuq_hbm, wuk_hbm, wuv_hbm,
                 o_hbm, ckv_out, cpe_out,
                 x, wdkv, wdq, wuq, wuk, wuv, qlat, posf, trig, ckv, pet, pen, qaug, kn, vt,
                 s_buf, c_buf, p_buf, al_buf, m_s, acc, o_nat, o_help,
                 load_sem, c_send, c_recv, pe_send, pe_recv, f_send, q_send, q_recv, t_send, t_recv, o_send, o_recv, out_sem,
                 *, scale2, rows, nope, rot, vdim, heads, groups):
    f32 = jnp.float32
    bf16 = jnp.bfloat16
    NT = (((1,), (1,)), ((), ()))
    NN = (((1,), (0,)), ((), ()))
    half = rows // 2
    qk = nope + rot
    pairs = GROUP // 2
    ngroup = heads // GROUP
    me = lax.axis_index('sp')
    given = jnp.where(me == 3, 2, jnp.where(me == 2, 1, 0))
    helped = jnp.where(me == 2, 0, 1)
    partner = jnp.where(me == 3, 2, 3)
    help_group = jnp.where(me == 1, 3, 4)
    help_turn = jnp.where(me == 2, 2 * ngroup, jnp.where(me == 3, 2, 3))
    n_own = ngroup - given
    n_all = n_own + helped

    loads = [pltpu.make_async_copy(s, d, load_sem.at[i]) for i, (s, d) in enumerate(
        ((x_hbm, x), (wdkv_hbm, wdkv), (wdq_hbm, wdq), (wuq_hbm, wuq), (wuk_hbm, wuk), (wuv_hbm, wuv)))]
    for c in loads[:3]:
        c.start()
    barrier = pltpu.get_barrier_semaphore()
    for d in range(1, groups):
        pl.semaphore_signal(barrier, inc=1, device_id={'sp': lax.rem(me + d, groups)}, device_id_type=pl.DeviceIdType.MESH)

    def remote(s, d, ssem, rsem, to):
        return pltpu.make_async_remote_copy(src_ref=s, dst_ref=d, send_sem=ssem, recv_sem=rsem,
                                            device_id={'sp': to}, device_id_type=pl.DeviceIdType.MESH)

    def latent_copies(origin, to):
        return (remote(ckv.at[origin], ckv.at[origin], c_send.at[to], c_recv.at[origin], to),
                remote(pet.at[origin], pet.at[origin], pe_send.at[to], pe_recv.at[origin], to))

    def forward_copies(origin):
        to = 5 - me
        return (remote(ckv.at[origin], ckv.at[origin], f_send.at[0], c_recv.at[origin], to),
                remote(pet.at[origin], pet.at[origin], f_send.at[1], pe_recv.at[origin], to))

    def query_copies(to):
        return (remote(qlat.at[0], qlat.at[1], q_send.at[0], q_recv.at[0], to),
                remote(posf.at[0], posf.at[1], t_send, t_recv, to))

    def query_halves():
        top, low = pl.ds(0, half), pl.ds(half, half)
        return (remote(qlat.at[0, low], qlat.at[1, low], q_send.at[1], q_recv.at[1], 2),
                remote(posf.at[0], posf.at[1], t_send, t_recv, 0),
                remote(qlat.at[0, top], qlat.at[1, top], q_send.at[0], q_recv.at[0], 0))

    def query_relay():
        low = pl.ds(half, half)
        return remote(qlat.at[1, low], qlat.at[1, low], q_send.at[2], q_recv.at[2], 0)

    def query_share():
        return (remote(qlat.at[1], qlat.at[1], q_send.at[0], q_recv.at[0], 1),
                remote(posf.at[1], posf.at[1], t_send, t_recv, 1))

    def latent_share(origin):
        spare = 6 - 2 * origin
        return (remote(ckv.at[origin], ckv.at[origin], c_send.at[spare], c_recv.at[origin], 1),
                remote(pet.at[origin], pet.at[origin], pe_send.at[spare], pe_recv.at[origin], 1))

    def start(copies):
        for c in copies:
            c.start()

    def received(origin):
        for c in latent_copies(origin, me):
            c.wait_recv()
        unpack_rope(origin)

    def unpack_rope(origin):
        wide = jnp.concatenate([pet[origin].astype(f32), jnp.zeros((128 - rot, rows), f32)], axis=0)
        pen[origin] = wide.T.astype(bf16)

    hr = rot // 2

    def cols(i):
        return slice(i * half, (i + 1) * half)

    freq_i = lax.broadcasted_iota(jnp.int32, (hr, rows), 0)
    freq = jnp.zeros((hr, rows), f32)
    for i, f in enumerate(rope_freqs(rot)):
        freq = jnp.where(freq_i == i, f, freq)

    def turn(i):
        angle = posf[i, :1] * freq
        trig[i, :hr] = jnp.cos(angle)
        trig[i, hr:] = jnp.sin(angle)

    posf[0] = jnp.broadcast_to(pos_ref[...].astype(f32).reshape(1, rows), (8, rows))
    turn(0)
    cos_t, sin_t = trig[0, :hr], trig[0, hr:]
    qaug[...] = jnp.zeros_like(qaug)
    vt[:, vdim:, :] = jnp.ones((vt.shape[0], vt.shape[1] - vdim, vt.shape[2]), vt.dtype)
    acc[...] = jnp.zeros_like(acc)
    loads[0].wait()
    loads[1].wait()
    for c in loads[3:]:
        c.start()
    kvt = lax.dot_general(wdkv[...], x[...], NT, preferred_element_type=f32)
    rank = ckv.shape[2]
    a = kvt[:rank]
    norm = a * lax.rsqrt(jnp.sum(a * a, axis=0, keepdims=True) / rank + NORM_EPS)
    c_own = (norm.T * gkv_ref[...].reshape(1, rank)).astype(bf16)
    ckv[me] = c_own
    ckv_out[...] = c_own
    z1, z2 = kvt[rank:rank + hr], kvt[rank + hr:]
    pe_own = jnp.concatenate([z1 * cos_t - z2 * sin_t, z2 * cos_t + z1 * sin_t], axis=0).astype(bf16)
    pet[me] = pe_own
    cpe_out[...] = pe_own
    loads[2].wait()
    qrank = wdq.shape[1]

    def query_latent(part):
        ql = lax.dot_general(x[cols(part)], wdq[...], NN, preferred_element_type=f32)
        ql = ql * lax.rsqrt(jnp.sum(ql * ql, axis=1, keepdims=True) / qrank + NORM_EPS) * gq_ref[...].reshape(1, qrank)
        qlat[0, cols(part)] = ql.astype(bf16)

    query_latent(0)
    pl.semaphore_wait(barrier, groups - 1)

    @pl.when(me == 0)
    def _():
        for t in (1, 3):
            start(latent_copies(me, t))

    @pl.when(me == 1)
    def _():
        for t in (2, 0):
            start(latent_copies(me, t))

    @pl.when(me == 2)
    def _():
        start(latent_copies(me, 3))

    query_latent(1)
    unpack_rope(me)
    for c in loads[3:]:
        c.wait()

    @pl.when(me == 2)
    def _():
        start(query_copies(3))

    @pl.when(me == 3)
    def _():
        start(query_halves())
        start(latent_copies(me, 0))

    FULL = ((0, 0), (1, 0), (0, 1), (1, 1))
    OWN = ((0, 0), (0, 1), (1, 1))
    row_i = lax.broadcasted_iota(jnp.int32, (half, half), 0)
    col_i = lax.broadcasted_iota(jnp.int32, (half, half), 1)

    def score_stage(u, blk, own, gi):
        tops = [None, None]

        def place(s, k, i):
            s_buf[u, cols(k), cols(i)] = s
            top = jnp.max(s, axis=0, keepdims=True)
            tops[i] = top if tops[i] is None else jnp.maximum(tops[i], top)

        def dot(k0, k1, i0, i1):
            lhs = jnp.concatenate([kn[u // 2, pl.ds(pl.multiple_of(blk * rows + k0 * half, half), (k1 - k0) * half), :],
                                   pen[blk, k0 * half:k1 * half, :]], axis=1)
            return lax.dot_general(lhs, qaug[lax.rem(gi, 2), u, :, i0 * half:i1 * half], NN, preferred_element_type=f32)

        if own:
            s = dot(0, 1, 0, 2)
            place(jnp.where(row_i <= col_i, s[:, :half], -jnp.inf), 0, 0)
            place(s[:, half:], 0, 1)
            place(jnp.where(row_i <= col_i, dot(1, 2, 1, 2), -jnp.inf), 1, 1)
            s_buf[u, cols(1), cols(0)] = jnp.full((half, half), -jnp.inf, f32)
        else:
            s = dot(0, 2, 0, 2)
            for k, i in FULL:
                place(s[cols(k), cols(i)], k, i)
        for i in range(2):
            c_buf[u, :, cols(i)] = tops[i]

    def exp_stage(u, slot):
        h = slot * GROUP + u
        m_old = m_s[h]
        m_new = jnp.maximum(m_old, c_buf[u])
        al_buf[u] = jnp.exp2((m_old - m_new) * scale2)
        m_s[h] = m_new
        for k, i in FULL:
            p_buf[u, cols(k), cols(i)] = jnp.exp2((s_buf[u, cols(k), cols(i)] - m_new[:, cols(i)]) * scale2).astype(bf16)

    def value_stage(u, slot, blk):
        h = slot * GROUP + u
        v = vt[jnp.minimum(slot, SLOTS - 1) * GROUP + u, :, pl.ds(pl.multiple_of(blk * rows, rows), rows)]
        for i in range(2):
            t = lax.dot_general(v, p_buf[u, :, cols(i)], NN, preferred_element_type=f32)
            acc[h, :, cols(i)] = t + acc[h, :, cols(i)] * al_buf[u, :, cols(i)]

    def place_of(gi):
        helping = gi == help_turn
        target = jnp.where(helping, partner, me)
        grp = jnp.where(helping, help_group, gi - (gi > help_turn).astype(jnp.int32))
        return helping, target, grp, lax.rem(gi, SLOTS)

    def output_copy(grp):
        return pltpu.make_async_copy(o_nat.at[pl.ds(grp * pairs, pairs)], o_hbm.at[pl.ds(grp * pairs, pairs)], out_sem.at[grp])

    def help_copy(grp, to):
        return remote(o_help, o_nat.at[pl.ds(grp * pairs, pairs)], o_send, o_recv.at[grp], to)

    def finish(slot, gi):
        outs = []
        for j in range(pairs):
            t = jnp.concatenate([acc[slot * GROUP + h, :vdim, :] / acc[slot * GROUP + h, vdim:vdim + 1, :] for h in (2 * j, 2 * j + 1)], axis=0)
            outs.append(t.T.astype(bf16))
        for h in range(GROUP):
            acc[slot * GROUP + h] = jnp.zeros(acc.shape[1:], f32)

        helping, _, grp, _ = place_of(gi)

        @pl.when(jnp.logical_not(helping))
        def _():
            for j in range(pairs):
                o_nat[grp * pairs + j] = outs[j]
            output_copy(grp).start()

        @pl.when(helping)
        def _():
            for j in range(pairs):
                o_help[j] = outs[j]
            help_copy(help_group, partner).start()

    def step(carry, new, own, after=None, values_only=False):
        (slot1, _, _, _), (slot2, blk2, last2, gi2) = carry
        for u in range(GROUP):
            value_stage(u, slot2, blk2)
            if not values_only:
                exp_stage(u, slot1)
            if new is not None:
                score_stage(u, new[1], own, new[3])
        if after is not None:
            after()

        @pl.when(last2 == 1)
        def _():
            finish(slot2, gi2)

    def keys_and_values(slot, head0, blk):
        c = ckv[blk]
        at = pl.multiple_of(blk * rows, rows)
        for j in range(GROUP // 4):
            wk = wuk[pl.ds(pl.multiple_of((head0 + 4 * j) * nope, 4 * nope), 4 * nope), :]
            kk = lax.dot_general(c, wk, NT, preferred_element_type=f32).astype(bf16)
            kn[2 * j, pl.ds(at, rows), :] = kk[:, :128]
            kn[2 * j + 1, pl.ds(at, rows), :] = kk[:, 128:]
            wv = wuv[pl.ds(pl.multiple_of((head0 + 4 * j) * vdim, 4 * vdim), 4 * vdim), :]
            vv = lax.dot_general(wv, c, NT, preferred_element_type=f32).astype(bf16)
            for i in range(4):
                vt[slot * GROUP + 4 * j + i, :vdim, pl.ds(at, rows)] = vv[i * vdim:(i + 1) * vdim, :]

    def queries(buf, src, head0):
        ct, st = trig[src, :hr], trig[src, hr:]
        for j in range(GROUP // 4):
            w = wuq[pl.ds(pl.multiple_of((head0 + 4 * j) * qk, 4 * qk), 4 * qk), :]
            q = lax.dot_general(w, qlat[src], NT, preferred_element_type=f32)
            for i in range(4):
                u = 4 * j + i
                qh = q[i * qk:(i + 1) * qk]
                lo = (u % 2) * nope
                qaug[buf, u, lo:lo + nope, :] = qh[:nope].astype(bf16)
                r1, r2 = qh[nope:nope + hr], qh[nope + hr:]
                qaug[buf, u, 2 * nope:2 * nope + rot, :] = jnp.concatenate([r1 * ct - r2 * st, r2 * ct + r1 * st], axis=0).astype(bf16)

    def clear(slot):
        for u in range(GROUP):
            m_s[slot * GROUP + u] = jnp.full((1, rows), -jnp.inf, f32)

    def block_at(helping, target, i):
        usual = jnp.where(i == 0, target, lax.rem(i + target - 2, jnp.maximum(target, 1)))
        return jnp.where(helping & (me < 2), jnp.where(i < 2, i, 5 - i), usual)

    def group(gi, carry):
        helping, target, grp, slot = place_of(gi)
        gn = jnp.minimum(gi + 1, n_all - 1)
        helping_n, target_n, grp_n, _ = place_of(gn)
        slot_n = lax.rem(gi + 1, SLOTS)

        @pl.when((gi == help_turn - 1) & ((me == 1) | (me == 3)))
        def _():
            for c in query_copies(me):
                c.wait_recv()
            turn(1)

        @pl.when((gi == help_turn - 1) & (me == 0))
        def _():
            for c in query_halves()[1:] + (query_relay(),):
                c.wait_recv()
            start(query_share())
            turn(1)

        fresh = ((gi == 0) & (me > 0)) | (helping & (me < 2))

        def one(i, carry):
            blk = block_at(helping, target, i)
            more = i < target
            blk_n = jnp.where(more, block_at(helping, target, i + 1), block_at(helping_n, target_n, 0))

            @pl.when(fresh & more & (blk_n != me))
            def _():
                received(blk_n)

                @pl.when((me >= 2) & (blk_n == 3 - me))
                def _():
                    start(forward_copies(blk_n))

                @pl.when((me == 0) & (blk_n >= 2))
                def _():
                    start(latent_share(blk_n))

            @pl.when((gi == 0) & (me == 2) & (i == 0))
            def _():
                query_halves()[0].wait_recv()
                query_relay().start()
                start(latent_copies(me, 0))

            new = (slot, blk, (i == target).astype(jnp.int32), gi)

            def next_keys():
                keys_and_values(jnp.where(more, slot, slot_n), jnp.where(more, grp, grp_n) * GROUP, blk_n)

            def after_own():
                queries(lax.rem(gi + 1, 2), helping_n.astype(jnp.int32), grp_n * GROUP)
                next_keys()
                clear(slot_n)

            @pl.when(blk == target)
            def _():
                step(carry, new, True, after_own)

            @pl.when(blk != target)
            def _():
                step(carry, new, False, next_keys)

            return new, carry[0]

        return lax.fori_loop(0, target + 1, one, carry)

    idle = (jnp.int32(SLOTS), jnp.int32(0), jnp.int32(0), jnp.int32(0))
    queries(0, 0, 0)

    @pl.when(me >= 0)
    def _():
        keys_and_values(0, 0, me)
        clear(0)

    carry = lax.fori_loop(0, n_all, group, (idle, idle))
    step(carry, None, False)
    step((idle, carry[0]), None, False, values_only=True)

    def sent(copies):
        for c in copies:
            c.wait_send()

    @pl.when(me == 0)
    def _():
        sent(latent_copies(me, 1) + latent_copies(me, 3) + query_share() + latent_share(2) + latent_share(3))

    @pl.when(me == 1)
    def _():
        sent(latent_copies(me, 2) + latent_copies(me, 0))

    @pl.when(me == 2)
    def _():
        sent(latent_copies(me, 3) + latent_copies(me, 0) + forward_copies(1) + query_copies(3) + (query_relay(),))

    @pl.when(me == 3)
    def _():
        sent(latent_copies(me, 0) + forward_copies(0) + query_halves())

    @pl.when(helped > 0)
    def _():
        help_copy(help_group, partner).wait_send()

    for k in range(2):
        @pl.when(k < given)
        def _():
            help_copy(n_own + k, me).wait_recv()
            output_copy(n_own + k).start()

    for grp in range(ngroup):
        output_copy(grp).wait()


def layer(pos, gq, gkv, x, wdkv, wdq, wuq, wuk, wuv, scale2, heads, groups):
    rows, dim = x.shape
    rank = gkv.shape[0]
    rot = wdkv.shape[0] - rank
    qrank = wdq.shape[1]
    nope = wuk.shape[0] // heads
    vdim = wuv.shape[0] // heads
    seq = rows * groups
    vm = pl.BlockSpec(memory_space=pltpu.VMEM)
    anym = pl.BlockSpec(memory_space=pl.ANY)
    f32 = jnp.float32
    bf16 = jnp.bfloat16
    dma = pltpu.SemaphoreType.DMA
    return pl.pallas_call(
        functools.partial(layer_kernel, scale2=scale2, rows=rows, nope=nope, rot=rot, vdim=vdim, heads=heads, groups=groups),
        out_shape=(jax.ShapeDtypeStruct((heads // 2, rows, 2 * vdim), bf16),
                   jax.ShapeDtypeStruct((rows, rank), bf16),
                   jax.ShapeDtypeStruct((rot, rows), bf16)),
        in_specs=[vm, vm, vm] + [anym] * 6,
        out_specs=(anym, vm, vm),
        scratch_shapes=[
            pltpu.VMEM(x.shape, bf16),
            pltpu.VMEM(wdkv.shape, bf16),
            pltpu.VMEM(wdq.shape, bf16),
            pltpu.VMEM(wuq.shape, bf16),
            pltpu.VMEM(wuk.shape, bf16),
            pltpu.VMEM(wuv.shape, bf16),
            pltpu.VMEM((2, rows, qrank), bf16),
            pltpu.VMEM((2, 8, rows), f32),
            pltpu.VMEM((2, rot, rows), f32),
            pltpu.VMEM((groups, rows, rank), bf16),
            pltpu.VMEM((groups, rot, rows), bf16),
            pltpu.VMEM((groups, rows, 128), bf16),
            pltpu.VMEM((2, GROUP, 256, rows), bf16),
            pltpu.VMEM((GROUP // 2, seq, 128), bf16),
            pltpu.VMEM((SLOTS * GROUP, vdim + 16, seq), bf16),
            pltpu.VMEM((GROUP, rows, rows), f32),
            pltpu.VMEM((GROUP, 1, rows), f32),
            pltpu.VMEM((GROUP, rows, rows), bf16),
            pltpu.VMEM((GROUP, 1, rows), f32),
            pltpu.VMEM(((SLOTS + 1) * GROUP, 1, rows), f32),
            pltpu.VMEM(((SLOTS + 1) * GROUP, vdim + 16, rows), f32),
            pltpu.VMEM((heads // 2, rows, 2 * vdim), bf16),
            pltpu.VMEM((GROUP // 2, rows, 2 * vdim), bf16),
            dma((6,)),
            dma((groups,)), dma((groups,)), dma((groups,)), dma((groups,)), dma((2,)),
            dma((3,)), dma((3,)), dma, dma,
            dma, dma((heads // GROUP,)),
            dma((heads // GROUP,)),
        ],
        compiler_params=pltpu.CompilerParams(vmem_limit_bytes=62 * 1024 * 1024, collective_id=0, has_side_effects=True),
        cost_estimate=pl.CostEstimate(flops=40_000_000_000, bytes_accessed=40_000_000, transcendentals=30_000_000),
    )(pos, gq, gkv, x, wdkv, wdq, wuq, wuk, wuv)


def project_kernel(ckv_ref, cpe_ref, o_hbm, w_hbm, out_hbm, ckv_out, cpe_out, o, w, total, out, o_sem, w_sem, out_sem, *, tile):
    f32 = jnp.float32
    npair = o.shape[0]
    depth, dim = w.shape
    parts = dim // tile
    deep = depth // parts
    per = npair // parts

    def cut(i):
        return pl.ds(i * tile, tile)

    o_copies = [pltpu.make_async_copy(o_hbm.at[pl.ds(i * per, per)], o.at[pl.ds(i * per, per)], o_sem.at[i]) for i in range(parts)]
    fine = deep // 4
    w_copies = [[pltpu.make_async_copy(w_hbm.at[pl.ds(i * deep + j * fine, fine)], w.at[pl.ds(i * deep + j * fine, fine)], w_sem.at[i, j])
                 for j in range(4)] for i in range(parts)]
    out_copies = [pltpu.make_async_copy(out.at[:, cut(i)], out_hbm.at[:, cut(i)], out_sem.at[i]) for i in range(parts)]
    for i in range(parts):
        o_copies[i].start()
        for c in w_copies[i]:
            c.start()
    ckv_out[...] = ckv_ref[...]
    cpe_out[...] = cpe_ref[...]
    for i in range(parts):
        o_copies[i].wait()
        for c in w_copies[i]:
            c.wait()
        lhs = jnp.concatenate([o[i * per + j] for j in range(per)], axis=1)
        for n in range(parts):
            t = jnp.dot(lhs, w[i * deep:(i + 1) * deep, cut(n)], preferred_element_type=f32)
            if i > 0:
                t = t + total[:, cut(n)]
            if i < parts - 1:
                total[:, cut(n)] = t
            else:
                out[:, cut(n)] = t.astype(out.dtype)
                out_copies[n].start()
    for c in out_copies:
        c.wait()


def project(o, ckv, cpe, w):
    npair, rows, width = o.shape
    dim = w.shape[1]
    tile = 512
    parts = dim // tile
    bf16 = jnp.bfloat16
    vm = pl.BlockSpec(memory_space=pltpu.VMEM)
    anym = pl.BlockSpec(memory_space=pl.ANY)
    dma = pltpu.SemaphoreType.DMA
    return pl.pallas_call(
        functools.partial(project_kernel, tile=tile),
        in_specs=[vm, vm, anym, anym],
        out_specs=(anym, vm, vm),
        out_shape=(jax.ShapeDtypeStruct((rows, dim), bf16), jax.ShapeDtypeStruct(ckv.shape, ckv.dtype), jax.ShapeDtypeStruct(cpe.shape, cpe.dtype)),
        scratch_shapes=[pltpu.VMEM(o.shape, bf16), pltpu.VMEM(w.shape, bf16), pltpu.VMEM((rows, dim), jnp.float32), pltpu.VMEM((rows, dim), bf16),
                        dma((parts,)), dma((parts, 4)), dma((parts,))],
        compiler_params=pltpu.CompilerParams(vmem_limit_bytes=62 * 1024 * 1024),
        cost_estimate=pl.CostEstimate(flops=2 * rows * dim * w.shape[0], bytes_accessed=2 * w.size, transcendentals=0),
    )(ckv, cpe, o, w)


def solution(mesh):
    groups = mesh.shape['sp']
    tok_spec = P(('dp', 'sp'))
    rows_spec = P(('dp', 'sp'), None)
    replicated = P()

    def local_step(tok_in, tok_pos, w_dq, g_q, w_uq, w_dkv, g_kv, w_uk, w_uv, w_o):
        heads, qk_dim = w_uq.shape[1:]
        kv_rank = g_kv.shape[0]
        rot_dim = w_dkv.shape[1] - kv_rank
        v_dim = w_uv.shape[2]
        attn_scale = (0.1 * math.log(YARN_FACTOR) + 1.0) ** 2 / math.sqrt(qk_dim)
        def flat(w):
            return jnp.transpose(w, (1, 2, 0)).reshape(-1, w.shape[0])

        o, ckv, cpe = layer(tok_pos, g_q, g_kv, tok_in, w_dkv.T, w_dq, flat(w_uq), flat(w_uk), flat(w_uv),
                                      attn_scale * math.log2(math.e), heads, groups)
        attn_out, cache_kv, cache_pe = project(o, ckv, cpe, w_o.reshape(heads * v_dim, -1))
        return attn_out, cache_kv, cache_pe.T

    return jax.shard_map(local_step, mesh=mesh, in_specs=(rows_spec, tok_spec, replicated, replicated, replicated, replicated, replicated, replicated, replicated, replicated), out_specs=(rows_spec, rows_spec, rows_spec), check_vma=False)
```

```python
import functools
import math
import jax
import jax.numpy as jnp
from jax import lax
from jax.experimental import pallas as pl
from jax.experimental.pallas import tpu as pltpu
from jax.sharding import PartitionSpec as P

ROPE_THETA = 10000.0
YARN_FACTOR = 40.0
ORIG_CTX = 4096.0
BETA_FAST = 32.0
BETA_SLOW = 1.0
NORM_EPS = 1e-6


def rope_freqs(rot_dim):
    half_dim = rot_dim // 2
    log_base = 2.0 * math.log(ROPE_THETA)
    low_idx = max(math.floor(rot_dim * math.log(ORIG_CTX / (BETA_FAST * 2.0 * math.pi)) / log_base), 0)
    high_idx = min(math.ceil(rot_dim * math.log(ORIG_CTX / (BETA_SLOW * 2.0 * math.pi)) / log_base), half_dim - 1)
    spread = max(high_idx - low_idx, 0.001)
    freq_list = []
    for freq_idx in range(half_dim):
        base_freq = ROPE_THETA ** (-2.0 * freq_idx / rot_dim)
        ramp_val = min(max((freq_idx - low_idx) / spread, 0.0), 1.0)
        freq_list.append(base_freq / YARN_FACTOR * ramp_val + base_freq * (1.0 - ramp_val))
    return freq_list


GROUP = 8
SLOTS = 3
LAYER_VMEM = 65500000


def layer_kernel(pos_ref, gq_ref, gkv_ref, x_hbm, wdkv_hbm, wdq_hbm, wuq_hbm, wuk_hbm, wuv_hbm, wo_hbm,
                 out_hbm, ckv_out, cpe_out,
                 wdkv, wo, wuq, wuk, wuv, qlat, posf, trig, ckv, pet, pen, qaug, kn, vt,
                 s_buf, c_buf, p_buf, al_buf, m_s, acc, o_nat, o_help,
                 load_sem, c_send, c_recv, pe_send, pe_recv, f_send, q_send, q_recv, t_send, t_recv, o_send, o_recv, wo_sem, out_sem,
                 *, scale2, rows, nope, rot, vdim, heads, groups):
    f32 = jnp.float32
    bf16 = jnp.bfloat16
    NT = (((1,), (1,)), ((), ()))
    NN = (((1,), (0,)), ((), ()))
    half = rows // 2
    qk = nope + rot
    pairs = GROUP // 2
    ngroup = heads // GROUP
    me = lax.axis_index('sp')
    given = jnp.where(me == 3, 2, jnp.where(me == 2, 1, 0))
    helped = jnp.where(me == 2, 0, 1)
    partner = jnp.where(me == 3, 2, 3)
    help_group = jnp.where(me == 1, 3, 4)
    help_turn = jnp.where(me == 2, 2 * ngroup, jnp.where(me == 3, 2, 3))
    n_own = ngroup - given
    n_all = n_own + helped

    tiles = x_hbm.shape[1] // rows
    x_loads = [pltpu.make_async_copy(x_hbm.at[:, pl.ds(i * rows, rows)], p_buf.at[i], load_sem.at[i]) for i in range(tiles)]
    qrank = wdq_hbm.shape[1]
    part = GROUP * qk
    w_loads = [pltpu.make_async_copy(s, d, load_sem.at[tiles + i]) for i, (s, d) in enumerate(
        ((wdkv_hbm, wdkv), (wdq_hbm, wo.at[:, pl.ds(0, qrank)]), (wuk_hbm, wuk), (wuv_hbm, wuv)))]
    uq_loads = [pltpu.make_async_copy(wuq_hbm.at[pl.ds(i * part, part)], wuq.at[pl.ds(i * part, part)], load_sem.at[tiles + 4 + i]) for i in range(ngroup)]
    wide = wo_hbm.shape[1] - qrank
    wo_loads = [pltpu.make_async_copy(wo_hbm.at[:, pl.ds(a, n)], wo.at[:, pl.ds(a, n)], wo_sem.at[i])
                for i, (a, n) in enumerate(((qrank, wide), (0, qrank)))]
    for c in x_loads + w_loads[:2]:
        c.start()
    barrier = pltpu.get_barrier_semaphore()
    for d in range(1, groups):
        pl.semaphore_signal(barrier, inc=1, device_id={'sp': lax.rem(me + d, groups)}, device_id_type=pl.DeviceIdType.MESH)

    def remote(s, d, ssem, rsem, to):
        return pltpu.make_async_remote_copy(src_ref=s, dst_ref=d, send_sem=ssem, recv_sem=rsem,
                                            device_id={'sp': to}, device_id_type=pl.DeviceIdType.MESH)

    def latent_copies(origin, to):
        return (remote(ckv.at[origin], ckv.at[origin], c_send.at[to], c_recv.at[origin], to),
                remote(pet.at[origin], pet.at[origin], pe_send.at[to], pe_recv.at[origin], to))

    def forward_copies(origin):
        to = 5 - me
        return (remote(ckv.at[origin], ckv.at[origin], f_send.at[0], c_recv.at[origin], to),
                remote(pet.at[origin], pet.at[origin], f_send.at[1], pe_recv.at[origin], to))

    def query_copies(to):
        return (remote(qlat.at[0], qlat.at[1], q_send.at[0], q_recv.at[0], to),
                remote(posf.at[0], posf.at[1], t_send, t_recv, to))

    def query_halves():
        top, low = pl.ds(0, half), pl.ds(half, half)
        return (remote(qlat.at[0, low], qlat.at[1, low], q_send.at[1], q_recv.at[1], 2),
                remote(posf.at[0], posf.at[1], t_send, t_recv, 0),
                remote(qlat.at[0, top], qlat.at[1, top], q_send.at[0], q_recv.at[0], 0))

    def query_relay():
        low = pl.ds(half, half)
        return remote(qlat.at[1, low], qlat.at[1, low], q_send.at[2], q_recv.at[2], 0)

    def query_share():
        return (remote(qlat.at[1], qlat.at[1], q_send.at[0], q_recv.at[0], 1),
                remote(posf.at[1], posf.at[1], t_send, t_recv, 1))

    def latent_share(origin):
        spare = 6 - 2 * origin
        return (remote(ckv.at[origin], ckv.at[origin], c_send.at[spare], c_recv.at[origin], 1),
                remote(pet.at[origin], pet.at[origin], pe_send.at[spare], pe_recv.at[origin], 1))

    def start(copies):
        for c in copies:
            c.start()

    def received(origin):
        for c in latent_copies(origin, me):
            c.wait_recv()
        unpack_rope(origin)

    def unpack_rope(origin):
        wide = jnp.concatenate([pet[origin].astype(f32), jnp.zeros((128 - rot, rows), f32)], axis=0)
        pen[origin] = wide.T.astype(bf16)

    hr = rot // 2

    def cols(i):
        return slice(i * half, (i + 1) * half)

    freq_i = lax.broadcasted_iota(jnp.int32, (hr, rows), 0)
    freq = jnp.zeros((hr, rows), f32)
    for i, f in enumerate(rope_freqs(rot)):
        freq = jnp.where(freq_i == i, f, freq)

    def turn(i):
        angle = posf[i, :1] * freq
        trig[i, :hr] = jnp.cos(angle)
        trig[i, hr:] = jnp.sin(angle)

    posf[0] = jnp.broadcast_to(pos_ref[...].astype(f32).reshape(1, rows), (8, rows))
    turn(0)
    cos_t, sin_t = trig[0, :hr], trig[0, hr:]
    qaug[...] = jnp.zeros_like(qaug)
    vt[:, vdim:, :] = jnp.ones((vt.shape[0], vt.shape[1] - vdim, vt.shape[2]), vt.dtype)
    acc[...] = jnp.zeros_like(acc)
    for c in x_loads + w_loads[:1]:
        c.wait()
    for c in uq_loads[:1] + w_loads[2:] + uq_loads[1:]:
        c.start()

    def x_rows(cut):
        return jnp.concatenate([p_buf[i, cut, :] for i in range(tiles)], axis=1)

    kvt = lax.dot_general(wdkv[...], x_rows(slice(0, rows)), NT, preferred_element_type=f32)
    rank = ckv.shape[2]
    a = kvt[:rank]
    norm = a * lax.rsqrt(jnp.sum(a * a, axis=0, keepdims=True) / rank + NORM_EPS)
    c_own = (norm.T * gkv_ref[...].reshape(1, rank)).astype(bf16)
    ckv[me] = c_own
    ckv_out[...] = c_own
    z1, z2 = kvt[rank:rank + hr], kvt[rank + hr:]
    pe_own = jnp.concatenate([z1 * cos_t - z2 * sin_t, z2 * cos_t + z1 * sin_t], axis=0).astype(bf16)
    pet[me] = pe_own
    cpe_out[...] = pe_own
    w_loads[1].wait()
    def query_latent(part):
        ql = lax.dot_general(x_rows(cols(part)), wo[:, :qrank], NN, preferred_element_type=f32)
        ql = ql * lax.rsqrt(jnp.sum(ql * ql, axis=1, keepdims=True) / qrank + NORM_EPS) * gq_ref[...].reshape(1, qrank)
        qlat[0, cols(part)] = ql.astype(bf16)

    query_latent(0)
    pl.semaphore_wait(barrier, groups - 1)

    @pl.when(me == 0)
    def _():
        for t in (1, 3):
            start(latent_copies(me, t))

    @pl.when(me == 1)
    def _():
        for t in (2, 0):
            start(latent_copies(me, t))

    @pl.when(me == 2)
    def _():
        start(latent_copies(me, 3))

    query_latent(1)
    unpack_rope(me)
    @pl.when(me == 2)
    def _():
        start(query_copies(3))

    @pl.when(me == 3)
    def _():
        start(query_halves())
        start(latent_copies(me, 0))

    FULL = ((0, 0), (1, 0), (0, 1), (1, 1))
    OWN = ((0, 0), (0, 1), (1, 1))
    row_i = lax.broadcasted_iota(jnp.int32, (half, half), 0)
    col_i = lax.broadcasted_iota(jnp.int32, (half, half), 1)

    def score_stage(u, blk, own, gi):
        tops = [None, None]

        def place(s, k, i):
            s_buf[u, cols(k), cols(i)] = s
            top = jnp.max(s, axis=0, keepdims=True)
            tops[i] = top if tops[i] is None else jnp.maximum(tops[i], top)

        def dot(k0, k1, i0, i1):
            lhs = jnp.concatenate([kn[u // 2, pl.ds(pl.multiple_of(blk * rows + k0 * half, half), (k1 - k0) * half), :],
                                   pen[blk, k0 * half:k1 * half, :]], axis=1)
            return lax.dot_general(lhs, qaug[lax.rem(gi, 2), u, :, i0 * half:i1 * half], NN, preferred_element_type=f32)

        if own:
            s = dot(0, 1, 0, 2)
            place(jnp.where(row_i <= col_i, s[:, :half], -jnp.inf), 0, 0)
            place(s[:, half:], 0, 1)
            place(jnp.where(row_i <= col_i, dot(1, 2, 1, 2), -jnp.inf), 1, 1)
            s_buf[u, cols(1), cols(0)] = jnp.full((half, half), -jnp.inf, f32)
        else:
            s = dot(0, 2, 0, 2)
            for k, i in FULL:
                place(s[cols(k), cols(i)], k, i)
        for i in range(2):
            c_buf[u, :, cols(i)] = tops[i]

    def exp_stage(u, slot):
        h = slot * GROUP + u
        m_old = m_s[h]
        m_new = jnp.maximum(m_old, c_buf[u])
        al_buf[u] = jnp.exp2((m_old - m_new) * scale2)
        m_s[h] = m_new
        for k, i in FULL:
            p_buf[u, cols(k), cols(i)] = jnp.exp2((s_buf[u, cols(k), cols(i)] - m_new[:, cols(i)]) * scale2).astype(bf16)

    def value_stage(u, slot, blk):
        h = slot * GROUP + u
        v = vt[h, :, pl.ds(pl.multiple_of(blk * rows, rows), rows)]
        for i in range(2):
            t = lax.dot_general(v, p_buf[u, :, cols(i)], NN, preferred_element_type=f32)
            acc[h, :, cols(i)] = t + acc[h, :, cols(i)] * al_buf[u, :, cols(i)]

    def place_of(gi):
        helping = gi == help_turn
        target = jnp.where(helping, partner, me)
        grp = jnp.where(helping, help_group, gi - (gi > help_turn).astype(jnp.int32))
        return helping, target, grp, lax.rem(gi, SLOTS)

    def help_copy(grp, to):
        return remote(o_help, o_nat.at[pl.ds(grp * pairs, pairs)], o_send, o_recv.at[grp], to)

    def finish(slot, gi):
        outs = []
        for j in range(pairs):
            t = jnp.concatenate([acc[slot * GROUP + h, :vdim, :] / acc[slot * GROUP + h, vdim:vdim + 1, :] for h in (2 * j, 2 * j + 1)], axis=0)
            outs.append(t.T.astype(bf16))
        for h in range(GROUP):
            acc[slot * GROUP + h] = jnp.zeros(acc.shape[1:], f32)

        helping, _, grp, _ = place_of(gi)

        @pl.when(jnp.logical_not(helping))
        def _():
            for j in range(pairs):
                o_nat[grp * pairs + j] = outs[j]

        @pl.when(helping)
        def _():
            for j in range(pairs):
                o_help[j] = outs[j]
            help_copy(help_group, partner).start()

    def step(carry, new, own, after=None, values_only=False):
        (slot1, _, _, _), (slot2, blk2, last2, gi2) = carry
        for u in range(GROUP):
            value_stage(u, slot2, blk2)
            if not values_only:
                exp_stage(u, slot1)
            if new is not None:
                score_stage(u, new[1], own, new[3])
        if after is not None:
            after()

        @pl.when(last2 == 1)
        def _():
            finish(slot2, gi2)

    def keys_and_values(slot, head0, blk):
        c = ckv[blk]
        at = pl.multiple_of(blk * rows, rows)
        for j in range(GROUP // 4):
            wk = wuk[pl.ds(pl.multiple_of((head0 + 4 * j) * nope, 4 * nope), 4 * nope), :]
            kk = lax.dot_general(c, wk, NT, preferred_element_type=f32).astype(bf16)
            kn[2 * j, pl.ds(at, rows), :] = kk[:, :128]
            kn[2 * j + 1, pl.ds(at, rows), :] = kk[:, 128:]
            wv = wuv[pl.ds(pl.multiple_of((head0 + 4 * j) * vdim, 4 * vdim), 4 * vdim), :]
            vv = lax.dot_general(wv, c, NT, preferred_element_type=f32).astype(bf16)
            for i in range(4):
                vt[slot * GROUP + 4 * j + i, :vdim, pl.ds(at, rows)] = vv[i * vdim:(i + 1) * vdim, :]

    def queries(buf, src, head0):
        ct, st = trig[src, :hr], trig[src, hr:]
        for j in range(GROUP // 4):
            w = wuq[pl.ds(pl.multiple_of((head0 + 4 * j) * qk, 4 * qk), 4 * qk), :]
            q = lax.dot_general(w, qlat[src], NT, preferred_element_type=f32)
            for i in range(4):
                u = 4 * j + i
                qh = q[i * qk:(i + 1) * qk]
                lo = (u % 2) * nope
                qaug[buf, u, lo:lo + nope, :] = qh[:nope].astype(bf16)
                r1, r2 = qh[nope:nope + hr], qh[nope + hr:]
                qaug[buf, u, 2 * nope:2 * nope + rot, :] = jnp.concatenate([r1 * ct - r2 * st, r2 * ct + r1 * st], axis=0).astype(bf16)

    def clear(slot):
        for u in range(GROUP):
            m_s[slot * GROUP + u] = jnp.full((1, rows), -jnp.inf, f32)

    def block_at(helping, target, i):
        usual = jnp.where(i == 0, target, lax.rem(i + target - 2, jnp.maximum(target, 1)))
        return jnp.where(helping & (me < 2), jnp.where(i < 2, i, 5 - i), usual)

    def group(gi, carry):
        helping, target, grp, slot = place_of(gi)
        gn = jnp.minimum(gi + 1, n_all - 1)
        helping_n, target_n, grp_n, _ = place_of(gn)
        slot_n = lax.rem(gi + 1, SLOTS)

        @pl.when((gi == help_turn - 1) & ((me == 1) | (me == 3)))
        def _():
            for c in query_copies(me):
                c.wait_recv()
            turn(1)

        @pl.when((gi == help_turn - 1) & (me == 0))
        def _():
            for c in query_halves()[1:] + (query_relay(),):
                c.wait_recv()
            start(query_share())
            turn(1)

        @pl.when(gi == 0)
        def _():
            for c in uq_loads[1:]:
                c.wait()

        @pl.when(gi == 1)
        def _():
            for c in wo_loads:
                c.start()

        fresh = ((gi == 0) & (me > 0)) | (helping & (me < 2))

        def one(i, carry):
            blk = block_at(helping, target, i)
            more = i < target
            blk_n = jnp.where(more, block_at(helping, target, i + 1), block_at(helping_n, target_n, 0))

            @pl.when(fresh & more & (blk_n != me))
            def _():
                received(blk_n)

                @pl.when((me >= 2) & (blk_n == 3 - me))
                def _():
                    start(forward_copies(blk_n))

                @pl.when((me == 0) & (blk_n >= 2))
                def _():
                    start(latent_share(blk_n))

            @pl.when((gi == 0) & (me == 2) & (i == 0))
            def _():
                query_halves()[0].wait_recv()
                query_relay().start()
                start(latent_copies(me, 0))

            new = (slot, blk, (i == target).astype(jnp.int32), gi)

            def next_keys():
                keys_and_values(jnp.where(more, slot, slot_n), jnp.where(more, grp, grp_n) * GROUP, blk_n)

            def after_own():
                queries(lax.rem(gi + 1, 2), helping_n.astype(jnp.int32), grp_n * GROUP)
                next_keys()
                clear(slot_n)

            @pl.when(blk == target)
            def _():
                step(carry, new, True, after_own)

            @pl.when(blk != target)
            def _():
                step(carry, new, False, next_keys)

            return new, carry[0]

        carry = lax.fori_loop(0, target + 1, one, carry)

        @pl.when(gi == 1)
        def _():
            for u in range(GROUP):
                acc[(SLOTS - 1) * GROUP + u] = jnp.zeros(acc.shape[1:], f32)

        return carry

    idle = (jnp.int32(SLOTS - 1), jnp.int32(0), jnp.int32(0), jnp.int32(0))
    uq_loads[0].wait()
    queries(0, 0, 0)
    for c in w_loads[2:]:
        c.wait()

    @pl.when(me >= 0)
    def _():
        keys_and_values(0, 0, me)
        clear(0)

    carry = lax.fori_loop(0, n_all, group, (idle, idle))
    step(carry, None, False)
    step((idle, carry[0]), None, False, values_only=True)

    def sent(copies):
        for c in copies:
            c.wait_send()

    @pl.when(me == 0)
    def _():
        sent(latent_copies(me, 1) + latent_copies(me, 3) + query_share() + latent_share(2) + latent_share(3))

    @pl.when(me == 1)
    def _():
        sent(latent_copies(me, 2) + latent_copies(me, 0))

    @pl.when(me == 2)
    def _():
        sent(latent_copies(me, 3) + latent_copies(me, 0) + forward_copies(1) + query_copies(3) + (query_relay(),))

    @pl.when(me == 3)
    def _():
        sent(latent_copies(me, 0) + forward_copies(0) + query_halves())

    @pl.when(helped > 0)
    def _():
        help_copy(help_group, partner).wait_send()

    for c in wo_loads:
        c.wait()
    deep = GROUP * vdim
    outs = [pltpu.make_async_copy(p_buf.at[n], out_hbm.at[:, pl.ds(n * rows, rows)], out_sem.at[n]) for n in range(tiles)]
    def product(grp, n):
        lhs = jnp.concatenate([o_nat[grp * pairs + j] for j in range(pairs)], axis=1)
        w = wo[pl.ds(pl.multiple_of(grp * deep, deep), deep), n * rows:(n + 1) * rows]
        return lax.dot_general(lhs, w, NN, preferred_element_type=f32)

    def arrive(grp):
        @pl.when(grp >= n_own)
        def _():
            help_copy(grp, me).wait_recv()

    for n in range(tiles):
        s_buf[n] = jnp.zeros((rows, rows), f32)

    def accumulate(grp, c):
        arrive(grp)
        for n in range(tiles):
            s_buf[n] = product(grp, n) + s_buf[n]
        return c

    lax.fori_loop(0, ngroup - 1, accumulate, 0)
    arrive(ngroup - 1)
    for n in range(tiles):
        p_buf[n] = (product(ngroup - 1, n) + s_buf[n]).astype(bf16)
        outs[n].start()
    for c in outs:
        c.wait()


def layer(pos, gq, gkv, x, wdkv, wdq, wuq, wuk, wuv, wo, scale2, heads, groups):
    rows, dim = x.shape
    rank = gkv.shape[0]
    rot = wdkv.shape[0] - rank
    qrank = wdq.shape[1]
    nope = wuk.shape[0] // heads
    vdim = wuv.shape[0] // heads
    seq = rows * groups
    vm = pl.BlockSpec(memory_space=pltpu.VMEM)
    anym = pl.BlockSpec(memory_space=pltpu.HBM)
    f32 = jnp.float32
    bf16 = jnp.bfloat16
    dma = pltpu.SemaphoreType.DMA
    return pl.pallas_call(
        functools.partial(layer_kernel, scale2=scale2, rows=rows, nope=nope, rot=rot, vdim=vdim, heads=heads, groups=groups),
        out_shape=(jax.ShapeDtypeStruct((rows, dim), bf16),
                   jax.ShapeDtypeStruct((rows, rank), bf16),
                   jax.ShapeDtypeStruct((rot, rows), bf16)),
        in_specs=[vm, vm, vm] + [anym] * 7,
        out_specs=(anym, vm, vm),
        scratch_shapes=[
            pltpu.VMEM(wdkv.shape, bf16),
            pltpu.VMEM(wo.shape, bf16),
            pltpu.VMEM(wuq.shape, bf16),
            pltpu.VMEM(wuk.shape, bf16),
            pltpu.VMEM(wuv.shape, bf16),
            pltpu.VMEM((2, rows, qrank), bf16),
            pltpu.VMEM((2, 8, rows), f32),
            pltpu.VMEM((2, rot, rows), f32),
            pltpu.VMEM((groups, rows, rank), bf16),
            pltpu.VMEM((groups, rot, rows), bf16),
            pltpu.VMEM((groups, rows, 128), bf16),
            pltpu.VMEM((2, GROUP, 256, rows), bf16),
            pltpu.VMEM((GROUP // 2, seq, 128), bf16),
            pltpu.VMEM((SLOTS * GROUP, vdim + 16, seq), bf16),
            pltpu.VMEM((GROUP, rows, rows), f32),
            pltpu.VMEM((GROUP, 1, rows), f32),
            pltpu.VMEM((GROUP, rows, rows), bf16),
            pltpu.VMEM((GROUP, 1, rows), f32),
            pltpu.VMEM((SLOTS * GROUP, 1, rows), f32),
            pltpu.VMEM((SLOTS * GROUP, vdim + 16, rows), f32),
            pltpu.VMEM((heads // 2, rows, 2 * vdim), bf16),
            pltpu.VMEM((GROUP // 2, rows, 2 * vdim), bf16),
            dma((x.shape[1] // rows + 4 + heads // GROUP,)),
            dma((groups,)), dma((groups,)), dma((groups,)), dma((groups,)), dma((2,)),
            dma((3,)), dma((3,)), dma, dma,
            dma, dma((heads // GROUP,)),
            dma((2,)), dma((dim // rows,)),
        ],
        compiler_params=pltpu.CompilerParams(vmem_limit_bytes=LAYER_VMEM, collective_id=0, has_side_effects=True),
        cost_estimate=pl.CostEstimate(flops=40_000_000_000, bytes_accessed=40_000_000, transcendentals=30_000_000),
    )(pos, gq, gkv, x, wdkv, wdq, wuq, wuk, wuv, wo)


def solution(mesh):
    groups = mesh.shape['sp']
    tok_spec = P(('dp', 'sp'))
    rows_spec = P(('dp', 'sp'), None)
    replicated = P()

    def local_step(tok_in, tok_pos, w_dq, g_q, w_uq, w_dkv, g_kv, w_uk, w_uv, w_o):
        heads, qk_dim = w_uq.shape[1:]
        kv_rank = g_kv.shape[0]
        rot_dim = w_dkv.shape[1] - kv_rank
        v_dim = w_uv.shape[2]
        attn_scale = (0.1 * math.log(YARN_FACTOR) + 1.0) ** 2 / math.sqrt(qk_dim)
        def flat(w):
            return jnp.transpose(w, (1, 2, 0)).reshape(-1, w.shape[0])

        attn_out, cache_kv, cache_pe = layer(tok_pos, g_q, g_kv, tok_in, w_dkv.T, w_dq, flat(w_uq), flat(w_uk), flat(w_uv), w_o.reshape(heads * v_dim, -1),
                                      attn_scale * math.log2(math.e), heads, groups)
        return attn_out, cache_kv, cache_pe.T

    return jax.shard_map(local_step, mesh=mesh, in_specs=(rows_spec, tok_spec, replicated, replicated, replicated, replicated, replicated, replicated, replicated, replicated), out_specs=(rows_spec, rows_spec, rows_spec), check_vma=False)
```

```python
import functools
import math
import jax
import jax.numpy as jnp
from jax import lax
from jax.experimental import pallas as pl
from jax.experimental.pallas import tpu as pltpu
from jax.sharding import PartitionSpec as P

ROPE_THETA = 10000.0
YARN_FACTOR = 40.0
ORIG_CTX = 4096.0
BETA_FAST = 32.0
BETA_SLOW = 1.0
NORM_EPS = 1e-6


def rope_freqs(rot_dim):
    half_dim = rot_dim // 2
    log_base = 2.0 * math.log(ROPE_THETA)
    low_idx = max(math.floor(rot_dim * math.log(ORIG_CTX / (BETA_FAST * 2.0 * math.pi)) / log_base), 0)
    high_idx = min(math.ceil(rot_dim * math.log(ORIG_CTX / (BETA_SLOW * 2.0 * math.pi)) / log_base), half_dim - 1)
    spread = max(high_idx - low_idx, 0.001)
    freq_list = []
    for freq_idx in range(half_dim):
        base_freq = ROPE_THETA ** (-2.0 * freq_idx / rot_dim)
        ramp_val = min(max((freq_idx - low_idx) / spread, 0.0), 1.0)
        freq_list.append(base_freq / YARN_FACTOR * ramp_val + base_freq * (1.0 - ramp_val))
    return freq_list


GROUP = 8
SLOTS = 3
LAYER_VMEM = 65500000


def layer_kernel(pos_ref, gq_ref, gkv_ref, x_hbm, wdkv_hbm, wdq_hbm, wuq_hbm, wuk_hbm, wuv_hbm, wo_hbm,
                 out_hbm, ckv_out, cpe_out,
                 wdkv, wo, wuq, wuk, wuv, qlat, posf, trig, ckv, pet, pen, qaug, kn, vt,
                 s_buf, c_buf, p_buf, al_buf, m_s, acc, o_nat, o_help,
                 load_sem, c_send, c_recv, pe_send, pe_recv, f_send, q_send, q_recv, t_send, t_recv, o_send, o_recv, wo_sem, out_sem,
                 *, scale2, rows, nope, rot, vdim, heads, groups):
    f32 = jnp.float32
    bf16 = jnp.bfloat16
    NT = (((1,), (1,)), ((), ()))
    NN = (((1,), (0,)), ((), ()))
    half = rows // 2
    qk = nope + rot
    pairs = GROUP // 2
    ngroup = heads // GROUP
    me = lax.axis_index('sp')
    given = jnp.where(me == 3, 2, jnp.where(me == 2, 1, 0))
    helped = jnp.where(me == 2, 0, 1)
    partner = jnp.where(me == 3, 2, 3)
    help_group = jnp.where(me == 1, 3, 4)
    help_turn = jnp.where(me == 2, 2 * ngroup, jnp.where(me == 3, 2, 3))
    n_own = ngroup - given
    n_all = n_own + helped

    tiles = x_hbm.shape[1] // rows
    x_loads = [pltpu.make_async_copy(x_hbm.at[:, pl.ds(i * rows, rows)], p_buf.at[i], load_sem.at[i]) for i in range(tiles)]
    qrank = wdq_hbm.shape[1]
    part = GROUP * qk
    w_loads = [pltpu.make_async_copy(s, d, load_sem.at[tiles + i]) for i, (s, d) in enumerate(
        ((wdkv_hbm, wdkv), (wdq_hbm, wo.at[:, pl.ds(0, qrank)]), (wuk_hbm, wuk), (wuv_hbm, wuv)))]
    uq_loads = [pltpu.make_async_copy(wuq_hbm.at[pl.ds(i * part, part)], wuq.at[pl.ds(i * part, part)], load_sem.at[tiles + 4 + i]) for i in range(ngroup)]
    wide = wo_hbm.shape[1] - qrank
    wo_loads = [pltpu.make_async_copy(wo_hbm.at[:, pl.ds(a, n)], wo.at[:, pl.ds(a, n)], wo_sem.at[i])
                for i, (a, n) in enumerate(((qrank, wide), (0, qrank)))]
    for c in x_loads + w_loads[:2]:
        c.start()
    barrier = pltpu.get_barrier_semaphore()
    for d in range(1, groups):
        pl.semaphore_signal(barrier, inc=1, device_id={'sp': lax.rem(me + d, groups)}, device_id_type=pl.DeviceIdType.MESH)

    def remote(s, d, ssem, rsem, to):
        return pltpu.make_async_remote_copy(src_ref=s, dst_ref=d, send_sem=ssem, recv_sem=rsem,
                                            device_id={'sp': to}, device_id_type=pl.DeviceIdType.MESH)

    def latent_copies(origin, to):
        return (remote(ckv.at[origin], ckv.at[origin], c_send.at[to], c_recv.at[origin], to),
                remote(pet.at[origin], pet.at[origin], pe_send.at[to], pe_recv.at[origin], to))

    def forward_copies(origin):
        to = 5 - me
        return (remote(ckv.at[origin], ckv.at[origin], f_send.at[0], c_recv.at[origin], to),
                remote(pet.at[origin], pet.at[origin], f_send.at[1], pe_recv.at[origin], to))

    def query_copies(to):
        return (remote(qlat.at[0], qlat.at[1], q_send.at[0], q_recv.at[0], to),
                remote(posf.at[0], posf.at[1], t_send, t_recv, to))

    def query_halves():
        top, low = pl.ds(0, half), pl.ds(half, half)
        return (remote(qlat.at[0, low], qlat.at[1, low], q_send.at[1], q_recv.at[1], 2),
                remote(posf.at[0], posf.at[1], t_send, t_recv, 0),
                remote(qlat.at[0, top], qlat.at[1, top], q_send.at[0], q_recv.at[0], 0))

    def query_relay():
        low = pl.ds(half, half)
        return remote(qlat.at[1, low], qlat.at[1, low], q_send.at[2], q_recv.at[2], 0)

    def query_share():
        return (remote(qlat.at[1], qlat.at[1], q_send.at[0], q_recv.at[0], 1),
                remote(posf.at[1], posf.at[1], t_send, t_recv, 1))

    def latent_share(origin):
        spare = 6 - 2 * origin
        return (remote(ckv.at[origin], ckv.at[origin], c_send.at[spare], c_recv.at[origin], 1),
                remote(pet.at[origin], pet.at[origin], pe_send.at[spare], pe_recv.at[origin], 1))

    def start(copies):
        for c in copies:
            c.start()

    def received(origin):
        for c in latent_copies(origin, me):
            c.wait_recv()
        unpack_rope(origin)

    def unpack_rope(origin):
        wide = jnp.concatenate([pet[origin].astype(f32), jnp.zeros((128 - rot, rows), f32)], axis=0)
        pen[origin] = wide.T.astype(bf16)

    hr = rot // 2

    def cols(i):
        return slice(i * half, (i + 1) * half)

    freq_i = lax.broadcasted_iota(jnp.int32, (hr, rows), 0)
    freq = jnp.zeros((hr, rows), f32)
    for i, f in enumerate(rope_freqs(rot)):
        freq = jnp.where(freq_i == i, f, freq)

    def turn(i):
        angle = posf[i, :1] * freq
        trig[i, :hr] = jnp.cos(angle)
        trig[i, hr:] = jnp.sin(angle)

    posf[0] = jnp.broadcast_to(pos_ref[...].astype(f32).reshape(1, rows), (8, rows))
    turn(0)
    cos_t, sin_t = trig[0, :hr], trig[0, hr:]
    qaug[...] = jnp.zeros_like(qaug)
    vt[:, vdim:, :] = jnp.ones((vt.shape[0], vt.shape[1] - vdim, vt.shape[2]), vt.dtype)
    acc[...] = jnp.zeros_like(acc)
    for c in x_loads + w_loads[:1]:
        c.wait()
    for c in uq_loads[:1] + w_loads[2:] + uq_loads[1:]:
        c.start()

    def x_rows(cut):
        return jnp.concatenate([p_buf[i, cut, :] for i in range(tiles)], axis=1)

    kvt = lax.dot_general(wdkv[...], x_rows(slice(0, rows)), NT, preferred_element_type=f32)
    rank = ckv.shape[2]
    a = kvt[:rank]
    norm = a * lax.rsqrt(jnp.sum(a * a, axis=0, keepdims=True) / rank + NORM_EPS)
    c_own = (norm.T * gkv_ref[...].reshape(1, rank)).astype(bf16)
    ckv[me] = c_own
    ckv_out[...] = c_own
    z1, z2 = kvt[rank:rank + hr], kvt[rank + hr:]
    pe_own = jnp.concatenate([z1 * cos_t - z2 * sin_t, z2 * cos_t + z1 * sin_t], axis=0).astype(bf16)
    pet[me] = pe_own
    cpe_out[...] = pe_own
    w_loads[1].wait()
    def query_latent(part):
        ql = lax.dot_general(x_rows(cols(part)), wo[:, :qrank], NN, preferred_element_type=f32)
        ql = ql * lax.rsqrt(jnp.sum(ql * ql, axis=1, keepdims=True) / qrank + NORM_EPS) * gq_ref[...].reshape(1, qrank)
        qlat[0, cols(part)] = ql.astype(bf16)

    query_latent(0)
    pl.semaphore_wait(barrier, groups - 1)

    @pl.when(me == 0)
    def _():
        for t in (1, 3):
            start(latent_copies(me, t))

    @pl.when(me == 1)
    def _():
        for t in (2, 0):
            start(latent_copies(me, t))

    @pl.when(me == 2)
    def _():
        start(latent_copies(me, 3))

    query_latent(1)
    unpack_rope(me)
    @pl.when(me == 2)
    def _():
        start(query_copies(3))

    @pl.when(me == 3)
    def _():
        start(query_halves())
        start(latent_copies(me, 0))

    FULL = ((0, 0), (1, 0), (0, 1), (1, 1))
    OWN = ((0, 0), (0, 1), (1, 1))
    row_i = lax.broadcasted_iota(jnp.int32, (half, half), 0)
    col_i = lax.broadcasted_iota(jnp.int32, (half, half), 1)

    def score_stage(u, blk, own, gi):
        tops = [None, None]

        def place(s, k, i):
            s_buf[u, cols(k), cols(i)] = s
            top = jnp.max(s, axis=0, keepdims=True)
            tops[i] = top if tops[i] is None else jnp.maximum(tops[i], top)

        def dot(k0, k1, i0, i1):
            lhs = jnp.concatenate([kn[u // 2, pl.ds(pl.multiple_of(blk * rows + k0 * half, half), (k1 - k0) * half), :],
                                   pen[blk, k0 * half:k1 * half, :]], axis=1)
            return lax.dot_general(lhs, qaug[lax.rem(gi, 2), u, :, i0 * half:i1 * half], NN, preferred_element_type=f32)

        if own:
            s = dot(0, 1, 0, 2)
            place(jnp.where(row_i <= col_i, s[:, :half], -jnp.inf), 0, 0)
            place(s[:, half:], 0, 1)
            place(jnp.where(row_i <= col_i, dot(1, 2, 1, 2), -jnp.inf), 1, 1)
            s_buf[u, cols(1), cols(0)] = jnp.full((half, half), -jnp.inf, f32)
        else:
            s = dot(0, 2, 0, 2)
            for k, i in FULL:
                place(s[cols(k), cols(i)], k, i)
        for i in range(2):
            c_buf[u, :, cols(i)] = tops[i]

    def exp_stage(u, slot):
        h = slot * GROUP + u
        m_old = m_s[h]
        m_new = jnp.maximum(m_old, c_buf[u])
        al_buf[u] = jnp.exp2((m_old - m_new) * scale2)
        m_s[h] = m_new
        for k, i in FULL:
            p_buf[u, cols(k), cols(i)] = jnp.exp2((s_buf[u, cols(k), cols(i)] - m_new[:, cols(i)]) * scale2).astype(bf16)

    def value_stage(u, slot, blk):
        h = slot * GROUP + u
        v = vt[h, :, pl.ds(pl.multiple_of(blk * rows, rows), rows)]
        for i in range(2):
            t = lax.dot_general(v, p_buf[u, :, cols(i)], NN, preferred_element_type=f32)
            acc[h, :, cols(i)] = t + acc[h, :, cols(i)] * al_buf[u, :, cols(i)]

    def place_of(gi):
        helping = gi == help_turn
        target = jnp.where(helping, partner, me)
        grp = jnp.where(helping, help_group, gi - (gi > help_turn).astype(jnp.int32))
        return helping, target, grp, lax.rem(gi, SLOTS)

    def help_copy(grp, to):
        return remote(o_help, o_nat.at[pl.ds(grp * pairs, pairs)], o_send, o_recv.at[grp], to)

    def finish(slot, gi):
        outs = []
        for j in range(pairs):
            t = jnp.concatenate([acc[slot * GROUP + h, :vdim, :] / acc[slot * GROUP + h, vdim:vdim + 1, :] for h in (2 * j, 2 * j + 1)], axis=0)
            outs.append(t.T.astype(bf16))
        for h in range(GROUP):
            acc[slot * GROUP + h] = jnp.zeros(acc.shape[1:], f32)

        helping, _, grp, _ = place_of(gi)

        @pl.when(jnp.logical_not(helping))
        def _():
            for j in range(pairs):
                o_nat[grp * pairs + j] = outs[j]

        @pl.when(helping)
        def _():
            for j in range(pairs):
                o_help[j] = outs[j]
            help_copy(help_group, partner).start()

    def step(carry, new, own, after=None, values_only=False):
        (slot1, _, _, _), (slot2, blk2, last2, gi2) = carry
        for u in range(GROUP):
            value_stage(u, slot2, blk2)
            if not values_only:
                exp_stage(u, slot1)
            if new is not None:
                score_stage(u, new[1], own, new[3])
        if after is not None:
            after()

        @pl.when(last2 == 1)
        def _():
            finish(slot2, gi2)

    def keys_and_values(slot, head0, blk):
        c = ckv[blk]
        at = pl.multiple_of(blk * rows, rows)
        for j in range(GROUP // 4):
            wk = wuk[pl.ds(pl.multiple_of((head0 + 4 * j) * nope, 4 * nope), 4 * nope), :]
            kk = lax.dot_general(c, wk, NT, preferred_element_type=f32).astype(bf16)
            kn[2 * j, pl.ds(at, rows), :] = kk[:, :128]
            kn[2 * j + 1, pl.ds(at, rows), :] = kk[:, 128:]
            wv = wuv[pl.ds(pl.multiple_of((head0 + 4 * j) * vdim, 4 * vdim), 4 * vdim), :]
            vv = lax.dot_general(wv, c, NT, preferred_element_type=f32).astype(bf16)
            for i in range(4):
                vt[slot * GROUP + 4 * j + i, :vdim, pl.ds(at, rows)] = vv[i * vdim:(i + 1) * vdim, :]

    def queries(buf, src, head0):
        ct, st = trig[src, :hr], trig[src, hr:]
        for j in range(GROUP // 4):
            w = wuq[pl.ds(pl.multiple_of((head0 + 4 * j) * qk, 4 * qk), 4 * qk), :]
            q = lax.dot_general(w, qlat[src], NT, preferred_element_type=f32)
            for i in range(4):
                u = 4 * j + i
                qh = q[i * qk:(i + 1) * qk]
                lo = (u % 2) * nope
                qaug[buf, u, lo:lo + nope, :] = qh[:nope].astype(bf16)
                r1, r2 = qh[nope:nope + hr], qh[nope + hr:]
                qaug[buf, u, 2 * nope:2 * nope + rot, :] = jnp.concatenate([r1 * ct - r2 * st, r2 * ct + r1 * st], axis=0).astype(bf16)

    def clear(slot):
        for u in range(GROUP):
            m_s[slot * GROUP + u] = jnp.full((1, rows), -jnp.inf, f32)

    def block_at(helping, target, i):
        usual = jnp.where(i == 0, target, lax.rem(i + target - 2, jnp.maximum(target, 1)))
        return jnp.where(helping & (me < 2), jnp.where(i < 2, i, 5 - i), usual)

    def group(gi, carry):
        helping, target, grp, slot = place_of(gi)
        gn = jnp.minimum(gi + 1, n_all - 1)
        helping_n, target_n, grp_n, _ = place_of(gn)
        slot_n = lax.rem(gi + 1, SLOTS)

        @pl.when((gi == help_turn - 1) & ((me == 1) | (me == 3)))
        def _():
            for c in query_copies(me):
                c.wait_recv()
            turn(1)

        @pl.when((gi == help_turn - 1) & (me == 0))
        def _():
            for c in query_halves()[1:] + (query_relay(),):
                c.wait_recv()
            start(query_share())
            turn(1)

        @pl.when(gi == 0)
        def _():
            for c in uq_loads[1:]:
                c.wait()

        @pl.when(gi == 1)
        def _():
            for c in wo_loads:
                c.start()

        fresh = ((gi == 0) & (me > 0)) | (helping & (me < 2))

        def one(i, carry):
            blk = block_at(helping, target, i)
            more = i < target
            blk_n = jnp.where(more, block_at(helping, target, i + 1), block_at(helping_n, target_n, 0))

            @pl.when(fresh & more & (blk_n != me))
            def _():
                received(blk_n)

                @pl.when((me >= 2) & (blk_n == 3 - me))
                def _():
                    start(forward_copies(blk_n))

                @pl.when((me == 0) & (blk_n >= 2))
                def _():
                    start(latent_share(blk_n))

            @pl.when((gi == 0) & (me == 2) & (i == 0))
            def _():
                query_halves()[0].wait_recv()
                query_relay().start()
                start(latent_copies(me, 0))

            new = (slot, blk, (i == target).astype(jnp.int32), gi)

            def next_keys():
                keys_and_values(jnp.where(more, slot, slot_n), jnp.where(more, grp, grp_n) * GROUP, blk_n)

            def after_own():
                queries(lax.rem(gi + 1, 2), helping_n.astype(jnp.int32), grp_n * GROUP)
                next_keys()
                clear(slot_n)

            @pl.when(blk == target)
            def _():
                step(carry, new, True, after_own)

            @pl.when(blk != target)
            def _():
                step(carry, new, False, next_keys)

            return new, carry[0]

        carry = lax.fori_loop(0, target + 1, one, carry)

        @pl.when(gi == 1)
        def _():
            for u in range(GROUP):
                acc[(SLOTS - 1) * GROUP + u] = jnp.zeros(acc.shape[1:], f32)

        return carry

    idle = (jnp.int32(SLOTS - 1), jnp.int32(0), jnp.int32(0), jnp.int32(0))
    uq_loads[0].wait()
    queries(0, 0, 0)
    for c in w_loads[2:]:
        c.wait()

    @pl.when(me >= 0)
    def _():
        keys_and_values(0, 0, me)
        clear(0)

    carry = lax.fori_loop(0, n_all, group, (idle, idle))
    step(carry, None, False)
    step((idle, carry[0]), None, False, values_only=True)

    for c in wo_loads:
        c.wait()
    deep = GROUP * vdim
    outs = [pltpu.make_async_copy(p_buf.at[n], out_hbm.at[:, pl.ds(n * rows, rows)], out_sem.at[n]) for n in range(tiles)]
    def product(grp, n):
        lhs = jnp.concatenate([o_nat[grp * pairs + j] for j in range(pairs)], axis=1)
        w = wo[pl.ds(pl.multiple_of(grp * deep, deep), deep), n * rows:(n + 1) * rows]
        return lax.dot_general(lhs, w, NN, preferred_element_type=f32)

    def arrive(grp):
        @pl.when(grp >= n_own)
        def _():
            help_copy(grp, me).wait_recv()

    for n in range(tiles):
        s_buf[n] = jnp.zeros((rows, rows), f32)

    def accumulate(grp, c):
        arrive(grp)
        for n in range(tiles):
            s_buf[n] = product(grp, n) + s_buf[n]
        return c

    lax.fori_loop(0, ngroup - 1, accumulate, 0)
    arrive(ngroup - 1)
    for n in range(tiles):
        p_buf[n] = (product(ngroup - 1, n) + s_buf[n]).astype(bf16)
        outs[n].start()
    def sent(copies):
        for c in copies:
            c.wait_send()

    @pl.when(me == 0)
    def _():
        sent(latent_copies(me, 1) + latent_copies(me, 3) + query_share() + latent_share(2) + latent_share(3))

    @pl.when(me == 1)
    def _():
        sent(latent_copies(me, 2) + latent_copies(me, 0))

    @pl.when(me == 2)
    def _():
        sent(latent_copies(me, 3) + latent_copies(me, 0) + forward_copies(1) + query_copies(3) + (query_relay(),))

    @pl.when(me == 3)
    def _():
        sent(latent_copies(me, 0) + forward_copies(0) + query_halves())

    @pl.when(helped > 0)
    def _():
        help_copy(help_group, partner).wait_send()

    for c in outs:
        c.wait()


def layer(pos, gq, gkv, x, wdkv, wdq, wuq, wuk, wuv, wo, scale2, heads, groups):
    rows, dim = x.shape
    rank = gkv.shape[0]
    rot = wdkv.shape[0] - rank
    qrank = wdq.shape[1]
    nope = wuk.shape[0] // heads
    vdim = wuv.shape[0] // heads
    seq = rows * groups
    vm = pl.BlockSpec(memory_space=pltpu.VMEM)
    anym = pl.BlockSpec(memory_space=pltpu.HBM)
    f32 = jnp.float32
    bf16 = jnp.bfloat16
    dma = pltpu.SemaphoreType.DMA
    return pl.pallas_call(
        functools.partial(layer_kernel, scale2=scale2, rows=rows, nope=nope, rot=rot, vdim=vdim, heads=heads, groups=groups),
        out_shape=(jax.ShapeDtypeStruct((rows, dim), bf16),
                   jax.ShapeDtypeStruct((rows, rank), bf16),
                   jax.ShapeDtypeStruct((rot, rows), bf16)),
        in_specs=[vm, vm, vm] + [anym] * 7,
        out_specs=(anym, vm, vm),
        scratch_shapes=[
            pltpu.VMEM(wdkv.shape, bf16),
            pltpu.VMEM(wo.shape, bf16),
            pltpu.VMEM(wuq.shape, bf16),
            pltpu.VMEM(wuk.shape, bf16),
            pltpu.VMEM(wuv.shape, bf16),
            pltpu.VMEM((2, rows, qrank), bf16),
            pltpu.VMEM((2, 8, rows), f32),
            pltpu.VMEM((2, rot, rows), f32),
            pltpu.VMEM((groups, rows, rank), bf16),
            pltpu.VMEM((groups, rot, rows), bf16),
            pltpu.VMEM((groups, rows, 128), bf16),
            pltpu.VMEM((2, GROUP, 256, rows), bf16),
            pltpu.VMEM((GROUP // 2, seq, 128), bf16),
            pltpu.VMEM((SLOTS * GROUP, vdim + 16, seq), bf16),
            pltpu.VMEM((GROUP, rows, rows), f32),
            pltpu.VMEM((GROUP, 1, rows), f32),
            pltpu.VMEM((GROUP, rows, rows), bf16),
            pltpu.VMEM((GROUP, 1, rows), f32),
            pltpu.VMEM((SLOTS * GROUP, 1, rows), f32),
            pltpu.VMEM((SLOTS * GROUP, vdim + 16, rows), f32),
            pltpu.VMEM((heads // 2, rows, 2 * vdim), bf16),
            pltpu.VMEM((GROUP // 2, rows, 2 * vdim), bf16),
            dma((x.shape[1] // rows + 4 + heads // GROUP,)),
            dma((groups,)), dma((groups,)), dma((groups,)), dma((groups,)), dma((2,)),
            dma((3,)), dma((3,)), dma, dma,
            dma, dma((heads // GROUP,)),
            dma((2,)), dma((dim // rows,)),
        ],
        compiler_params=pltpu.CompilerParams(vmem_limit_bytes=LAYER_VMEM, collective_id=0, has_side_effects=True),
        cost_estimate=pl.CostEstimate(flops=40_000_000_000, bytes_accessed=40_000_000, transcendentals=30_000_000),
    )(pos, gq, gkv, x, wdkv, wdq, wuq, wuk, wuv, wo)


def deliver_kernel(out_in, ckv_in, cpe_in, out_hbm, ckv_out, cpe_out, out, ckv, cpe, in_sem, out_sem):
    half = out.shape[0] // 2
    steps = ((ckv_in, ckv, ckv_out, None), (cpe_in, cpe, cpe_out, None), (out_in, out, out_hbm, 0), (out_in, out, out_hbm, half))

    def view(ref, start):
        return ref if start is None else ref.at[pl.ds(start, half)]

    ins = [pltpu.make_async_copy(view(a, n), view(b, n), in_sem.at[i]) for i, (a, b, _, n) in enumerate(steps)]
    outs = [pltpu.make_async_copy(view(b, n), view(c, n), out_sem.at[i]) for i, (_, b, c, n) in enumerate(steps)]
    for c in ins:
        c.start()
    for a, b in zip(ins, outs):
        a.wait()
        b.start()
    for c in outs:
        c.wait()


def deliver(*arrays):
    anym = pl.BlockSpec(memory_space=pl.ANY)
    return pl.pallas_call(
        deliver_kernel,
        in_specs=[anym] * 3,
        out_specs=(anym,) * 3,
        out_shape=tuple(jax.ShapeDtypeStruct(a.shape, a.dtype) for a in arrays),
        scratch_shapes=[pltpu.VMEM(a.shape, a.dtype) for a in arrays] + [pltpu.SemaphoreType.DMA((4,)), pltpu.SemaphoreType.DMA((4,))],
        compiler_params=pltpu.CompilerParams(vmem_limit_bytes=62 * 1024 * 1024),
        cost_estimate=pl.CostEstimate(flops=1000, bytes_accessed=6_000_000, transcendentals=0),
    )(*arrays)


def solution(mesh):
    groups = mesh.shape['sp']
    tok_spec = P(('dp', 'sp'))
    rows_spec = P(('dp', 'sp'), None)
    replicated = P()

    def local_step(tok_in, tok_pos, w_dq, g_q, w_uq, w_dkv, g_kv, w_uk, w_uv, w_o):
        heads, qk_dim = w_uq.shape[1:]
        kv_rank = g_kv.shape[0]
        rot_dim = w_dkv.shape[1] - kv_rank
        v_dim = w_uv.shape[2]
        attn_scale = (0.1 * math.log(YARN_FACTOR) + 1.0) ** 2 / math.sqrt(qk_dim)
        def flat(w):
            return jnp.transpose(w, (1, 2, 0)).reshape(-1, w.shape[0])

        attn_out, cache_kv, cache_pe = layer(tok_pos, g_q, g_kv, tok_in, w_dkv.T, w_dq, flat(w_uq), flat(w_uk), flat(w_uv), w_o.reshape(heads * v_dim, -1),
                                      attn_scale * math.log2(math.e), heads, groups)
        attn_out, cache_kv, cache_pe = deliver(attn_out, cache_kv, cache_pe)
        return attn_out, cache_kv, cache_pe.T

    return jax.shard_map(local_step, mesh=mesh, in_specs=(rows_spec, tok_spec, replicated, replicated, replicated, replicated, replicated, replicated, replicated, replicated), out_specs=(rows_spec, rows_spec, rows_spec), check_vma=False)
```

```python
import functools
import math
import jax
import jax.numpy as jnp
from jax import lax
from jax.experimental import pallas as pl
from jax.experimental.pallas import tpu as pltpu
from jax.sharding import PartitionSpec as P

ROPE_THETA = 10000.0
YARN_FACTOR = 40.0
ORIG_CTX = 4096.0
BETA_FAST = 32.0
BETA_SLOW = 1.0
NORM_EPS = 1e-6


def rope_freqs(rot_dim):
    half_dim = rot_dim // 2
    log_base = 2.0 * math.log(ROPE_THETA)
    low_idx = max(math.floor(rot_dim * math.log(ORIG_CTX / (BETA_FAST * 2.0 * math.pi)) / log_base), 0)
    high_idx = min(math.ceil(rot_dim * math.log(ORIG_CTX / (BETA_SLOW * 2.0 * math.pi)) / log_base), half_dim - 1)
    spread = max(high_idx - low_idx, 0.001)
    freq_list = []
    for freq_idx in range(half_dim):
        base_freq = ROPE_THETA ** (-2.0 * freq_idx / rot_dim)
        ramp_val = min(max((freq_idx - low_idx) / spread, 0.0), 1.0)
        freq_list.append(base_freq / YARN_FACTOR * ramp_val + base_freq * (1.0 - ramp_val))
    return freq_list


GROUP = 8
SLOTS = 3
LAYER_VMEM = 65500000


def layer_kernel(pos_ref, gq_ref, gkv_ref, x_hbm, wdkv_hbm, wdq_hbm, wuq_hbm, wuk_hbm, wuv_hbm, wo_hbm,
                 out_hbm, ckv_out, cpe_out,
                 wdkv, wo, wuq, wuk, wuv, qlat, posf, trig, ckv, pet, pen, qaug, kn, vt,
                 s_buf, c_buf, p_buf, al_buf, m_s, acc, o_nat, o_help,
                 load_sem, c_send, c_recv, pe_send, pe_recv, f_send, q_send, q_recv, t_send, t_recv, o_send, o_recv, wo_sem, out_sem,
                 *, scale2, rows, nope, rot, vdim, heads, groups):
    f32 = jnp.float32
    bf16 = jnp.bfloat16
    NT = (((1,), (1,)), ((), ()))
    NN = (((1,), (0,)), ((), ()))
    half = rows // 2
    qk = nope + rot
    pairs = GROUP // 2
    ngroup = heads // GROUP
    me = lax.axis_index('sp')
    given = jnp.where(me == 3, 2, jnp.where(me == 2, 1, 0))
    helped = jnp.where(me == 2, 0, 1)
    partner = jnp.where(me == 3, 2, 3)
    help_group = jnp.where(me == 1, 3, 4)
    help_turn = jnp.where(me == 2, 2 * ngroup, jnp.where(me == 3, 2, 3))
    n_own = ngroup - given
    n_all = n_own + helped

    tiles = x_hbm.shape[1] // rows
    x_loads = [pltpu.make_async_copy(x_hbm.at[:, pl.ds(i * rows, rows)], p_buf.at[i], load_sem.at[i]) for i in range(tiles)]
    qrank = wdq_hbm.shape[1]
    part = GROUP * qk
    w_loads = [pltpu.make_async_copy(s, d, load_sem.at[tiles + i]) for i, (s, d) in enumerate(
        ((wdkv_hbm, wdkv), (wdq_hbm, wo.at[:, pl.ds(0, qrank)]), (wuk_hbm, wuk), (wuv_hbm, wuv)))]
    uq_loads = [pltpu.make_async_copy(wuq_hbm.at[pl.ds(i * part, part)], wuq.at[pl.ds(i * part, part)], load_sem.at[tiles + 4 + i]) for i in range(ngroup)]
    wide = wo_hbm.shape[1] - qrank
    wo_loads = [pltpu.make_async_copy(wo_hbm.at[:, pl.ds(a, n)], wo.at[:, pl.ds(a, n)], wo_sem.at[i])
                for i, (a, n) in enumerate(((qrank, wide), (0, qrank)))]
    for c in x_loads + w_loads[:2]:
        c.start()
    barrier = pltpu.get_barrier_semaphore()
    for d in range(1, groups):
        pl.semaphore_signal(barrier, inc=1, device_id={'sp': lax.rem(me + d, groups)}, device_id_type=pl.DeviceIdType.MESH)

    def remote(s, d, ssem, rsem, to):
        return pltpu.make_async_remote_copy(src_ref=s, dst_ref=d, send_sem=ssem, recv_sem=rsem,
                                            device_id={'sp': to}, device_id_type=pl.DeviceIdType.MESH)

    def latent_copies(origin, to):
        return (remote(ckv.at[origin], ckv.at[origin], c_send.at[to], c_recv.at[origin], to),
                remote(pet.at[origin], pet.at[origin], pe_send.at[to], pe_recv.at[origin], to))

    def forward_copies(origin):
        to = 5 - me
        return (remote(ckv.at[origin], ckv.at[origin], f_send.at[0], c_recv.at[origin], to),
                remote(pet.at[origin], pet.at[origin], f_send.at[1], pe_recv.at[origin], to))

    def query_copies(to):
        return (remote(qlat.at[0], qlat.at[1], q_send.at[0], q_recv.at[0], to),
                remote(posf.at[0], posf.at[1], t_send, t_recv, to))

    def query_halves():
        top, low = pl.ds(0, half), pl.ds(half, half)
        return (remote(qlat.at[0, low], qlat.at[1, low], q_send.at[1], q_recv.at[1], 2),
                remote(posf.at[0], posf.at[1], t_send, t_recv, 0),
                remote(qlat.at[0, top], qlat.at[1, top], q_send.at[0], q_recv.at[0], 0))

    def query_relay():
        low = pl.ds(half, half)
        return remote(qlat.at[1, low], qlat.at[1, low], q_send.at[2], q_recv.at[2], 0)

    def query_share():
        return (remote(qlat.at[1], qlat.at[1], q_send.at[0], q_recv.at[0], 1),
                remote(posf.at[1], posf.at[1], t_send, t_recv, 1))

    def latent_share(origin):
        spare = 6 - 2 * origin
        return (remote(ckv.at[origin], ckv.at[origin], c_send.at[spare], c_recv.at[origin], 1),
                remote(pet.at[origin], pet.at[origin], pe_send.at[spare], pe_recv.at[origin], 1))

    def start(copies):
        for c in copies:
            c.start()

    def received(origin):
        for c in latent_copies(origin, me):
            c.wait_recv()
        unpack_rope(origin)

    def unpack_rope(origin):
        wide = jnp.concatenate([pet[origin].astype(f32), jnp.zeros((128 - rot, rows), f32)], axis=0)
        pen[origin] = wide.T.astype(bf16)

    hr = rot // 2

    def cols(i):
        return slice(i * half, (i + 1) * half)

    freq_i = lax.broadcasted_iota(jnp.int32, (hr, rows), 0)
    freq = jnp.zeros((hr, rows), f32)
    for i, f in enumerate(rope_freqs(rot)):
        freq = jnp.where(freq_i == i, f, freq)

    def turn(i):
        angle = posf[i, :1] * freq
        trig[i, :hr] = jnp.cos(angle)
        trig[i, hr:] = jnp.sin(angle)

    posf[0] = jnp.broadcast_to(pos_ref[...].astype(f32).reshape(1, rows), (8, rows))
    turn(0)
    cos_t, sin_t = trig[0, :hr], trig[0, hr:]
    qaug[...] = jnp.zeros_like(qaug)
    vt[:, vdim:, :] = jnp.ones((vt.shape[0], vt.shape[1] - vdim, vt.shape[2]), vt.dtype)
    acc[...] = jnp.zeros_like(acc)
    for c in x_loads + w_loads[:1]:
        c.wait()
    for c in uq_loads[:1] + w_loads[2:] + uq_loads[1:]:
        c.start()

    def x_rows(cut):
        return jnp.concatenate([p_buf[i, cut, :] for i in range(tiles)], axis=1)

    kvt = lax.dot_general(wdkv[...], x_rows(slice(0, rows)), NT, preferred_element_type=f32)
    rank = ckv.shape[2]
    a = kvt[:rank]
    norm = a * lax.rsqrt(jnp.sum(a * a, axis=0, keepdims=True) / rank + NORM_EPS)
    c_own = (norm.T * gkv_ref[...].reshape(1, rank)).astype(bf16)
    ckv[me] = c_own
    ckv_out[...] = c_own
    z1, z2 = kvt[rank:rank + hr], kvt[rank + hr:]
    pe_own = jnp.concatenate([z1 * cos_t - z2 * sin_t, z2 * cos_t + z1 * sin_t], axis=0).astype(bf16)
    pet[me] = pe_own
    cpe_out[...] = pe_own
    w_loads[1].wait()
    def query_latent(part):
        ql = lax.dot_general(x_rows(cols(part)), wo[:, :qrank], NN, preferred_element_type=f32)
        ql = ql * lax.rsqrt(jnp.sum(ql * ql, axis=1, keepdims=True) / qrank + NORM_EPS) * gq_ref[...].reshape(1, qrank)
        qlat[0, cols(part)] = ql.astype(bf16)

    query_latent(0)
    pl.semaphore_wait(barrier, groups - 1)

    @pl.when(me == 0)
    def _():
        for t in (1, 3):
            start(latent_copies(me, t))

    @pl.when(me == 1)
    def _():
        for t in (2, 0):
            start(latent_copies(me, t))

    @pl.when(me == 2)
    def _():
        start(latent_copies(me, 3))

    query_latent(1)
    unpack_rope(me)
    @pl.when(me == 2)
    def _():
        start(query_copies(3))

    @pl.when(me == 3)
    def _():
        start(query_halves())
        start(latent_copies(me, 0))

    FULL = ((0, 0), (1, 0), (0, 1), (1, 1))
    OWN = ((0, 0), (0, 1), (1, 1))
    row_i = lax.broadcasted_iota(jnp.int32, (half, half), 0)
    col_i = lax.broadcasted_iota(jnp.int32, (half, half), 1)

    def score_stage(u, blk, own, gi):
        tops = [None, None]

        def place(s, k, i):
            s_buf[u, cols(k), cols(i)] = s
            top = jnp.max(s, axis=0, keepdims=True)
            tops[i] = top if tops[i] is None else jnp.maximum(tops[i], top)

        def dot(k0, k1, i0, i1):
            lhs = jnp.concatenate([kn[u // 2, pl.ds(pl.multiple_of(blk * rows + k0 * half, half), (k1 - k0) * half), :],
                                   pen[blk, k0 * half:k1 * half, :]], axis=1)
            return lax.dot_general(lhs, qaug[lax.rem(gi, 2), u, :, i0 * half:i1 * half], NN, preferred_element_type=f32)

        if own:
            s = dot(0, 1, 0, 2)
            place(jnp.where(row_i <= col_i, s[:, :half], -jnp.inf), 0, 0)
            place(s[:, half:], 0, 1)
            place(jnp.where(row_i <= col_i, dot(1, 2, 1, 2), -jnp.inf), 1, 1)
            s_buf[u, cols(1), cols(0)] = jnp.full((half, half), -jnp.inf, f32)
        else:
            s = dot(0, 2, 0, 2)
            for k, i in FULL:
                place(s[cols(k), cols(i)], k, i)
        for i in range(2):
            c_buf[u, :, cols(i)] = tops[i]

    def exp_stage(u, slot):
        h = slot * GROUP + u
        m_old = m_s[h]
        m_new = jnp.maximum(m_old, c_buf[u])
        al_buf[u] = jnp.exp2((m_old - m_new) * scale2)
        m_s[h] = m_new
        for k, i in FULL:
            p_buf[u, cols(k), cols(i)] = jnp.exp2((s_buf[u, cols(k), cols(i)] - m_new[:, cols(i)]) * scale2).astype(bf16)

    def value_stage(u, slot, blk):
        h = slot * GROUP + u
        v = vt[h, :, pl.ds(pl.multiple_of(blk * rows, rows), rows)]
        for i in range(2):
            t = lax.dot_general(v, p_buf[u, :, cols(i)], NN, preferred_element_type=f32)
            acc[h, :, cols(i)] = t + acc[h, :, cols(i)] * al_buf[u, :, cols(i)]

    def place_of(gi):
        helping = gi == help_turn
        target = jnp.where(helping, partner, me)
        grp = jnp.where(helping, help_group, gi - (gi > help_turn).astype(jnp.int32))
        return helping, target, grp, lax.rem(gi, SLOTS)

    def help_copy(grp, to):
        return remote(o_help, o_nat.at[pl.ds(grp * pairs, pairs)], o_send, o_recv.at[grp], to)

    def finish(slot, gi):
        outs = []
        for j in range(pairs):
            t = jnp.concatenate([acc[slot * GROUP + h, :vdim, :] / acc[slot * GROUP + h, vdim:vdim + 1, :] for h in (2 * j, 2 * j + 1)], axis=0)
            outs.append(t.T.astype(bf16))
        for h in range(GROUP):
            acc[slot * GROUP + h] = jnp.zeros(acc.shape[1:], f32)

        helping, _, grp, _ = place_of(gi)

        @pl.when(jnp.logical_not(helping))
        def _():
            for j in range(pairs):
                o_nat[grp * pairs + j] = outs[j]

        @pl.when(helping)
        def _():
            for j in range(pairs):
                o_help[j] = outs[j]
            help_copy(help_group, partner).start()

    def step(carry, new, own, after=None, values_only=False):
        (slot1, _, _, _), (slot2, blk2, last2, gi2) = carry
        for u in range(GROUP):
            value_stage(u, slot2, blk2)
            if not values_only:
                exp_stage(u, slot1)
            if new is not None:
                score_stage(u, new[1], own, new[3])
        if after is not None:
            after()

        @pl.when(last2 == 1)
        def _():
            finish(slot2, gi2)

    def keys_and_values(slot, head0, blk):
        c = ckv[blk]
        at = pl.multiple_of(blk * rows, rows)
        for j in range(GROUP // 4):
            wk = wuk[pl.ds(pl.multiple_of((head0 + 4 * j) * nope, 4 * nope), 4 * nope), :]
            kk = lax.dot_general(c, wk, NT, preferred_element_type=f32).astype(bf16)
            kn[2 * j, pl.ds(at, rows), :] = kk[:, :128]
            kn[2 * j + 1, pl.ds(at, rows), :] = kk[:, 128:]
            wv = wuv[pl.ds(pl.multiple_of((head0 + 4 * j) * vdim, 4 * vdim), 4 * vdim), :]
            vv = lax.dot_general(wv, c, NT, preferred_element_type=f32).astype(bf16)
            for i in range(4):
                vt[slot * GROUP + 4 * j + i, :vdim, pl.ds(at, rows)] = vv[i * vdim:(i + 1) * vdim, :]

    def queries(buf, src, head0):
        ct, st = trig[src, :hr], trig[src, hr:]
        for j in range(GROUP // 4):
            w = wuq[pl.ds(pl.multiple_of((head0 + 4 * j) * qk, 4 * qk), 4 * qk), :]
            q = lax.dot_general(w, qlat[src], NT, preferred_element_type=f32)
            for i in range(4):
                u = 4 * j + i
                qh = q[i * qk:(i + 1) * qk]
                lo = (u % 2) * nope
                qaug[buf, u, lo:lo + nope, :] = qh[:nope].astype(bf16)
                r1, r2 = qh[nope:nope + hr], qh[nope + hr:]
                qaug[buf, u, 2 * nope:2 * nope + rot, :] = jnp.concatenate([r1 * ct - r2 * st, r2 * ct + r1 * st], axis=0).astype(bf16)

    def clear(slot):
        for u in range(GROUP):
            m_s[slot * GROUP + u] = jnp.full((1, rows), -jnp.inf, f32)

    def block_at(helping, target, i):
        usual = jnp.where(i == 0, target, lax.rem(i + target - 2, jnp.maximum(target, 1)))
        return jnp.where(helping & (me < 2), jnp.where(i < 2, i, 5 - i), usual)

    def group(gi, carry):
        helping, target, grp, slot = place_of(gi)
        gn = jnp.minimum(gi + 1, n_all - 1)
        helping_n, target_n, grp_n, _ = place_of(gn)
        slot_n = lax.rem(gi + 1, SLOTS)

        @pl.when((gi == help_turn - 1) & ((me == 1) | (me == 3)))
        def _():
            for c in query_copies(me):
                c.wait_recv()
            turn(1)

        @pl.when((gi == help_turn - 1) & (me == 0))
        def _():
            for c in query_halves()[1:] + (query_relay(),):
                c.wait_recv()
            start(query_share())
            turn(1)

        @pl.when(gi == 0)
        def _():
            for c in uq_loads[1:]:
                c.wait()

        @pl.when(gi == 1)
        def _():
            for c in wo_loads:
                c.start()

        fresh = ((gi == 0) & (me > 0)) | (helping & (me < 2))

        def one(i, carry):
            blk = block_at(helping, target, i)
            more = i < target
            blk_n = jnp.where(more, block_at(helping, target, i + 1), block_at(helping_n, target_n, 0))

            @pl.when(fresh & more & (blk_n != me))
            def _():
                received(blk_n)

                @pl.when((me >= 2) & (blk_n == 3 - me))
                def _():
                    start(forward_copies(blk_n))

                @pl.when((me == 0) & (blk_n >= 2))
                def _():
                    start(latent_share(blk_n))

            new = (slot, blk, (i == target).astype(jnp.int32), gi)

            def next_keys():
                keys_and_values(jnp.where(more, slot, slot_n), jnp.where(more, grp, grp_n) * GROUP, blk_n)

            def after_own():
                queries(lax.rem(gi + 1, 2), helping_n.astype(jnp.int32), grp_n * GROUP)
                next_keys()
                clear(slot_n)

            @pl.when(blk == target)
            def _():
                step(carry, new, True, after_own)

            @pl.when(blk != target)
            def _():
                step(carry, new, False, next_keys)

            return new, carry[0]

        carry = lax.fori_loop(0, target + 1, one, carry)

        @pl.when(gi == 1)
        def _():
            for u in range(GROUP):
                acc[(SLOTS - 1) * GROUP + u] = jnp.zeros(acc.shape[1:], f32)

        return carry

    idle = (jnp.int32(SLOTS - 1), jnp.int32(0), jnp.int32(0), jnp.int32(0))
    uq_loads[0].wait()
    queries(0, 0, 0)

    @pl.when(me == 2)
    def _():
        query_halves()[0].wait_recv()
        query_relay().start()
        start(latent_copies(me, 0))

    for c in w_loads[2:]:
        c.wait()

    @pl.when(me >= 0)
    def _():
        keys_and_values(0, 0, me)
        clear(0)

    carry = lax.fori_loop(0, n_all, group, (idle, idle))
    step(carry, None, False)
    step((idle, carry[0]), None, False, values_only=True)

    for c in wo_loads:
        c.wait()
    deep = GROUP * vdim
    outs = [pltpu.make_async_copy(p_buf.at[n], out_hbm.at[:, pl.ds(n * rows, rows)], out_sem.at[n]) for n in range(tiles)]
    def product(grp, n):
        lhs = jnp.concatenate([o_nat[grp * pairs + j] for j in range(pairs)], axis=1)
        w = wo[pl.ds(pl.multiple_of(grp * deep, deep), deep), n * rows:(n + 1) * rows]
        return lax.dot_general(lhs, w, NN, preferred_element_type=f32)

    def arrive(grp):
        @pl.when(grp >= n_own)
        def _():
            help_copy(grp, me).wait_recv()

    for n in range(tiles):
        s_buf[n] = jnp.zeros((rows, rows), f32)

    def accumulate(grp, c):
        arrive(grp)
        for n in range(tiles):
            s_buf[n] = product(grp, n) + s_buf[n]
        return c

    lax.fori_loop(0, ngroup - 1, accumulate, 0)
    arrive(ngroup - 1)
    for n in range(tiles):
        p_buf[n] = (product(ngroup - 1, n) + s_buf[n]).astype(bf16)
        outs[n].start()
    def sent(copies):
        for c in copies:
            c.wait_send()

    @pl.when(me == 0)
    def _():
        sent(latent_copies(me, 1) + latent_copies(me, 3) + query_share() + latent_share(2) + latent_share(3))

    @pl.when(me == 1)
    def _():
        sent(latent_copies(me, 2) + latent_copies(me, 0))

    @pl.when(me == 2)
    def _():
        sent(latent_copies(me, 3) + latent_copies(me, 0) + forward_copies(1) + query_copies(3) + (query_relay(),))

    @pl.when(me == 3)
    def _():
        sent(latent_copies(me, 0) + forward_copies(0) + query_halves())

    @pl.when(helped > 0)
    def _():
        help_copy(help_group, partner).wait_send()

    for c in outs:
        c.wait()


def layer(pos, gq, gkv, x, wdkv, wdq, wuq, wuk, wuv, wo, scale2, heads, groups):
    rows, dim = x.shape
    rank = gkv.shape[0]
    rot = wdkv.shape[0] - rank
    qrank = wdq.shape[1]
    nope = wuk.shape[0] // heads
    vdim = wuv.shape[0] // heads
    seq = rows * groups
    vm = pl.BlockSpec(memory_space=pltpu.VMEM)
    anym = pl.BlockSpec(memory_space=pltpu.HBM)
    f32 = jnp.float32
    bf16 = jnp.bfloat16
    dma = pltpu.SemaphoreType.DMA
    return pl.pallas_call(
        functools.partial(layer_kernel, scale2=scale2, rows=rows, nope=nope, rot=rot, vdim=vdim, heads=heads, groups=groups),
        out_shape=(jax.ShapeDtypeStruct((rows, dim), bf16),
                   jax.ShapeDtypeStruct((rows, rank), bf16),
                   jax.ShapeDtypeStruct((rot, rows), bf16)),
        in_specs=[vm, vm, vm] + [anym] * 7,
        out_specs=(anym, vm, vm),
        scratch_shapes=[
            pltpu.VMEM(wdkv.shape, bf16),
            pltpu.VMEM(wo.shape, bf16),
            pltpu.VMEM(wuq.shape, bf16),
            pltpu.VMEM(wuk.shape, bf16),
            pltpu.VMEM(wuv.shape, bf16),
            pltpu.VMEM((2, rows, qrank), bf16),
            pltpu.VMEM((2, 8, rows), f32),
            pltpu.VMEM((2, rot, rows), f32),
            pltpu.VMEM((groups, rows, rank), bf16),
            pltpu.VMEM((groups, rot, rows), bf16),
            pltpu.VMEM((groups, rows, 128), bf16),
            pltpu.VMEM((2, GROUP, 256, rows), bf16),
            pltpu.VMEM((GROUP // 2, seq, 128), bf16),
            pltpu.VMEM((SLOTS * GROUP, vdim + 16, seq), bf16),
            pltpu.VMEM((GROUP, rows, rows), f32),
            pltpu.VMEM((GROUP, 1, rows), f32),
            pltpu.VMEM((GROUP, rows, rows), bf16),
            pltpu.VMEM((GROUP, 1, rows), f32),
            pltpu.VMEM((SLOTS * GROUP, 1, rows), f32),
            pltpu.VMEM((SLOTS * GROUP, vdim + 16, rows), f32),
            pltpu.VMEM((heads // 2, rows, 2 * vdim), bf16),
            pltpu.VMEM((GROUP // 2, rows, 2 * vdim), bf16),
            dma((x.shape[1] // rows + 4 + heads // GROUP,)),
            dma((groups,)), dma((groups,)), dma((groups,)), dma((groups,)), dma((2,)),
            dma((3,)), dma((3,)), dma, dma,
            dma, dma((heads // GROUP,)),
            dma((2,)), dma((dim // rows,)),
        ],
        compiler_params=pltpu.CompilerParams(vmem_limit_bytes=LAYER_VMEM, collective_id=0, has_side_effects=True),
        cost_estimate=pl.CostEstimate(flops=40_000_000_000, bytes_accessed=40_000_000, transcendentals=30_000_000),
    )(pos, gq, gkv, x, wdkv, wdq, wuq, wuk, wuv, wo)


def deliver_kernel(out_in, ckv_in, cpe_in, out_hbm, ckv_out, cpe_out, out, ckv, cpe, in_sem, out_sem):
    half = out.shape[0] // 2
    steps = ((ckv_in, ckv, ckv_out, None), (cpe_in, cpe, cpe_out, None), (out_in, out, out_hbm, 0), (out_in, out, out_hbm, half))

    def view(ref, start):
        return ref if start is None else ref.at[pl.ds(start, half)]

    ins = [pltpu.make_async_copy(view(a, n), view(b, n), in_sem.at[i]) for i, (a, b, _, n) in enumerate(steps)]
    outs = [pltpu.make_async_copy(view(b, n), view(c, n), out_sem.at[i]) for i, (_, b, c, n) in enumerate(steps)]
    for c in ins:
        c.start()
    for a, b in zip(ins, outs):
        a.wait()
        b.start()
    for c in outs:
        c.wait()


def deliver(*arrays):
    anym = pl.BlockSpec(memory_space=pl.ANY)
    return pl.pallas_call(
        deliver_kernel,
        in_specs=[anym] * 3,
        out_specs=(anym,) * 3,
        out_shape=tuple(jax.ShapeDtypeStruct(a.shape, a.dtype) for a in arrays),
        scratch_shapes=[pltpu.VMEM(a.shape, a.dtype) for a in arrays] + [pltpu.SemaphoreType.DMA((4,)), pltpu.SemaphoreType.DMA((4,))],
        compiler_params=pltpu.CompilerParams(vmem_limit_bytes=62 * 1024 * 1024),
        cost_estimate=pl.CostEstimate(flops=1000, bytes_accessed=6_000_000, transcendentals=0),
    )(*arrays)


def solution(mesh):
    groups = mesh.shape['sp']
    tok_spec = P(('dp', 'sp'))
    rows_spec = P(('dp', 'sp'), None)
    replicated = P()

    def local_step(tok_in, tok_pos, w_dq, g_q, w_uq, w_dkv, g_kv, w_uk, w_uv, w_o):
        heads, qk_dim = w_uq.shape[1:]
        kv_rank = g_kv.shape[0]
        rot_dim = w_dkv.shape[1] - kv_rank
        v_dim = w_uv.shape[2]
        attn_scale = (0.1 * math.log(YARN_FACTOR) + 1.0) ** 2 / math.sqrt(qk_dim)
        def flat(w):
            return jnp.transpose(w, (1, 2, 0)).reshape(-1, w.shape[0])

        attn_out, cache_kv, cache_pe = layer(tok_pos, g_q, g_kv, tok_in, w_dkv.T, w_dq, flat(w_uq), flat(w_uk), flat(w_uv), w_o.reshape(heads * v_dim, -1),
                                      attn_scale * math.log2(math.e), heads, groups)
        attn_out, cache_kv, cache_pe = deliver(attn_out, cache_kv, cache_pe)
        return attn_out, cache_kv, cache_pe.T

    return jax.shard_map(local_step, mesh=mesh, in_specs=(rows_spec, tok_spec, replicated, replicated, replicated, replicated, replicated, replicated, replicated, replicated), out_specs=(rows_spec, rows_spec, rows_spec), check_vma=False)
```

```python
import functools
import math
import jax
import jax.numpy as jnp
from jax import lax
from jax.experimental import pallas as pl
from jax.experimental.pallas import tpu as pltpu
from jax.sharding import PartitionSpec as P

ROPE_THETA = 10000.0
YARN_FACTOR = 40.0
ORIG_CTX = 4096.0
BETA_FAST = 32.0
BETA_SLOW = 1.0
NORM_EPS = 1e-6


def rope_freqs(rot_dim):
    half_dim = rot_dim // 2
    log_base = 2.0 * math.log(ROPE_THETA)
    low_idx = max(math.floor(rot_dim * math.log(ORIG_CTX / (BETA_FAST * 2.0 * math.pi)) / log_base), 0)
    high_idx = min(math.ceil(rot_dim * math.log(ORIG_CTX / (BETA_SLOW * 2.0 * math.pi)) / log_base), half_dim - 1)
    spread = max(high_idx - low_idx, 0.001)
    freq_list = []
    for freq_idx in range(half_dim):
        base_freq = ROPE_THETA ** (-2.0 * freq_idx / rot_dim)
        ramp_val = min(max((freq_idx - low_idx) / spread, 0.0), 1.0)
        freq_list.append(base_freq / YARN_FACTOR * ramp_val + base_freq * (1.0 - ramp_val))
    return freq_list


GROUP = 8
SLOTS = 3
LAYER_VMEM = 65500000


def layer_kernel(pos_ref, gq_ref, gkv_ref, x_hbm, wdkv_hbm, wdq_hbm, wuq_hbm, wuk_hbm, wuv_hbm, wo_hbm,
                 out_hbm, ckv_out, cpe_out,
                 wdkv, wo, wuq, wuk, wuv, qlat, posf, trig, ckv, pet, pen, qaug, kn, vt,
                 s_buf, c_buf, p_buf, al_buf, m_s, acc, o_nat, o_help,
                 load_sem, c_send, c_recv, pe_send, pe_recv, f_send, q_send, q_recv, t_send, t_recv, o_send, o_recv, wo_sem, out_sem,
                 *, scale2, rows, nope, rot, vdim, heads, groups):
    f32 = jnp.float32
    bf16 = jnp.bfloat16
    NT = (((1,), (1,)), ((), ()))
    NN = (((1,), (0,)), ((), ()))
    half = rows // 2
    qk = nope + rot
    pairs = GROUP // 2
    ngroup = heads // GROUP
    me = lax.axis_index('sp')
    given = jnp.where(me == 3, 2, jnp.where(me == 2, 1, 0))
    helped = jnp.where(me == 2, 0, 1)
    partner = jnp.where(me == 3, 2, 3)
    help_group = jnp.where(me == 1, 3, 4)
    help_turn = jnp.where(me == 2, 2 * ngroup, jnp.where(me == 3, 2, 3))
    n_own = ngroup - given
    n_all = n_own + helped

    tiles = x_hbm.shape[1] // rows
    x_loads = [pltpu.make_async_copy(x_hbm.at[:, pl.ds(i * rows, rows)], p_buf.at[i], load_sem.at[i]) for i in range(tiles)]
    qrank = wdq_hbm.shape[1]
    part = GROUP * qk
    w_loads = [pltpu.make_async_copy(s, d, load_sem.at[tiles + i]) for i, (s, d) in enumerate(
        ((wdkv_hbm, wdkv), (wdq_hbm, wo.at[:, pl.ds(0, qrank)]), (wuk_hbm, wuk), (wuv_hbm, wuv)))]
    uq_loads = [pltpu.make_async_copy(wuq_hbm.at[pl.ds(i * part, part)], wuq.at[pl.ds(i * part, part)], load_sem.at[tiles + 4 + i]) for i in range(ngroup)]
    wide = wo_hbm.shape[1] - qrank
    wo_loads = [pltpu.make_async_copy(wo_hbm.at[:, pl.ds(a, n)], wo.at[:, pl.ds(a, n)], wo_sem.at[i])
                for i, (a, n) in enumerate(((qrank, wide), (0, qrank)))]
    for c in x_loads + w_loads[:2]:
        c.start()
    barrier = pltpu.get_barrier_semaphore()
    for d in range(1, groups):
        pl.semaphore_signal(barrier, inc=1, device_id={'sp': lax.rem(me + d, groups)}, device_id_type=pl.DeviceIdType.MESH)

    def remote(s, d, ssem, rsem, to):
        return pltpu.make_async_remote_copy(src_ref=s, dst_ref=d, send_sem=ssem, recv_sem=rsem,
                                            device_id={'sp': to}, device_id_type=pl.DeviceIdType.MESH)

    def latent_copies(origin, to):
        return (remote(ckv.at[origin], ckv.at[origin], c_send.at[to], c_recv.at[origin], to),
                remote(pet.at[origin], pet.at[origin], pe_send.at[to], pe_recv.at[origin], to))

    def forward_copies(origin):
        to = 5 - me
        return (remote(ckv.at[origin], ckv.at[origin], f_send.at[0], c_recv.at[origin], to),
                remote(pet.at[origin], pet.at[origin], f_send.at[1], pe_recv.at[origin], to))

    def query_copies(to):
        return (remote(qlat.at[0], qlat.at[1], q_send.at[0], q_recv.at[0], to),
                remote(posf.at[0], posf.at[1], t_send, t_recv, to))

    def query_halves():
        top, low = pl.ds(0, half), pl.ds(half, half)
        return (remote(qlat.at[0, top], qlat.at[1, top], q_send.at[1], q_recv.at[1], 2),
                remote(posf.at[0], posf.at[1], t_send, t_recv, 0),
                remote(qlat.at[0, low], qlat.at[1, low], q_send.at[0], q_recv.at[0], 0))

    def query_relay():
        top = pl.ds(0, half)
        return remote(qlat.at[1, top], qlat.at[1, top], q_send.at[2], q_recv.at[2], 0)

    def query_share():
        return (remote(qlat.at[1], qlat.at[1], q_send.at[0], q_recv.at[0], 1),
                remote(posf.at[1], posf.at[1], t_send, t_recv, 1))

    def latent_share(origin):
        spare = 6 - 2 * origin
        return (remote(ckv.at[origin], ckv.at[origin], c_send.at[spare], c_recv.at[origin], 1),
                remote(pet.at[origin], pet.at[origin], pe_send.at[spare], pe_recv.at[origin], 1))

    def start(copies):
        for c in copies:
            c.start()

    def received(origin):
        for c in latent_copies(origin, me):
            c.wait_recv()
        unpack_rope(origin)

    def unpack_rope(origin):
        wide = jnp.concatenate([pet[origin].astype(f32), jnp.zeros((128 - rot, rows), f32)], axis=0)
        pen[origin] = wide.T.astype(bf16)

    hr = rot // 2

    def cols(i):
        return slice(i * half, (i + 1) * half)

    freq_i = lax.broadcasted_iota(jnp.int32, (hr, rows), 0)
    freq = jnp.zeros((hr, rows), f32)
    for i, f in enumerate(rope_freqs(rot)):
        freq = jnp.where(freq_i == i, f, freq)

    def turn(i):
        angle = posf[i, :1] * freq
        trig[i, :hr] = jnp.cos(angle)
        trig[i, hr:] = jnp.sin(angle)

    posf[0] = jnp.broadcast_to(pos_ref[...].astype(f32).reshape(1, rows), (8, rows))
    turn(0)
    cos_t, sin_t = trig[0, :hr], trig[0, hr:]
    qaug[...] = jnp.zeros_like(qaug)
    vt[:, vdim:, :] = jnp.ones((vt.shape[0], vt.shape[1] - vdim, vt.shape[2]), vt.dtype)
    acc[...] = jnp.zeros_like(acc)
    for c in x_loads + w_loads[:1]:
        c.wait()
    for c in uq_loads[:1] + w_loads[2:] + uq_loads[1:]:
        c.start()

    def x_rows(cut):
        return jnp.concatenate([p_buf[i, cut, :] for i in range(tiles)], axis=1)

    kvt = lax.dot_general(wdkv[...], x_rows(slice(0, rows)), NT, preferred_element_type=f32)
    rank = ckv.shape[2]
    a = kvt[:rank]
    norm = a * lax.rsqrt(jnp.sum(a * a, axis=0, keepdims=True) / rank + NORM_EPS)
    c_own = (norm.T * gkv_ref[...].reshape(1, rank)).astype(bf16)
    ckv[me] = c_own
    ckv_out[...] = c_own
    z1, z2 = kvt[rank:rank + hr], kvt[rank + hr:]
    pe_own = jnp.concatenate([z1 * cos_t - z2 * sin_t, z2 * cos_t + z1 * sin_t], axis=0).astype(bf16)
    pet[me] = pe_own
    cpe_out[...] = pe_own
    w_loads[1].wait()
    def query_latent(part):
        ql = lax.dot_general(x_rows(cols(part)), wo[:, :qrank], NN, preferred_element_type=f32)
        ql = ql * lax.rsqrt(jnp.sum(ql * ql, axis=1, keepdims=True) / qrank + NORM_EPS) * gq_ref[...].reshape(1, qrank)
        qlat[0, cols(part)] = ql.astype(bf16)

    query_latent(0)
    pl.semaphore_wait(barrier, groups - 1)

    @pl.when(me == 0)
    def _():
        for t in (1, 3):
            start(latent_copies(me, t))

    @pl.when(me == 1)
    def _():
        for t in (2, 0):
            start(latent_copies(me, t))

    @pl.when(me == 2)
    def _():
        start(latent_copies(me, 3))

    @pl.when(me == 3)
    def _():
        query_halves()[0].start()

    query_latent(1)
    unpack_rope(me)
    @pl.when(me == 2)
    def _():
        start(query_copies(3))
        query_halves()[0].wait_recv()
        query_relay().start()
        start(latent_copies(me, 0))

    @pl.when(me == 3)
    def _():
        start(query_halves()[1:])
        start(latent_copies(me, 0))

    FULL = ((0, 0), (1, 0), (0, 1), (1, 1))
    OWN = ((0, 0), (0, 1), (1, 1))
    row_i = lax.broadcasted_iota(jnp.int32, (half, half), 0)
    col_i = lax.broadcasted_iota(jnp.int32, (half, half), 1)

    def score_stage(u, blk, own, gi):
        tops = [None, None]

        def place(s, k, i):
            s_buf[u, cols(k), cols(i)] = s
            top = jnp.max(s, axis=0, keepdims=True)
            tops[i] = top if tops[i] is None else jnp.maximum(tops[i], top)

        def dot(k0, k1, i0, i1):
            lhs = jnp.concatenate([kn[u // 2, pl.ds(pl.multiple_of(blk * rows + k0 * half, half), (k1 - k0) * half), :],
                                   pen[blk, k0 * half:k1 * half, :]], axis=1)
            return lax.dot_general(lhs, qaug[lax.rem(gi, 2), u, :, i0 * half:i1 * half], NN, preferred_element_type=f32)

        if own:
            s = dot(0, 1, 0, 2)
            place(jnp.where(row_i <= col_i, s[:, :half], -jnp.inf), 0, 0)
            place(s[:, half:], 0, 1)
            place(jnp.where(row_i <= col_i, dot(1, 2, 1, 2), -jnp.inf), 1, 1)
            s_buf[u, cols(1), cols(0)] = jnp.full((half, half), -jnp.inf, f32)
        else:
            s = dot(0, 2, 0, 2)
            for k, i in FULL:
                place(s[cols(k), cols(i)], k, i)
        for i in range(2):
            c_buf[u, :, cols(i)] = tops[i]

    def exp_stage(u, slot):
        h = slot * GROUP + u
        m_old = m_s[h]
        m_new = jnp.maximum(m_old, c_buf[u])
        al_buf[u] = jnp.exp2((m_old - m_new) * scale2)
        m_s[h] = m_new
        for k, i in FULL:
            p_buf[u, cols(k), cols(i)] = jnp.exp2((s_buf[u, cols(k), cols(i)] - m_new[:, cols(i)]) * scale2).astype(bf16)

    def value_stage(u, slot, blk):
        h = slot * GROUP + u
        v = vt[h, :, pl.ds(pl.multiple_of(blk * rows, rows), rows)]
        for i in range(2):
            t = lax.dot_general(v, p_buf[u, :, cols(i)], NN, preferred_element_type=f32)
            acc[h, :, cols(i)] = t + acc[h, :, cols(i)] * al_buf[u, :, cols(i)]

    def place_of(gi):
        helping = gi == help_turn
        target = jnp.where(helping, partner, me)
        grp = jnp.where(helping, help_group, gi - (gi > help_turn).astype(jnp.int32))
        return helping, target, grp, lax.rem(gi, SLOTS)

    def help_copy(grp, to):
        return remote(o_help, o_nat.at[pl.ds(grp * pairs, pairs)], o_send, o_recv.at[grp], to)

    def finish(slot, gi):
        outs = []
        for j in range(pairs):
            t = jnp.concatenate([acc[slot * GROUP + h, :vdim, :] / acc[slot * GROUP + h, vdim:vdim + 1, :] for h in (2 * j, 2 * j + 1)], axis=0)
            outs.append(t.T.astype(bf16))
        for h in range(GROUP):
            acc[slot * GROUP + h] = jnp.zeros(acc.shape[1:], f32)

        helping, _, grp, _ = place_of(gi)

        @pl.when(jnp.logical_not(helping))
        def _():
            for j in range(pairs):
                o_nat[grp * pairs + j] = outs[j]

        @pl.when(helping)
        def _():
            for j in range(pairs):
                o_help[j] = outs[j]
            help_copy(help_group, partner).start()

    def step(carry, new, own, after=None, values_only=False):
        (slot1, _, _, _), (slot2, blk2, last2, gi2) = carry
        for u in range(GROUP):
            value_stage(u, slot2, blk2)
            if not values_only:
                exp_stage(u, slot1)
            if new is not None:
                score_stage(u, new[1], own, new[3])
        if after is not None:
            after()

        @pl.when(last2 == 1)
        def _():
            finish(slot2, gi2)

    def keys_and_values(slot, head0, blk):
        c = ckv[blk]
        at = pl.multiple_of(blk * rows, rows)
        for j in range(GROUP // 4):
            wk = wuk[pl.ds(pl.multiple_of((head0 + 4 * j) * nope, 4 * nope), 4 * nope), :]
            kk = lax.dot_general(c, wk, NT, preferred_element_type=f32).astype(bf16)
            kn[2 * j, pl.ds(at, rows), :] = kk[:, :128]
            kn[2 * j + 1, pl.ds(at, rows), :] = kk[:, 128:]
            wv = wuv[pl.ds(pl.multiple_of((head0 + 4 * j) * vdim, 4 * vdim), 4 * vdim), :]
            vv = lax.dot_general(wv, c, NT, preferred_element_type=f32).astype(bf16)
            for i in range(4):
                vt[slot * GROUP + 4 * j + i, :vdim, pl.ds(at, rows)] = vv[i * vdim:(i + 1) * vdim, :]

    def queries(buf, src, head0):
        ct, st = trig[src, :hr], trig[src, hr:]
        for j in range(GROUP // 4):
            w = wuq[pl.ds(pl.multiple_of((head0 + 4 * j) * qk, 4 * qk), 4 * qk), :]
            q = lax.dot_general(w, qlat[src], NT, preferred_element_type=f32)
            for i in range(4):
                u = 4 * j + i
                qh = q[i * qk:(i + 1) * qk]
                lo = (u % 2) * nope
                qaug[buf, u, lo:lo + nope, :] = qh[:nope].astype(bf16)
                r1, r2 = qh[nope:nope + hr], qh[nope + hr:]
                qaug[buf, u, 2 * nope:2 * nope + rot, :] = jnp.concatenate([r1 * ct - r2 * st, r2 * ct + r1 * st], axis=0).astype(bf16)

    def clear(slot):
        for u in range(GROUP):
            m_s[slot * GROUP + u] = jnp.full((1, rows), -jnp.inf, f32)

    def block_at(helping, target, i):
        usual = jnp.where(i == 0, target, lax.rem(i + target - 2, jnp.maximum(target, 1)))
        return jnp.where(helping & (me < 2), jnp.where(i < 2, i, 5 - i), usual)

    def group(gi, carry):
        helping, target, grp, slot = place_of(gi)
        gn = jnp.minimum(gi + 1, n_all - 1)
        helping_n, target_n, grp_n, _ = place_of(gn)
        slot_n = lax.rem(gi + 1, SLOTS)

        @pl.when((gi == help_turn - 1) & ((me == 1) | (me == 3)))
        def _():
            for c in query_copies(me):
                c.wait_recv()
            turn(1)

        @pl.when((gi == help_turn - 1) & (me == 0))
        def _():
            for c in query_halves()[1:] + (query_relay(),):
                c.wait_recv()
            start(query_share())
            turn(1)

        @pl.when(gi == 0)
        def _():
            for c in uq_loads[1:]:
                c.wait()

        @pl.when(gi == 1)
        def _():
            for c in wo_loads:
                c.start()

        fresh = ((gi == 0) & (me > 0)) | (helping & (me < 2))

        def one(i, carry):
            blk = block_at(helping, target, i)
            more = i < target
            blk_n = jnp.where(more, block_at(helping, target, i + 1), block_at(helping_n, target_n, 0))

            @pl.when(fresh & more & (blk_n != me))
            def _():
                received(blk_n)

                @pl.when((me >= 2) & (blk_n == 3 - me))
                def _():
                    start(forward_copies(blk_n))

                @pl.when((me == 0) & (blk_n >= 2))
                def _():
                    start(latent_share(blk_n))

            new = (slot, blk, (i == target).astype(jnp.int32), gi)

            def next_keys():
                keys_and_values(jnp.where(more, slot, slot_n), jnp.where(more, grp, grp_n) * GROUP, blk_n)

            def after_own():
                queries(lax.rem(gi + 1, 2), helping_n.astype(jnp.int32), grp_n * GROUP)
                next_keys()
                clear(slot_n)

            @pl.when(blk == target)
            def _():
                step(carry, new, True, after_own)

            @pl.when(blk != target)
            def _():
                step(carry, new, False, next_keys)

            return new, carry[0]

        carry = lax.fori_loop(0, target + 1, one, carry)

        @pl.when(gi == 1)
        def _():
            for u in range(GROUP):
                acc[(SLOTS - 1) * GROUP + u] = jnp.zeros(acc.shape[1:], f32)

        return carry

    idle = (jnp.int32(SLOTS - 1), jnp.int32(0), jnp.int32(0), jnp.int32(0))
    uq_loads[0].wait()
    queries(0, 0, 0)

    for c in w_loads[2:]:
        c.wait()

    @pl.when(me >= 0)
    def _():
        keys_and_values(0, 0, me)
        clear(0)

    carry = lax.fori_loop(0, n_all, group, (idle, idle))
    step(carry, None, False)
    step((idle, carry[0]), None, False, values_only=True)

    for c in wo_loads:
        c.wait()
    deep = GROUP * vdim
    outs = [pltpu.make_async_copy(p_buf.at[n], out_hbm.at[:, pl.ds(n * rows, rows)], out_sem.at[n]) for n in range(tiles)]
    def product(grp, n):
        lhs = jnp.concatenate([o_nat[grp * pairs + j] for j in range(pairs)], axis=1)
        w = wo[pl.ds(pl.multiple_of(grp * deep, deep), deep), n * rows:(n + 1) * rows]
        return lax.dot_general(lhs, w, NN, preferred_element_type=f32)

    def arrive(grp):
        @pl.when(grp >= n_own)
        def _():
            help_copy(grp, me).wait_recv()

    for n in range(tiles):
        s_buf[n] = jnp.zeros((rows, rows), f32)

    def accumulate(grp, c):
        arrive(grp)
        for n in range(tiles):
            s_buf[n] = product(grp, n) + s_buf[n]
        return c

    lax.fori_loop(0, ngroup - 1, accumulate, 0)
    arrive(ngroup - 1)
    for n in range(tiles):
        p_buf[n] = (product(ngroup - 1, n) + s_buf[n]).astype(bf16)
        outs[n].start()
    def sent(copies):
        for c in copies:
            c.wait_send()

    @pl.when(me == 0)
    def _():
        sent(latent_copies(me, 1) + latent_copies(me, 3) + query_share() + latent_share(2) + latent_share(3))

    @pl.when(me == 1)
    def _():
        sent(latent_copies(me, 2) + latent_copies(me, 0))

    @pl.when(me == 2)
    def _():
        sent(latent_copies(me, 3) + latent_copies(me, 0) + forward_copies(1) + query_copies(3) + (query_relay(),))

    @pl.when(me == 3)
    def _():
        sent(latent_copies(me, 0) + forward_copies(0) + query_halves())

    @pl.when(helped > 0)
    def _():
        help_copy(help_group, partner).wait_send()

    for c in outs:
        c.wait()


def layer(pos, gq, gkv, x, wdkv, wdq, wuq, wuk, wuv, wo, scale2, heads, groups):
    rows, dim = x.shape
    rank = gkv.shape[0]
    rot = wdkv.shape[0] - rank
    qrank = wdq.shape[1]
    nope = wuk.shape[0] // heads
    vdim = wuv.shape[0] // heads
    seq = rows * groups
    vm = pl.BlockSpec(memory_space=pltpu.VMEM)
    anym = pl.BlockSpec(memory_space=pltpu.HBM)
    f32 = jnp.float32
    bf16 = jnp.bfloat16
    dma = pltpu.SemaphoreType.DMA
    return pl.pallas_call(
        functools.partial(layer_kernel, scale2=scale2, rows=rows, nope=nope, rot=rot, vdim=vdim, heads=heads, groups=groups),
        out_shape=(jax.ShapeDtypeStruct((rows, dim), bf16),
                   jax.ShapeDtypeStruct((rows, rank), bf16),
                   jax.ShapeDtypeStruct((rot, rows), bf16)),
        in_specs=[vm, vm, vm] + [anym] * 7,
        out_specs=(anym, vm, vm),
        scratch_shapes=[
            pltpu.VMEM(wdkv.shape, bf16),
            pltpu.VMEM(wo.shape, bf16),
            pltpu.VMEM(wuq.shape, bf16),
            pltpu.VMEM(wuk.shape, bf16),
            pltpu.VMEM(wuv.shape, bf16),
            pltpu.VMEM((2, rows, qrank), bf16),
            pltpu.VMEM((2, 8, rows), f32),
            pltpu.VMEM((2, rot, rows), f32),
            pltpu.VMEM((groups, rows, rank), bf16),
            pltpu.VMEM((groups, rot, rows), bf16),
            pltpu.VMEM((groups, rows, 128), bf16),
            pltpu.VMEM((2, GROUP, 256, rows), bf16),
            pltpu.VMEM((GROUP // 2, seq, 128), bf16),
            pltpu.VMEM((SLOTS * GROUP, vdim + 16, seq), bf16),
            pltpu.VMEM((GROUP, rows, rows), f32),
            pltpu.VMEM((GROUP, 1, rows), f32),
            pltpu.VMEM((GROUP, rows, rows), bf16),
            pltpu.VMEM((GROUP, 1, rows), f32),
            pltpu.VMEM((SLOTS * GROUP, 1, rows), f32),
            pltpu.VMEM((SLOTS * GROUP, vdim + 16, rows), f32),
            pltpu.VMEM((heads // 2, rows, 2 * vdim), bf16),
            pltpu.VMEM((GROUP // 2, rows, 2 * vdim), bf16),
            dma((x.shape[1] // rows + 4 + heads // GROUP,)),
            dma((groups,)), dma((groups,)), dma((groups,)), dma((groups,)), dma((2,)),
            dma((3,)), dma((3,)), dma, dma,
            dma, dma((heads // GROUP,)),
            dma((2,)), dma((dim // rows,)),
        ],
        compiler_params=pltpu.CompilerParams(vmem_limit_bytes=LAYER_VMEM, collective_id=0, has_side_effects=True),
        cost_estimate=pl.CostEstimate(flops=40_000_000_000, bytes_accessed=40_000_000, transcendentals=30_000_000),
    )(pos, gq, gkv, x, wdkv, wdq, wuq, wuk, wuv, wo)


def deliver_kernel(out_in, ckv_in, cpe_in, out_hbm, ckv_out, cpe_out, out, ckv, cpe, in_sem, out_sem):
    half = out.shape[0] // 2
    steps = ((ckv_in, ckv, ckv_out, None), (cpe_in, cpe, cpe_out, None), (out_in, out, out_hbm, 0), (out_in, out, out_hbm, half))

    def view(ref, start):
        return ref if start is None else ref.at[pl.ds(start, half)]

    ins = [pltpu.make_async_copy(view(a, n), view(b, n), in_sem.at[i]) for i, (a, b, _, n) in enumerate(steps)]
    outs = [pltpu.make_async_copy(view(b, n), view(c, n), out_sem.at[i]) for i, (_, b, c, n) in enumerate(steps)]
    for c in ins:
        c.start()
    for a, b in zip(ins, outs):
        a.wait()
        b.start()
    for c in outs:
        c.wait()


def deliver(*arrays):
    anym = pl.BlockSpec(memory_space=pl.ANY)
    return pl.pallas_call(
        deliver_kernel,
        in_specs=[anym] * 3,
        out_specs=(anym,) * 3,
        out_shape=tuple(jax.ShapeDtypeStruct(a.shape, a.dtype) for a in arrays),
        scratch_shapes=[pltpu.VMEM(a.shape, a.dtype) for a in arrays] + [pltpu.SemaphoreType.DMA((4,)), pltpu.SemaphoreType.DMA((4,))],
        compiler_params=pltpu.CompilerParams(vmem_limit_bytes=62 * 1024 * 1024),
        cost_estimate=pl.CostEstimate(flops=1000, bytes_accessed=6_000_000, transcendentals=0),
    )(*arrays)


def solution(mesh):
    groups = mesh.shape['sp']
    tok_spec = P(('dp', 'sp'))
    rows_spec = P(('dp', 'sp'), None)
    replicated = P()

    def local_step(tok_in, tok_pos, w_dq, g_q, w_uq, w_dkv, g_kv, w_uk, w_uv, w_o):
        heads, qk_dim = w_uq.shape[1:]
        kv_rank = g_kv.shape[0]
        rot_dim = w_dkv.shape[1] - kv_rank
        v_dim = w_uv.shape[2]
        attn_scale = (0.1 * math.log(YARN_FACTOR) + 1.0) ** 2 / math.sqrt(qk_dim)
        def flat(w):
            return jnp.transpose(w, (1, 2, 0)).reshape(-1, w.shape[0])

        attn_out, cache_kv, cache_pe = layer(tok_pos, g_q, g_kv, tok_in, w_dkv.T, w_dq, flat(w_uq), flat(w_uk), flat(w_uv), w_o.reshape(heads * v_dim, -1),
                                      attn_scale * math.log2(math.e), heads, groups)
        attn_out, cache_kv, cache_pe = deliver(attn_out, cache_kv, cache_pe)
        return attn_out, cache_kv, cache_pe.T

    return jax.shard_map(local_step, mesh=mesh, in_specs=(rows_spec, tok_spec, replicated, replicated, replicated, replicated, replicated, replicated, replicated, replicated), out_specs=(rows_spec, rows_spec, rows_spec), check_vma=False)
```

```python
import functools
import math
import jax
import jax.numpy as jnp
from jax import lax
from jax.experimental import pallas as pl
from jax.experimental.pallas import tpu as pltpu
from jax.sharding import PartitionSpec as P

ROPE_THETA = 10000.0
YARN_FACTOR = 40.0
ORIG_CTX = 4096.0
BETA_FAST = 32.0
BETA_SLOW = 1.0
NORM_EPS = 1e-6


def rope_freqs(rot_dim):
    half_dim = rot_dim // 2
    log_base = 2.0 * math.log(ROPE_THETA)
    low_idx = max(math.floor(rot_dim * math.log(ORIG_CTX / (BETA_FAST * 2.0 * math.pi)) / log_base), 0)
    high_idx = min(math.ceil(rot_dim * math.log(ORIG_CTX / (BETA_SLOW * 2.0 * math.pi)) / log_base), half_dim - 1)
    spread = max(high_idx - low_idx, 0.001)
    freq_list = []
    for freq_idx in range(half_dim):
        base_freq = ROPE_THETA ** (-2.0 * freq_idx / rot_dim)
        ramp_val = min(max((freq_idx - low_idx) / spread, 0.0), 1.0)
        freq_list.append(base_freq / YARN_FACTOR * ramp_val + base_freq * (1.0 - ramp_val))
    return freq_list


GROUP = 8
SLOTS = 3
LAYER_VMEM = 65500000


def layer_kernel(pos_ref, gq_ref, gkv_ref, x_hbm, wdkv_hbm, wdq_hbm, wuq_hbm, wuk_hbm, wuv_hbm, wo_hbm,
                 out_hbm, ckv_out, cpe_out,
                 wdkv, wo, wuq, wuk, wuv, qlat, posf, trig, ckv, pet, pen, qaug, kn, vt,
                 s_buf, c_buf, p_buf, al_buf, m_s, acc, o_nat, o_help,
                 load_sem, c_send, c_recv, pe_send, pe_recv, f_send, q_send, q_recv, t_send, t_recv, o_send, o_recv, wo_sem, out_sem,
                 *, scale2, rows, nope, rot, vdim, heads, groups):
    f32 = jnp.float32
    bf16 = jnp.bfloat16
    NT = (((1,), (1,)), ((), ()))
    NN = (((1,), (0,)), ((), ()))
    half = rows // 2
    qk = nope + rot
    pairs = GROUP // 2
    ngroup = heads // GROUP
    me = lax.axis_index('sp')
    given = jnp.where(me == 3, 2, jnp.where(me == 2, 1, 0))
    helped = jnp.where(me == 2, 0, 1)
    partner = jnp.where(me == 3, 2, 3)
    help_group = jnp.where(me == 1, 3, 4)
    help_turn = jnp.where(me == 2, 2 * ngroup, jnp.where(me == 3, 2, 3))
    n_own = ngroup - given
    n_all = n_own + helped

    tiles = x_hbm.shape[1] // rows
    x_loads = [pltpu.make_async_copy(x_hbm.at[:, pl.ds(i * rows, rows)], p_buf.at[i], load_sem.at[i]) for i in range(tiles)]
    qrank = wdq_hbm.shape[1]
    part = GROUP * qk
    w_loads = [pltpu.make_async_copy(s, d, load_sem.at[tiles + i]) for i, (s, d) in enumerate(
        ((wdkv_hbm, wdkv), (wdq_hbm, wo.at[:, pl.ds(0, qrank)]), (wuk_hbm, wuk), (wuv_hbm, wuv)))]
    uq_loads = [pltpu.make_async_copy(wuq_hbm.at[pl.ds(i * part, part)], wuq.at[pl.ds(i * part, part)], load_sem.at[tiles + 4 + i]) for i in range(ngroup)]
    wide = wo_hbm.shape[1] - qrank
    wo_loads = [pltpu.make_async_copy(wo_hbm.at[:, pl.ds(a, n)], wo.at[:, pl.ds(a, n)], wo_sem.at[i])
                for i, (a, n) in enumerate(((qrank, wide), (0, qrank)))]
    for c in x_loads + w_loads[:2]:
        c.start()
    barrier = pltpu.get_barrier_semaphore()
    for d in range(1, groups):
        pl.semaphore_signal(barrier, inc=1, device_id={'sp': lax.rem(me + d, groups)}, device_id_type=pl.DeviceIdType.MESH)

    def remote(s, d, ssem, rsem, to):
        return pltpu.make_async_remote_copy(src_ref=s, dst_ref=d, send_sem=ssem, recv_sem=rsem,
                                            device_id={'sp': to}, device_id_type=pl.DeviceIdType.MESH)

    def latent_copies(origin, to):
        return (remote(ckv.at[origin], ckv.at[origin], c_send.at[to], c_recv.at[origin], to),
                remote(pet.at[origin], pet.at[origin], pe_send.at[to], pe_recv.at[origin], to))

    def forward_copies(origin):
        to = 5 - me
        return (remote(ckv.at[origin], ckv.at[origin], f_send.at[0], c_recv.at[origin], to),
                remote(pet.at[origin], pet.at[origin], f_send.at[1], pe_recv.at[origin], to))

    def query_copies(to):
        return (remote(qlat.at[0], qlat.at[1], q_send.at[0], q_recv.at[0], to),
                remote(posf.at[0], posf.at[1], t_send, t_recv, to))

    def query_halves():
        top, low = pl.ds(0, half), pl.ds(half, half)
        return (remote(qlat.at[0, top], qlat.at[1, top], q_send.at[1], q_recv.at[1], 2),
                remote(posf.at[0], posf.at[1], t_send, t_recv, 0),
                remote(qlat.at[0, low], qlat.at[1, low], q_send.at[0], q_recv.at[0], 0))

    def query_relay():
        top = pl.ds(0, half)
        return remote(qlat.at[1, top], qlat.at[1, top], q_send.at[2], q_recv.at[2], 0)

    def query_share():
        return (remote(qlat.at[1], qlat.at[1], q_send.at[0], q_recv.at[0], 1),
                remote(posf.at[1], posf.at[1], t_send, t_recv, 1))

    def latent_share(origin):
        spare = 6 - 2 * origin
        return (remote(ckv.at[origin], ckv.at[origin], c_send.at[spare], c_recv.at[origin], 1),
                remote(pet.at[origin], pet.at[origin], pe_send.at[spare], pe_recv.at[origin], 1))

    def start(copies):
        for c in copies:
            c.start()

    def received(origin):
        for c in latent_copies(origin, me):
            c.wait_recv()
        unpack_rope(origin)

    def unpack_rope(origin):
        wide = jnp.concatenate([pet[origin].astype(f32), jnp.zeros((128 - rot, rows), f32)], axis=0)
        pen[origin] = wide.T.astype(bf16)

    hr = rot // 2

    def cols(i):
        return slice(i * half, (i + 1) * half)

    freq_i = lax.broadcasted_iota(jnp.int32, (hr, rows), 0)
    freq = jnp.zeros((hr, rows), f32)
    for i, f in enumerate(rope_freqs(rot)):
        freq = jnp.where(freq_i == i, f, freq)

    def turn(i):
        angle = posf[i, :1] * freq
        trig[i, :hr] = jnp.cos(angle)
        trig[i, hr:] = jnp.sin(angle)

    posf[0] = jnp.broadcast_to(pos_ref[...].astype(f32).reshape(1, rows), (8, rows))
    turn(0)
    cos_t, sin_t = trig[0, :hr], trig[0, hr:]
    qaug[...] = jnp.zeros_like(qaug)
    vt[:, vdim:, :] = jnp.ones((vt.shape[0], vt.shape[1] - vdim, vt.shape[2]), vt.dtype)
    acc[...] = jnp.zeros_like(acc)
    for c in x_loads + w_loads[:1]:
        c.wait()
    for c in uq_loads[:1] + w_loads[2:] + uq_loads[1:]:
        c.start()

    def x_rows(cut):
        return jnp.concatenate([p_buf[i, cut, :] for i in range(tiles)], axis=1)

    kvt = lax.dot_general(wdkv[...], x_rows(slice(0, rows)), NT, preferred_element_type=f32)
    rank = ckv.shape[2]
    a = kvt[:rank]
    norm = a * lax.rsqrt(jnp.sum(a * a, axis=0, keepdims=True) / rank + NORM_EPS)
    c_own = (norm.T * gkv_ref[...].reshape(1, rank)).astype(bf16)
    ckv[me] = c_own
    ckv_out[...] = c_own
    z1, z2 = kvt[rank:rank + hr], kvt[rank + hr:]
    pe_own = jnp.concatenate([z1 * cos_t - z2 * sin_t, z2 * cos_t + z1 * sin_t], axis=0).astype(bf16)
    pet[me] = pe_own
    cpe_out[...] = pe_own
    w_loads[1].wait()
    def query_latent(part):
        ql = lax.dot_general(x_rows(cols(part)), wo[:, :qrank], NN, preferred_element_type=f32)
        ql = ql * lax.rsqrt(jnp.sum(ql * ql, axis=1, keepdims=True) / qrank + NORM_EPS) * gq_ref[...].reshape(1, qrank)
        qlat[0, cols(part)] = ql.astype(bf16)

    query_latent(0)
    pl.semaphore_wait(barrier, groups - 1)

    @pl.when(me == 0)
    def _():
        for t in (1, 3):
            start(latent_copies(me, t))

    @pl.when(me == 1)
    def _():
        for t in (2, 0):
            start(latent_copies(me, t))

    @pl.when(me == 2)
    def _():
        start(latent_copies(me, 3))

    @pl.when(me == 3)
    def _():
        query_halves()[0].start()

    query_latent(1)
    unpack_rope(me)
    @pl.when(me == 2)
    def _():
        start(query_copies(3))
        query_halves()[0].wait_recv()
        query_relay().start()
        start(latent_copies(me, 0))

    @pl.when(me == 3)
    def _():
        start(query_halves()[1:])
        start(latent_copies(me, 0))

    FULL = ((0, 0), (1, 0), (0, 1), (1, 1))
    OWN = ((0, 0), (0, 1), (1, 1))
    row_i = lax.broadcasted_iota(jnp.int32, (half, half), 0)
    col_i = lax.broadcasted_iota(jnp.int32, (half, half), 1)

    def score_stage(u, blk, own, gi):
        tops = [None, None]

        def place(s, k, i):
            s_buf[u, cols(k), cols(i)] = s
            top = jnp.max(s, axis=0, keepdims=True)
            tops[i] = top if tops[i] is None else jnp.maximum(tops[i], top)

        def dot(k0, k1, i0, i1):
            lhs = jnp.concatenate([kn[u // 2, pl.ds(pl.multiple_of(blk * rows + k0 * half, half), (k1 - k0) * half), :],
                                   pen[blk, k0 * half:k1 * half, :]], axis=1)
            return lax.dot_general(lhs, qaug[lax.rem(gi, 2), u, :, i0 * half:i1 * half], NN, preferred_element_type=f32)

        if own:
            s = dot(0, 1, 0, 2)
            place(jnp.where(row_i <= col_i, s[:, :half], -jnp.inf), 0, 0)
            place(s[:, half:], 0, 1)
            place(jnp.where(row_i <= col_i, dot(1, 2, 1, 2), -jnp.inf), 1, 1)
            s_buf[u, cols(1), cols(0)] = jnp.full((half, half), -jnp.inf, f32)
        else:
            s = dot(0, 2, 0, 2)
            for k, i in FULL:
                place(s[cols(k), cols(i)], k, i)
        for i in range(2):
            c_buf[u, :, cols(i)] = tops[i]

    def exp_stage(u, slot):
        h = slot * GROUP + u
        m_old = m_s[h]
        m_new = jnp.maximum(m_old, c_buf[u])
        al_buf[u] = jnp.exp2((m_old - m_new) * scale2)
        m_s[h] = m_new
        for k, i in FULL:
            p_buf[u, cols(k), cols(i)] = jnp.exp2((s_buf[u, cols(k), cols(i)] - m_new[:, cols(i)]) * scale2).astype(bf16)

    def value_stage(u, slot, blk):
        h = slot * GROUP + u
        v = vt[h, :, pl.ds(pl.multiple_of(blk * rows, rows), rows)]
        for i in range(2):
            t = lax.dot_general(v, p_buf[u, :, cols(i)], NN, preferred_element_type=f32)
            acc[h, :, cols(i)] = t + acc[h, :, cols(i)] * al_buf[u, :, cols(i)]

    def place_of(gi):
        helping = gi == help_turn
        target = jnp.where(helping, partner, me)
        grp = jnp.where(helping, help_group, gi - (gi > help_turn).astype(jnp.int32))
        return helping, target, grp, lax.rem(gi, SLOTS)

    def help_copy(grp, to):
        return remote(o_help, o_nat.at[pl.ds(grp * pairs, pairs)], o_send, o_recv.at[grp], to)

    def finish(slot, gi):
        outs = []
        for j in range(pairs):
            t = jnp.concatenate([acc[slot * GROUP + h, :vdim, :] / acc[slot * GROUP + h, vdim:vdim + 1, :] for h in (2 * j, 2 * j + 1)], axis=0)
            outs.append(t.T.astype(bf16))
        for h in range(GROUP):
            acc[slot * GROUP + h] = jnp.zeros(acc.shape[1:], f32)

        helping, _, grp, _ = place_of(gi)

        @pl.when(jnp.logical_not(helping))
        def _():
            for j in range(pairs):
                o_nat[grp * pairs + j] = outs[j]

        @pl.when(helping)
        def _():
            for j in range(pairs):
                o_help[j] = outs[j]
            help_copy(help_group, partner).start()

    def step(carry, new, own, after=None, values_only=False):
        (slot1, _, _, _), (slot2, blk2, last2, gi2) = carry
        for u in range(GROUP):
            value_stage(u, slot2, blk2)
            if not values_only:
                exp_stage(u, slot1)
            if new is not None:
                score_stage(u, new[1], own, new[3])
        if after is not None:
            after()

        @pl.when(last2 == 1)
        def _():
            finish(slot2, gi2)

    def keys_and_values(slot, head0, blk):
        c = ckv[blk]
        at = pl.multiple_of(blk * rows, rows)
        for j in range(GROUP // 4):
            wk = wuk[pl.ds(pl.multiple_of((head0 + 4 * j) * nope, 4 * nope), 4 * nope), :]
            kk = lax.dot_general(c, wk, NT, preferred_element_type=f32).astype(bf16)
            kn[2 * j, pl.ds(at, rows), :] = kk[:, :128]
            kn[2 * j + 1, pl.ds(at, rows), :] = kk[:, 128:]
            wv = wuv[pl.ds(pl.multiple_of((head0 + 4 * j) * vdim, 4 * vdim), 4 * vdim), :]
            vv = lax.dot_general(wv, c, NT, preferred_element_type=f32).astype(bf16)
            for i in range(4):
                vt[slot * GROUP + 4 * j + i, :vdim, pl.ds(at, rows)] = vv[i * vdim:(i + 1) * vdim, :]

    def queries(buf, src, head0):
        ct, st = trig[src, :hr], trig[src, hr:]
        for j in range(GROUP // 4):
            w = wuq[pl.ds(pl.multiple_of((head0 + 4 * j) * qk, 4 * qk), 4 * qk), :]
            q = lax.dot_general(w, qlat[src], NT, preferred_element_type=f32)
            for i in range(4):
                u = 4 * j + i
                qh = q[i * qk:(i + 1) * qk]
                lo = (u % 2) * nope
                qaug[buf, u, lo:lo + nope, :] = qh[:nope].astype(bf16)
                r1, r2 = qh[nope:nope + hr], qh[nope + hr:]
                qaug[buf, u, 2 * nope:2 * nope + rot, :] = jnp.concatenate([r1 * ct - r2 * st, r2 * ct + r1 * st], axis=0).astype(bf16)

    def clear(slot):
        for u in range(GROUP):
            m_s[slot * GROUP + u] = jnp.full((1, rows), -jnp.inf, f32)

    def block_at(helping, target, i):
        usual = jnp.where(i == 0, target, lax.rem(i + target - 2, jnp.maximum(target, 1)))
        return jnp.where(helping & (me < 2), jnp.where(i < 2, i, 5 - i), usual)

    def group(gi, carry):
        helping, target, grp, slot = place_of(gi)
        gn = jnp.minimum(gi + 1, n_all - 1)
        helping_n, target_n, grp_n, _ = place_of(gn)
        slot_n = lax.rem(gi + 1, SLOTS)

        @pl.when((gi == help_turn - 1) & ((me == 1) | (me == 3)))
        def _():
            for c in query_copies(me):
                c.wait_recv()
            turn(1)

        @pl.when((gi == help_turn - 1) & (me == 0))
        def _():
            for c in query_halves()[1:] + (query_relay(),):
                c.wait_recv()
            start(query_share())
            turn(1)

        @pl.when(gi == 0)
        def _():
            for c in uq_loads[1:]:
                c.wait()

        @pl.when(gi == 1)
        def _():
            for c in wo_loads:
                c.start()

        fresh = ((gi == 0) & (me > 0)) | (helping & (me < 2))

        def one(i, carry):
            blk = block_at(helping, target, i)
            more = i < target
            blk_n = jnp.where(more, block_at(helping, target, i + 1), block_at(helping_n, target_n, 0))

            @pl.when(fresh & more & (blk_n != me))
            def _():
                received(blk_n)

                @pl.when((me >= 2) & (blk_n == 3 - me))
                def _():
                    start(forward_copies(blk_n))

                @pl.when((me == 0) & (blk_n >= 2))
                def _():
                    start(latent_share(blk_n))

            new = (slot, blk, (i == target).astype(jnp.int32), gi)

            def next_keys():
                keys_and_values(jnp.where(more, slot, slot_n), jnp.where(more, grp, grp_n) * GROUP, blk_n)

            def after_own():
                queries(lax.rem(gi + 1, 2), helping_n.astype(jnp.int32), grp_n * GROUP)
                next_keys()
                clear(slot_n)

            @pl.when(blk == target)
            def _():
                step(carry, new, True, after_own)

            @pl.when(blk != target)
            def _():
                step(carry, new, False, next_keys)

            return new, carry[0]

        carry = lax.fori_loop(0, target + 1, one, carry)

        @pl.when(gi == 1)
        def _():
            for u in range(GROUP):
                acc[(SLOTS - 1) * GROUP + u] = jnp.zeros(acc.shape[1:], f32)

        return carry

    idle = (jnp.int32(SLOTS - 1), jnp.int32(0), jnp.int32(0), jnp.int32(0))
    uq_loads[0].wait()
    queries(0, 0, 0)

    for c in w_loads[2:]:
        c.wait()

    @pl.when(me >= 0)
    def _():
        keys_and_values(0, 0, me)
        clear(0)

    carry = lax.fori_loop(0, n_all, group, (idle, idle))
    step(carry, None, False)
    step((idle, carry[0]), None, False, values_only=True)

    for c in wo_loads:
        c.wait()
    deep = GROUP * vdim
    outs = [pltpu.make_async_copy(p_buf.at[n], out_hbm.at[:, pl.ds(n * rows, rows)], out_sem.at[n]) for n in range(tiles)]
    def product(grp, n):
        lhs = jnp.concatenate([o_nat[grp * pairs + j] for j in range(pairs)], axis=1)
        w = wo[pl.ds(pl.multiple_of(grp * deep, deep), deep), n * rows:(n + 1) * rows]
        return lax.dot_general(lhs, w, NN, preferred_element_type=f32)

    def arrive(grp):
        @pl.when(grp >= n_own)
        def _():
            help_copy(grp, me).wait_recv()

    for n in range(tiles):
        s_buf[n] = product(0, n)

    last = ngroup - 2

    def accumulate(i, c):
        grp = i + (i == last).astype(jnp.int32)
        arrive(grp)
        for n in range(tiles):
            s_buf[n] = product(grp, n) + s_buf[n]
        return c

    lax.fori_loop(1, ngroup - 1, accumulate, 0)
    arrive(last)
    for n in range(tiles):
        p_buf[n] = (product(last, n) + s_buf[n]).astype(bf16)
        outs[n].start()
    def sent(copies):
        for c in copies:
            c.wait_send()

    @pl.when(me == 0)
    def _():
        sent(latent_copies(me, 1) + latent_copies(me, 3) + query_share() + latent_share(2) + latent_share(3))

    @pl.when(me == 1)
    def _():
        sent(latent_copies(me, 2) + latent_copies(me, 0))

    @pl.when(me == 2)
    def _():
        sent(latent_copies(me, 3) + latent_copies(me, 0) + forward_copies(1) + query_copies(3) + (query_relay(),))

    @pl.when(me == 3)
    def _():
        sent(latent_copies(me, 0) + forward_copies(0) + query_halves())

    @pl.when(helped > 0)
    def _():
        help_copy(help_group, partner).wait_send()

    for c in outs:
        c.wait()


def layer(pos, gq, gkv, x, wdkv, wdq, wuq, wuk, wuv, wo, scale2, heads, groups):
    rows, dim = x.shape
    rank = gkv.shape[0]
    rot = wdkv.shape[0] - rank
    qrank = wdq.shape[1]
    nope = wuk.shape[0] // heads
    vdim = wuv.shape[0] // heads
    seq = rows * groups
    vm = pl.BlockSpec(memory_space=pltpu.VMEM)
    anym = pl.BlockSpec(memory_space=pltpu.HBM)
    f32 = jnp.float32
    bf16 = jnp.bfloat16
    dma = pltpu.SemaphoreType.DMA
    return pl.pallas_call(
        functools.partial(layer_kernel, scale2=scale2, rows=rows, nope=nope, rot=rot, vdim=vdim, heads=heads, groups=groups),
        out_shape=(jax.ShapeDtypeStruct((rows, dim), bf16),
                   jax.ShapeDtypeStruct((rows, rank), bf16),
                   jax.ShapeDtypeStruct((rot, rows), bf16)),
        in_specs=[vm, vm, vm] + [anym] * 7,
        out_specs=(anym, vm, vm),
        scratch_shapes=[
            pltpu.VMEM(wdkv.shape, bf16),
            pltpu.VMEM(wo.shape, bf16),
            pltpu.VMEM(wuq.shape, bf16),
            pltpu.VMEM(wuk.shape, bf16),
            pltpu.VMEM(wuv.shape, bf16),
            pltpu.VMEM((2, rows, qrank), bf16),
            pltpu.VMEM((2, 8, rows), f32),
            pltpu.VMEM((2, rot, rows), f32),
            pltpu.VMEM((groups, rows, rank), bf16),
            pltpu.VMEM((groups, rot, rows), bf16),
            pltpu.VMEM((groups, rows, 128), bf16),
            pltpu.VMEM((2, GROUP, 256, rows), bf16),
            pltpu.VMEM((GROUP // 2, seq, 128), bf16),
            pltpu.VMEM((SLOTS * GROUP, vdim + 16, seq), bf16),
            pltpu.VMEM((GROUP, rows, rows), f32),
            pltpu.VMEM((GROUP, 1, rows), f32),
            pltpu.VMEM((GROUP, rows, rows), bf16),
            pltpu.VMEM((GROUP, 1, rows), f32),
            pltpu.VMEM((SLOTS * GROUP, 1, rows), f32),
            pltpu.VMEM((SLOTS * GROUP, vdim + 16, rows), f32),
            pltpu.VMEM((heads // 2, rows, 2 * vdim), bf16),
            pltpu.VMEM((GROUP // 2, rows, 2 * vdim), bf16),
            dma((x.shape[1] // rows + 4 + heads // GROUP,)),
            dma((groups,)), dma((groups,)), dma((groups,)), dma((groups,)), dma((2,)),
            dma((3,)), dma((3,)), dma, dma,
            dma, dma((heads // GROUP,)),
            dma((2,)), dma((dim // rows,)),
        ],
        compiler_params=pltpu.CompilerParams(vmem_limit_bytes=LAYER_VMEM, collective_id=0, has_side_effects=True),
        cost_estimate=pl.CostEstimate(flops=40_000_000_000, bytes_accessed=40_000_000, transcendentals=30_000_000),
    )(pos, gq, gkv, x, wdkv, wdq, wuq, wuk, wuv, wo)


def deliver_kernel(out_in, ckv_in, cpe_in, out_hbm, ckv_out, cpe_out, out, ckv, cpe, in_sem, out_sem):
    half = out.shape[0] // 2
    steps = ((ckv_in, ckv, ckv_out, None), (cpe_in, cpe, cpe_out, None), (out_in, out, out_hbm, 0), (out_in, out, out_hbm, half))

    def view(ref, start):
        return ref if start is None else ref.at[pl.ds(start, half)]

    ins = [pltpu.make_async_copy(view(a, n), view(b, n), in_sem.at[i]) for i, (a, b, _, n) in enumerate(steps)]
    outs = [pltpu.make_async_copy(view(b, n), view(c, n), out_sem.at[i]) for i, (_, b, c, n) in enumerate(steps)]
    for c in ins:
        c.start()
    for a, b in zip(ins, outs):
        a.wait()
        b.start()
    for c in outs:
        c.wait()


def deliver(*arrays):
    anym = pl.BlockSpec(memory_space=pl.ANY)
    return pl.pallas_call(
        deliver_kernel,
        in_specs=[anym] * 3,
        out_specs=(anym,) * 3,
        out_shape=tuple(jax.ShapeDtypeStruct(a.shape, a.dtype) for a in arrays),
        scratch_shapes=[pltpu.VMEM(a.shape, a.dtype) for a in arrays] + [pltpu.SemaphoreType.DMA((4,)), pltpu.SemaphoreType.DMA((4,))],
        compiler_params=pltpu.CompilerParams(vmem_limit_bytes=62 * 1024 * 1024),
        cost_estimate=pl.CostEstimate(flops=1000, bytes_accessed=6_000_000, transcendentals=0),
    )(*arrays)


def solution(mesh):
    groups = mesh.shape['sp']
    tok_spec = P(('dp', 'sp'))
    rows_spec = P(('dp', 'sp'), None)
    replicated = P()

    def local_step(tok_in, tok_pos, w_dq, g_q, w_uq, w_dkv, g_kv, w_uk, w_uv, w_o):
        heads, qk_dim = w_uq.shape[1:]
        kv_rank = g_kv.shape[0]
        rot_dim = w_dkv.shape[1] - kv_rank
        v_dim = w_uv.shape[2]
        attn_scale = (0.1 * math.log(YARN_FACTOR) + 1.0) ** 2 / math.sqrt(qk_dim)
        def flat(w):
            return jnp.transpose(w, (1, 2, 0)).reshape(-1, w.shape[0])

        attn_out, cache_kv, cache_pe = layer(tok_pos, g_q, g_kv, tok_in, w_dkv.T, w_dq, flat(w_uq), flat(w_uk), flat(w_uv), w_o.reshape(heads * v_dim, -1),
                                      attn_scale * math.log2(math.e), heads, groups)
        attn_out, cache_kv, cache_pe = deliver(attn_out, cache_kv, cache_pe)
        return attn_out, cache_kv, cache_pe.T

    return jax.shard_map(local_step, mesh=mesh, in_specs=(rows_spec, tok_spec, replicated, replicated, replicated, replicated, replicated, replicated, replicated, replicated), out_specs=(rows_spec, rows_spec, rows_spec), check_vma=False)
```
